32 devices in a mesh: groups: 2 (over y), seq: 16 (over z, x, core).
Axes of the slice: x: 2, y: 2, z: 4, core: 2. Of those that a mesh axis runs over, the one named last changes fastest.
Arguments:
- queries: bfloat16 [8192, 2048], P(('groups', 'seq')), parts along dimension 0, may hold values from -20 to 20
- keys: bfloat16 [8192, 2048], P(('groups', 'seq')), parts along dimension 0, may hold values from -20 to 20
- values: bfloat16 [8192, 2048], P(('groups', 'seq')), parts along dimension 0, may hold values from -6 to 6
- block_counts: int32 [16], P('groups'), parts along dimension 0, may hold values from 2 to 6, as said below
- last_tokens: int32 [32], P('groups'), parts along dimension 0, may hold values from 64 to 128
- pack_order: int32 [32], P('groups'), parts along dimension 0, may hold values from 0 to 15, as said below
- decode_slot: int32 [16], P('groups'), parts along dimension 0, may hold values from 0 to 7, each once
Outputs:
- attended: bfloat16 [8192, 2048], P(('groups', 'seq')), parts along dimension 0
- cache_keys: bfloat16 [32, 32, 128, 128], P(('groups', 'seq')), parts along dimension 0
- cache_values: bfloat16 [32, 32, 128, 128], P(('groups', 'seq')), parts along dimension 0
The draws below stay inside these ranges and needn't reach their ends.
There are 2 independent parts, one for each index of `groups`. The reference program is written for one: setup_inputs(seed, part) draws one part's arguments, and reference() takes and returns one part's arrays. A program takes and returns all parts, laid end to end along the dimension named above; each array names one. Nothing has to cross between parts.
Inputs may be any that keep to these rules, and one draw needn't show every extreme that they name: `block_counts`: they sum to 24; the largest equals 6. `pack_order`: each prompt number appears once. The last 1 positions hold null prompts, and the position before them a conditional prompt of 6 blocks. `decode_slot`: each slot appears once.
All inputs are finite; a program needn't handle non-finite values.
Results may differ from the reference program's by a relative error of at most 0.0034.
Values may be sent and summed in bfloat16 or wider, within the bound.
A program may use at most 64 MiB of HBM per device.

```python
import jax
import jax.numpy as jnp
from jax import lax

HEADS = 16
HEAD_DIM = 128
BLOCK = 128
MAXB = 6
BLK_DEV = 2
NB = 32
TOKENS = 4096
PAIRS = 8
SPLITS = 1
SLICE = 128


def draw_queries(key, part):
    noise = jnp.clip(jax.random.normal(jax.random.fold_in(key, 1), (TOKENS, HEADS * HEAD_DIM), jnp.float32), -6.0, 6.0)
    return noise.astype(jnp.bfloat16)


def draw_keys(key, part):
    noise = jnp.clip(jax.random.normal(jax.random.fold_in(key, 2), (TOKENS, HEADS * HEAD_DIM), jnp.float32), -6.0, 6.0)
    return noise.astype(jnp.bfloat16)


def pack_plan(key):
    base = jax.random.fold_in(key, 11)
    first_key, second_key, third_key, fourth_key = jax.random.split(base, 4)
    pair_ids = jnp.arange(PAIRS, dtype=jnp.int32)
    biggest = jax.random.randint(first_key, (), 0, PAIRS).astype(jnp.int32)
    counts = jnp.where(pair_ids == biggest, MAXB, 2).astype(jnp.int32)
    extra = NB - PAIRS - (2 * (PAIRS - 1) + MAXB)

    def add_one(step, current):
        scores = jax.random.randint(jax.random.fold_in(second_key, step), (PAIRS,), 0, 1 << 20).astype(jnp.int32) * PAIRS + pair_ids
        scores = jnp.where(current < MAXB, scores, -1)
        chosen = jnp.argmax(scores).astype(jnp.int32)
        return current + (pair_ids == chosen).astype(jnp.int32)
    counts = lax.fori_loop(0, extra, add_one, counts)
    null_order = jax.random.permutation(third_key, PAIRS).astype(jnp.int32)
    tail_nulls = PAIRS + null_order[:BLK_DEV - 1]
    spare_nulls = PAIRS + null_order[BLK_DEV - 1:]
    spare_count = PAIRS - BLK_DEV + 1
    cond_order = jax.random.permutation(fourth_key, PAIRS).astype(jnp.int32)
    rank_keys = jnp.where(cond_order == biggest, PAIRS, pair_ids).astype(jnp.int32)
    cond_seq = cond_order[jnp.argsort(rank_keys, stable=True)][:PAIRS - 1]
    first_edge = BLK_DEV
    middle_edge = NB // BLK_DEV // 2 * BLK_DEV
    order = jnp.zeros((2 * PAIRS,), jnp.int32)

    def place(step, carry):
        current, write, start, queue = carry
        prompt = cond_seq[step]
        size = counts[prompt]
        filler = (start + size == first_edge) | (start + size == middle_edge)
        current = current.at[write].set(jnp.where(filler, spare_nulls[queue], prompt))
        bump = filler.astype(jnp.int32)
        write = write + bump
        start = start + bump
        queue = queue + bump
        current = current.at[write].set(prompt)
        return (current, write + 1, start + size, queue)
    zero = jnp.zeros((), jnp.int32)
    order, write, start, queue = lax.fori_loop(0, PAIRS - 1, place, (order, zero, zero, zero))

    def rest(index, current):
        keep = index >= queue
        target = jnp.where(keep, write + index - queue, 2 * PAIRS - 1).astype(jnp.int32)
        return current.at[target].set(jnp.where(keep, spare_nulls[index], current[target]))
    order = lax.fori_loop(0, spare_count, rest, order)
    order = order.at[2 * PAIRS - BLK_DEV].set(biggest)
    order = order.at[2 * PAIRS - BLK_DEV + 1:].set(tail_nulls)
    return (counts, order.astype(jnp.int32))


def draw_block_counts(key, part):
    counts, order = pack_plan(key)
    return counts


def draw_pack_order(key, part):
    counts, order = pack_plan(key)
    return order


def touch_ends(array, rng, smallest, high):
    shape = array.shape
    spot = [jax.random.randint(jax.random.fold_in(rng, axis), (), 0, shape[axis]) for axis in range(len(shape))]
    array = array.at[tuple(spot)].set(smallest)
    longest = shape.index(max(shape))
    spot[longest] = (spot[longest] + 1) % shape[longest]
    return array.at[tuple(spot)].set(high)


def levels(rng, shape, cuts, smallest, largest):
    factor_of = 1.0
    for dim, parts in cuts:
        draws = jax.random.uniform(jax.random.fold_in(jax.random.fold_in(rng, 6), dim), (parts,), jnp.float32, smallest / len(cuts), largest / len(cuts))
        factor_of = factor_of * jnp.repeat(jnp.exp(draws), shape[dim] // parts).reshape((-1,) + (1,) * (len(shape) - 1 - dim))
    return factor_of


def bell_draw(rng, shape, scale, reach, cuts=(), kind=jnp.bfloat16):
    factor_of = levels(rng, shape, cuts, -0.22, 0.18) if cuts else 1.0
    array = jax.random.normal(rng, shape, jnp.float32) * scale * factor_of
    return jnp.minimum(jnp.maximum(array, -reach), reach).astype(kind)


def setup_inputs(seed: int = 0, part: int = 0) -> dict:
    splits = jax.random.split(jax.random.key(seed), 8)
    own_keys = jax.random.split(jax.random.fold_in(splits[7], part), 8)
    queries = draw_queries(jax.random.fold_in(jax.random.fold_in(splits[7], part), 71), part)
    keys = draw_keys(jax.random.fold_in(jax.random.fold_in(splits[7], part), 71), part)
    values = bell_draw(own_keys[2], (TOKENS, HEADS * HEAD_DIM), 1.0, 6.0, ((0, 16),))
    block_counts = draw_block_counts(jax.random.fold_in(jax.random.fold_in(splits[7], part), 71), part)
    last_tokens = touch_ends(jax.random.randint(own_keys[4], (2 * PAIRS,), BLOCK // 2, BLOCK + 1), jax.random.fold_in(own_keys[4], 1), BLOCK // 2, BLOCK).astype(jnp.int32)
    pack_order = draw_pack_order(jax.random.fold_in(jax.random.fold_in(splits[7], part), 71), part)
    decode_slot = jax.random.permutation(own_keys[6], PAIRS).astype(jnp.int32)
    return {"queries": queries, "keys": keys, "values": values, "block_counts": block_counts, "last_tokens": last_tokens, "pack_order": pack_order, "decode_slot": decode_slot}


MASKED_SCORE = -1.0e30


def block_tables(block_counts, last_tokens, pack_order, decode_slot, total_blocks, block):
    pair_count = block_counts.shape[0]
    prompts = 2 * pair_count
    prompt_ids = jnp.arange(prompts, dtype=jnp.int32)
    prompt_sizes = jnp.concatenate([block_counts, jnp.ones((pair_count,), jnp.int32)])
    picked = (pack_order[:, None] == prompt_ids[None, :]).astype(jnp.int32)
    packed_sizes = jnp.sum(picked * prompt_sizes[None, :], axis=1).astype(jnp.int32)
    packed_tails = jnp.sum(picked * last_tokens[None, :], axis=1).astype(jnp.int32)
    block_ends = jnp.cumsum(packed_sizes).astype(jnp.int32)
    starts = block_ends - packed_sizes
    blocks = jnp.arange(total_blocks, dtype=jnp.int32)
    member = ((starts[None, :] <= blocks[:, None]) & (blocks[:, None] < block_ends[None, :])).astype(jnp.int32)
    position = jnp.sum(member * prompt_ids[None, :], axis=1).astype(jnp.int32)
    prompt = jnp.sum(member * pack_order[None, :], axis=1).astype(jnp.int32)
    within = blocks - jnp.sum(member * starts[None, :], axis=1).astype(jnp.int32)
    is_last = (blocks + 1) == jnp.sum(member * block_ends[None, :], axis=1).astype(jnp.int32)
    valid_tokens = jnp.where(is_last, jnp.sum(member * packed_tails[None, :], axis=1).astype(jnp.int32), block).astype(jnp.int32)
    pair_ids = jnp.arange(pair_count, dtype=jnp.int32)
    earlier = (decode_slot[None, :] < decode_slot[:, None]).astype(jnp.int32)
    slot_start = jnp.sum(earlier * (block_counts + 1)[None, :], axis=1).astype(jnp.int32)
    pair_of = prompt % pair_count
    owner = (pair_of[:, None] == pair_ids[None, :]).astype(jnp.int32)
    base_slot = jnp.sum(owner * slot_start[None, :], axis=1).astype(jnp.int32)
    own_count = jnp.sum(owner * block_counts[None, :], axis=1).astype(jnp.int32)
    destination = base_slot + jnp.where(prompt >= pair_count, own_count, within)
    hits = (destination[None, :] == blocks[:, None]).astype(jnp.int32)
    source = jnp.sum(hits * blocks[None, :], axis=1).astype(jnp.int32)
    return position, valid_tokens, source


def reference(queries, keys, values, block_counts, last_tokens, pack_order, decode_slot):
    position, valid_tokens, source = block_tables(block_counts, last_tokens, pack_order, decode_slot, NB, BLOCK)
    features = HEADS * HEAD_DIM
    back = MAXB - 1
    span = (back + 1) * BLOCK
    padding = jnp.zeros((back * BLOCK, features), jnp.bfloat16)
    padded_keys = jnp.concatenate([padding, keys], axis=0)
    padded_values = jnp.concatenate([padding, values], axis=0)
    padded_docs = jnp.concatenate([jnp.full((back,), -1, jnp.int32), position])
    padded_valid = jnp.concatenate([jnp.zeros((back,), jnp.int32), valid_tokens])
    token_ids = jnp.arange(BLOCK, dtype=jnp.int32)
    key_blocks = jnp.repeat(jnp.arange(back + 1, dtype=jnp.int32), BLOCK)
    key_tokens = jnp.tile(token_ids, back + 1)
    score_scale = HEAD_DIM ** -0.5

    def one_block(block_index):
        start = (block_index * BLOCK).astype(jnp.int32)
        key_window = lax.dynamic_slice_in_dim(padded_keys, start, span, 0).reshape(span, HEADS, HEAD_DIM)
        value_window = lax.dynamic_slice_in_dim(padded_values, start, span, 0).reshape(span, HEADS, HEAD_DIM)
        window_docs = lax.dynamic_slice_in_dim(padded_docs, block_index, back + 1)
        window_valid = lax.dynamic_slice_in_dim(padded_valid, block_index, back + 1)
        query_block = lax.dynamic_slice_in_dim(queries, start, BLOCK, 0).reshape(BLOCK, HEADS, HEAD_DIM)
        own_doc = window_docs[back]
        own_valid = window_valid[back]
        key_ok = (jnp.repeat(window_docs, BLOCK) == own_doc) & (key_tokens < jnp.repeat(window_valid, BLOCK))
        causal = (key_blocks[None, :] < back) | (key_tokens[None, :] <= token_ids[:, None])
        allowed = causal & key_ok[None, :]
        scores = jnp.einsum("qhd,khd->hqk", query_block.astype(jnp.float32), key_window.astype(jnp.float32)) * score_scale
        scores = jnp.where(allowed[None], scores, MASKED_SCORE)
        peak = jnp.max(scores, axis=2, keepdims=True)
        weights = jnp.exp(scores - peak)
        totals = jnp.sum(weights, axis=2, keepdims=True)
        rounded = lax.optimization_barrier(weights.astype(jnp.bfloat16)).astype(jnp.float32)
        mixed = jnp.einsum("hqk,khd->hqd", rounded, value_window.astype(jnp.float32)) / totals
        mixed = jnp.where((token_ids < own_valid)[None, :, None], mixed, 0.0)
        return jnp.transpose(mixed, (1, 0, 2)).reshape(BLOCK, features).astype(jnp.bfloat16)

    attended = lax.map(one_block, jnp.arange(NB, dtype=jnp.int32)).reshape(TOKENS, features)

    def relayout(source_array):
        grid = source_array.reshape(NB, SPLITS, SLICE, HEADS, HEAD_DIM)
        reordered = jnp.take(grid, source, axis=0)
        return jnp.transpose(reordered, (3, 1, 0, 2, 4)).reshape(HEADS * SPLITS, NB, SLICE, HEAD_DIM)

    return attended, relayout(keys), relayout(values)
```

```python
import functools
import math

import jax
import jax.numpy as jnp
from jax import lax
from jax.experimental import pallas as pl
from jax.experimental.pallas import tpu as pltpu
from jax.sharding import PartitionSpec as P

HEADS = 16
HEAD_DIM = 128
BLOCK = 128
MAXB = 6
BACK = MAXB - 1
HIDDEN = -1e30
PLANE = 4
CHUNKS = 4
RELAY = BACK
ROUND = 2


def window_tables(counts_ref, tails_ref, order_ref, first, width):
    pairs = counts_ref.shape[0]
    prompts = order_ref.shape[0]

    def place(i, carry):
        start, docs, valids = carry
        prompt = order_ref[i]
        counted = counts_ref[lax.rem(prompt, pairs)]
        size = jnp.where(prompt < pairs, counted, 1)
        tail = tails_ref[prompt]
        end = start + size
        new_docs, new_valids = [], []
        for w in range(width):
            b = first + w
            inside = (start <= b) & (b < end)
            new_docs.append(jnp.where(inside, i, docs[w]))
            new_valids.append(
                jnp.where(inside, jnp.where(b + 1 == end, tail, BLOCK), valids[w])
            )
        return end, tuple(new_docs), tuple(new_valids)

    none = jnp.int32(-1)
    zero = jnp.int32(0)
    _, docs, valids = lax.fori_loop(
        0, prompts, place, (zero, (none,) * width, (zero,) * width)
    )
    return docs, valids


def exchange(
    n,
    counts_ref,
    tails_ref,
    order_ref,
    q_hbm,
    k_hbm,
    v_hbm,
    out_ref,
    landed_ref,
    q_ref,
    own,
    halo,
    relay,
    bias,
    halo_send,
    halo_recv,
    cache_sem,
    own_sem,
    load_sem,
):
    me = lax.axis_index("seq")
    role = lax.rem(me, PLANE)
    plane = me // PLANE
    planes = n // PLANE
    tokens, features = q_ref.shape
    here = tokens // BLOCK
    splits = n // HEADS
    part = BLOCK // splits
    wide = features // CHUNKS

    loads = [
        pltpu.make_async_copy(src, dst, load_sem.at[i])
        for i, (src, dst) in enumerate(
            ((k_hbm, own.at[0]), (v_hbm, own.at[1]), (q_hbm, q_ref))
        )
    ]
    for copy in loads:
        copy.start()

    barrier = pltpu.get_barrier_semaphore()

    def greet(r, carry):
        pl.semaphore_signal(
            barrier,
            inc=1,
            device_id={"seq": lax.rem(me + r, n)},
            device_id_type=pl.DeviceIdType.MESH,
        )
        return carry

    lax.fori_loop(1, n, greet, 0)
    loads[0].wait()
    loads[1].wait()
    pl.semaphore_wait(barrier, n - 1)

    pending = []

    def spot(block, c):
        return (
            slice(None),
            pl.ds(block * BLOCK, BLOCK),
            pl.ds(c * wide, wide),
        )

    def mine(block):
        return lambda c: own.at[spot(block, c)]

    def held(slot):
        if slot >= RELAY:
            return lambda c: relay.at[spot(slot - RELAY, c)]
        return lambda c: halo.at[spot(slot, c)]

    def start(cond, c, moves):
        copies = []
        for src, target, slot in moves:
            copy = pltpu.make_async_remote_copy(
                src_ref=src(c),
                dst_ref=held(slot)(c),
                send_sem=halo_send.at[len(pending)],
                recv_sem=halo_recv.at[slot, c],
                device_id={"seq": lax.rem(target + n, n)},
                device_id_type=pl.DeviceIdType.MESH,
            )
            pending.append((cond, copy))
            copies.append(copy)

        @pl.when(cond)
        def _():
            for copy in copies:
                copy.start()

    def await_slots(cond, c, slots):
        @pl.when(cond)
        def _():
            for slot in slots:
                ref = held(slot)(c)
                pltpu.make_async_copy(ref, ref, halo_recv.at[slot, c]).wait()

    more = plane < planes - 1
    late = plane > 0
    for c in range(CHUNKS):
        start((role == 3) & more, c, [(mine(0), me + 3, RELAY), (mine(1), me + 3, 0)])
        if c < ROUND:
            moves = [(mine(1), me - 2, RELAY + 1), (mine(0), me - 2, RELAY)]
        else:
            moves = [(mine(1), me + 2, 2), (mine(0), me + 2, 1)]
        start((role == 2) & more, c, moves)
        start((role == 1) & more, c, [(mine(1), me + 3, 0)])
        start(role == 1, c, [(mine(0), me + 1, 3), (mine(1), me + 1, 4)])
        start(role == 0, c, [(mine(1), me + 2, 2), (mine(0), me + 2, 1)])
        start(
            (role == 0) | (role == 2),
            c,
            [(mine(0), me + 1, 3), (mine(1), me + 1, 4)],
        )

    def piece(owner, block):
        head = owner // splits
        cols = pl.ds(pl.multiple_of(head * HEAD_DIM, HEAD_DIM), HEAD_DIM)
        if splits == 1:
            return own.at[:, :, cols]
        offset = pl.multiple_of(block * BLOCK + lax.rem(owner, splits) * part, part)
        return own.at[:, pl.ds(offset, part), cols]

    def place(block):
        if splits == 1:
            return landed_ref.at[:, pl.ds(pl.multiple_of(me * tokens, tokens), tokens)]
        return landed_ref.at[
            :, pl.ds(pl.multiple_of((me * here + block) * part, part), part)
        ]

    pieces = 1 if splits == 1 else here

    def give(s, carry):
        sign = 1 - 2 * lax.rem(s, 2)
        target = lax.rem(me + n // 2 + sign * ((s + 1) // 2), n)
        for block in range(pieces):
            pltpu.make_async_remote_copy(
                src_ref=piece(target, block),
                dst_ref=place(block),
                send_sem=cache_sem.at[0],
                recv_sem=cache_sem.at[1],
                device_id={"seq": target},
                device_id_type=pl.DeviceIdType.MESH,
            ).start()
        return carry

    cuts = [(n - 1) * i // CHUNKS for i in range(CHUNKS + 1)]

    docs, valids = window_tables(
        counts_ref, tails_ref, order_ref, me * here - BACK, BACK + here
    )
    row = lax.broadcasted_iota(jnp.int32, (BLOCK, BLOCK), 0)
    col = lax.broadcasted_iota(jnp.int32, (BLOCK, BLOCK), 1)
    for b in range(here):
        for w in range(BACK + here):
            if w > BACK + b:
                shade = jnp.full((BLOCK, BLOCK), HIDDEN, jnp.float32)
            else:
                limit = jnp.where(docs[w] == docs[BACK + b], valids[w], 0)
                seen = col < limit
                if w == BACK + b:
                    seen = seen & (col <= row)
                shade = jnp.where(seen, 0.0, HIDDEN)
            bias[b * BLOCK : (b + 1) * BLOCK, w * BLOCK : (w + 1) * BLOCK] = shade
    column = lax.broadcasted_iota(jnp.int32, (BLOCK, HEAD_DIM), 0)
    real = jnp.concatenate(
        [column < valids[BACK + b] for b in range(here)], axis=0
    )

    empty = jnp.zeros((BLOCK, features), halo.dtype)
    for slot, reach in ((0, 3), (1, 2), (2, 2), (3, 1), (4, 1)):

        @pl.when(me < reach)
        def _():
            for kv in range(2):
                halo[kv, slot * BLOCK : (slot + 1) * BLOCK, :] = empty

    loads[2].wait()

    factor = HEAD_DIM ** (-0.5) * math.log2(math.e)
    prior = BACK * BLOCK
    nt = (((1,), (1,)), ((), ()))

    def one_head(h, carry):
        cols = pl.ds(pl.multiple_of(h * HEAD_DIM, HEAD_DIM), HEAD_DIM)
        q = q_ref[:, cols]
        s1 = lax.dot_general(q, halo[0, :, cols], nt, preferred_element_type=jnp.float32)
        s2 = lax.dot_general(q, own[0, :, cols], nt, preferred_element_type=jnp.float32)
        s1 = s1 + bias[:, :prior]
        s2 = s2 + bias[:, prior:]
        peak = jnp.maximum(
            jnp.max(s1, axis=1, keepdims=True), jnp.max(s2, axis=1, keepdims=True)
        )
        w1 = jnp.exp2((s1 - peak) * factor)
        w2 = jnp.exp2((s2 - peak) * factor)
        total = jnp.sum(w1, axis=1, keepdims=True) + jnp.sum(w2, axis=1, keepdims=True)
        mixed = jnp.dot(
            w1.astype(jnp.bfloat16), halo[1, :, cols], preferred_element_type=jnp.float32
        ) + jnp.dot(
            w2.astype(jnp.bfloat16), own[1, :, cols], preferred_element_type=jnp.float32
        )
        out_ref[:, cols] = jnp.where(real, mixed / total, 0.0).astype(out_ref.dtype)
        return carry

    for c in range(CHUNKS):
        lax.fori_loop(cuts[c], cuts[c + 1], give, 0)
        if c < ROUND:
            await_slots((role == 0) & more, c, [RELAY, RELAY + 1])
            start(
                (role == 0) & more,
                c,
                [(held(RELAY + 1), me + PLANE, 2), (held(RELAY), me + PLANE, 1)],
            )
        await_slots((role == 2) & late, c, [RELAY, 0])
        start(
            (role == 2) & late, c, [(held(RELAY), me - 2 + n, 3), (held(0), me - 2 + n, 4)]
        )
        await_slots((role == 0) & late, c, [2, 3, 4])
        await_slots(role == 2, c, [2, 3, 4])
        start(
            (role == 2) | ((role == 0) & late),
            c,
            [(held(2), me + 1, 0), (held(3), me + 1, 1), (held(4), me + 1, 2)],
        )
        await_slots((role == 0) & late, c, [0, 1])
        await_slots(role == 1, c, [3, 4])
        await_slots((role == 1) & late, c, [0, 1, 2])
        await_slots(role == 2, c, [1])
        await_slots(role == 3, c, [0, 1, 2, 3, 4])
        each = HEADS // CHUNKS
        lax.fori_loop(c * each, (c + 1) * each, one_head, 0)

    copies = [
        pltpu.make_async_copy(piece(me, block), place(block), own_sem.at[block])
        for block in range(pieces)
    ]
    for copy in copies:
        copy.start()

    for cond, copy in pending:

        @pl.when(cond)
        def _():
            copy.wait_send()

    for copy in copies:
        copy.wait()
    others = landed_ref.shape[1] // n * (n - 1)
    ref = landed_ref.at[:, pl.ds(0, others)]
    pltpu.make_async_copy(ref, ref, cache_sem.at[0]).wait()
    pltpu.make_async_copy(ref, ref, cache_sem.at[1]).wait()


def reorder(
    counts_ref,
    order_ref,
    slot_ref,
    landed_ref,
    mixed_ref,
    attended_ref,
    keys_ref,
    values_ref,
    staged,
    passed,
    who,
    base,
    in_sem,
    out_sem,
):
    enter = pltpu.make_async_copy(mixed_ref, passed, in_sem.at[2])
    enter.start()
    pairs = counts_ref.shape[0]
    prompts = order_ref.shape[0]
    blocks, part = staged.shape[1:3]

    def invert(p, carry):
        who[slot_ref[p]] = p
        return carry

    lax.fori_loop(0, pairs, invert, 0)

    def lay(s, first):
        p = who[s]
        base[p] = first
        return first + counts_ref[p] + 1

    lax.fori_loop(0, pairs, lay, jnp.int32(0))

    def fetch(i, first):
        prompt = order_ref[i]
        pair = lax.rem(prompt, pairs)
        null = prompt >= pairs
        counted = counts_ref[pair]
        size = jnp.where(null, 1, counted)
        target = base[pair] + jnp.where(null, counted, 0)

        def one(w, carry):
            for kv in range(2):
                pltpu.make_async_copy(
                    landed_ref.at[kv, pl.ds((first + w) * part, part)],
                    staged.at[kv, target + w],
                    in_sem.at[kv],
                ).start()
            return carry

        lax.fori_loop(0, size, one, 0)
        return first + size

    lax.fori_loop(0, prompts, fetch, jnp.int32(0))
    enter.wait()
    outs = [pltpu.make_async_copy(passed, attended_ref, out_sem.at[2])]
    outs[0].start()
    for kv, ref in enumerate((keys_ref, values_ref)):
        pltpu.make_async_copy(staged.at[kv], staged.at[kv], in_sem.at[kv]).wait()
        copy = pltpu.make_async_copy(staged.at[kv], ref.at[0], out_sem.at[kv])
        copy.start()
        outs.append(copy)
    for copy in outs:
        copy.wait()


def handoff(
    n,
    counts_ref,
    tails_ref,
    order_ref,
    q_hbm,
    k_hbm,
    v_hbm,
    out_ref,
    landed_ref,
    q_ref,
    own,
    kv,
    qs,
    mixed_ref,
    bias,
    load_sem,
    local_sem,
    kv_send,
    kv_recv,
    q_send,
    q_recv,
    halo_send,
    halo_recv,
    land_send,
    land_recv,
    out_send,
    out_recv,
):
    me = lax.axis_index("seq")
    role = lax.rem(me, PLANE)
    plane = me // PLANE
    planes = n // PLANE
    tokens, features = q_ref.shape
    here = tokens // BLOCK
    width = PLANE * here
    skip = width - BACK
    peers = (role + 1 - 2 * lax.rem(role, 2), lax.rem(role + 2, PLANE), PLANE - 1 - role)
    more = plane < planes - 1
    late = plane > 0

    def rows(first, count):
        return pl.ds(pl.multiple_of(first * BLOCK, BLOCK), count * BLOCK)

    def cols(head):
        return pl.ds(pl.multiple_of(head * HEAD_DIM, HEAD_DIM), HEAD_DIM)

    def remote(src, dst, send, recv, target):
        pltpu.make_async_remote_copy(
            src_ref=src,
            dst_ref=dst,
            send_sem=send,
            recv_sem=recv,
            device_id={"seq": target},
            device_id_type=pl.DeviceIdType.MESH,
        ).start()

    def await_(ref, sem):
        pltpu.make_async_copy(ref, ref, sem).wait()

    mine = rows(BACK + role * here, here)
    place = rows(role * here, here)

    loads = [
        pltpu.make_async_copy(src, dst, load_sem.at[i])
        for i, (src, dst) in enumerate(
            ((k_hbm, own.at[0]), (v_hbm, own.at[1]), (q_hbm, q_ref))
        )
    ]
    loads[0].start()
    loads[1].start()
    for j in range(planes):
        here_cols = cols(j * PLANE + role)
        for i, src in enumerate((k_hbm, v_hbm)):
            pltpu.make_async_copy(
                src.at[:, here_cols], kv.at[j, i, mine], local_sem.at[0]
            ).start()
    loads[2].start()
    for j in range(planes):
        here_cols = cols(j * PLANE + role)
        pltpu.make_async_copy(
            q_hbm.at[:, here_cols], qs.at[j, place], local_sem.at[1]
        ).start()

    barrier = pltpu.get_barrier_semaphore()
    base = plane * PLANE
    for peer in peers:
        pl.semaphore_signal(
            barrier,
            inc=1,
            device_id={"seq": base + peer},
            device_id_type=pl.DeviceIdType.MESH,
        )
    for step in range(1, planes):
        pl.semaphore_signal(
            barrier,
            inc=1,
            device_id={"seq": lax.rem(me + step * PLANE, n)},
            device_id_type=pl.DeviceIdType.MESH,
        )

    loads[0].wait()
    loads[1].wait()
    pl.semaphore_wait(barrier, PLANE - 1 + planes - 1)

    def share(t, carry):
        j = planes - 1 - t
        for k in (1, 2, 0):
            head = j * PLANE + peers[k]
            remote(
                own.at[:, :, cols(head)],
                kv.at[j, :, mine],
                kv_send.at[0],
                kv_recv.at[k, j],
                base + peers[k],
            )
        return carry

    lax.fori_loop(0, planes, share, 0)
    loads[2].wait()

    def share_q(t, carry):
        j = planes - 1 - t
        for k in (1, 2, 0):
            head = j * PLANE + peers[k]
            remote(
                q_ref.at[:, cols(head)],
                qs.at[j, place],
                q_send.at[0],
                q_recv.at[k, j],
                base + peers[k],
            )
        return carry

    lax.fori_loop(0, planes, share_q, 0)

    def forward(j, rho):
        first = BACK + rho * here

        @pl.when(more & (rho * here >= skip))
        def _():
            remote(
                kv.at[j, :, rows(first, here)],
                kv.at[j, :, rows(jnp.maximum(rho * here - skip, 0), here)],
                halo_send.at[0],
                halo_recv.at[j, rho],
                me + PLANE,
            )

        @pl.when(more & (rho * here < skip) & (rho * here + here > skip))
        def _():
            remote(
                kv.at[j, :, rows(BACK + skip, BACK % here)],
                kv.at[j, :, rows(0, BACK % here)],
                halo_send.at[0],
                halo_recv.at[j, rho],
                me + PLANE,
            )

        @pl.when(j < plane)
        def _():
            remote(
                kv.at[j, :, rows(first, here)],
                landed_ref.at[:, rows(plane * width + rho * here, here)],
                land_send.at[0, j],
                land_recv.at[0],
                j * PLANE + role,
            )

    await_(kv.at[:, :, mine], local_sem.at[0])

    def forward_mine(t, carry):
        forward(planes - 1 - t, role)
        return carry

    lax.fori_loop(0, planes, forward_mine, 0)

    def take(k):
        def body(t, carry):
            j = planes - 1 - t
            await_(kv.at[j, :, rows(BACK + peers[k] * here, here)], kv_recv.at[k, j])
            forward(j, peers[k])
            return carry

        return body

    lax.fori_loop(0, planes, take(0), 0)

    docs, valids = window_tables(
        counts_ref, tails_ref, order_ref, plane * width - BACK, BACK + width
    )
    row = lax.broadcasted_iota(jnp.int32, (BLOCK, BLOCK), 0)
    col = lax.broadcasted_iota(jnp.int32, (BLOCK, BLOCK), 1)
    for i in range(PLANE):
        for b in range(here):
            target = BACK + i * here + b
            for w in range(BACK + here):
                if w > BACK + b:
                    shade = jnp.full((BLOCK, BLOCK), HIDDEN, jnp.float32)
                else:
                    source = i * here + w
                    limit = jnp.where(docs[source] == docs[target], valids[source], 0)
                    seen = col < limit
                    if w == BACK + b:
                        seen = seen & (col <= row)
                    shade = jnp.where(seen, 0.0, HIDDEN)
                bias[i, b * BLOCK : (b + 1) * BLOCK, w * BLOCK : (w + 1) * BLOCK] = shade
    column = lax.broadcasted_iota(jnp.int32, (BLOCK, HEAD_DIM), 0)

    @pl.when(plane == 0)
    def _():
        empty = jnp.zeros((planes, 2, BACK * BLOCK, HEAD_DIM), kv.dtype)
        kv[:, :, : BACK * BLOCK, :] = empty

    def take_both(t, carry):
        take(1)(t, carry)
        take(2)(t, carry)
        return carry

    lax.fori_loop(0, planes, take_both, 0)

    def climb(t, carry):
        j = planes - 1 - t

        @pl.when(j > plane)
        def _():
            remote(
                kv.at[j, :, rows(BACK, skip)],
                landed_ref.at[:, rows(plane * width, skip)],
                land_send.at[1, j],
                land_recv.at[0],
                j * PLANE + role,
            )

        return carry

    lax.fori_loop(0, planes, climb, 0)
    settle = pltpu.make_async_copy(
        kv.at[plane, :, rows(BACK, width)],
        landed_ref.at[:, rows(plane * width, width)],
        load_sem.at[0],
    )
    settle.start()
    await_(qs.at[:, place], local_sem.at[1])

    factor = HEAD_DIM ** (-0.5) * math.log2(math.e)
    nt = (((1,), (1,)), ((), ()))
    span = (BACK + here) * BLOCK

    def attend(j, i):
        window = pl.ds(i * tokens, span)
        q = qs[j, pl.ds(i * tokens, tokens), :]
        s = lax.dot_general(q, kv[j, 0, window, :], nt, preferred_element_type=jnp.float32)
        s = s + bias[i]
        peak = jnp.max(s, axis=1, keepdims=True)
        w = jnp.exp2((s - peak) * factor)
        total = jnp.sum(w, axis=1, keepdims=True)
        mixed = jnp.dot(
            w.astype(jnp.bfloat16), kv[j, 1, window, :], preferred_element_type=jnp.float32
        )
        real = jnp.concatenate(
            [column < valids[BACK + i * here + b] for b in range(here)], axis=0
        )
        mixed_ref[j, i] = jnp.where(real, mixed / total, 0.0).astype(mixed_ref.dtype)

    def give(j, i):
        target = out_ref.at[:, cols(j * PLANE + role)]

        @pl.when(role == i)
        def _():
            pltpu.make_async_copy(mixed_ref.at[j, i], target, local_sem.at[2]).start()

        @pl.when(role != i)
        def _():
            remote(mixed_ref.at[j, i], target, out_send.at[0], out_recv.at[0], base + i)

    def one_head(t, carry):
        j = planes - 1 - t
        for k in range(PLANE - 1):
            await_(qs.at[j, rows(peers[k] * here, here)], q_recv.at[k, j])
        attend(j, PLANE - 1)

        @pl.when(t > 0)
        def _():
            give(jnp.minimum(j + 1, planes - 1), 0)

        @pl.when(late)
        def _():
            for rho in range(PLANE):
                count = min(here, (rho + 1) * here - skip)
                if count > 0:
                    await_(
                        kv.at[j, :, rows(max(rho * here - skip, 0), count)],
                        halo_recv.at[j, rho],
                    )

        @pl.when(late & (j > plane))
        def _():
            remote(
                kv.at[j, :, rows(0, BACK)],
                landed_ref.at[:, rows(jnp.maximum(plane * width - BACK, 0), BACK)],
                land_send.at[2, j],
                land_recv.at[0],
                j * PLANE + role,
            )

        for i in range(PLANE - 2, -1, -1):
            attend(j, i)
            give(j, i + 1)
        return carry

    lax.fori_loop(0, planes, one_head, 0)

    settled = pltpu.make_async_copy(
        kv.at[plane, :, rows(0, BACK)],
        landed_ref.at[:, rows(jnp.maximum(plane * width - BACK, 0), BACK)],
        load_sem.at[1],
    )

    @pl.when(late)
    def _():
        settled.start()

    give(0, 0)

    others = features // PLANE * (PLANE - 1)
    await_(own.at[:, :, pl.ds(0, others)], kv_send.at[0])
    await_(q_ref.at[:, pl.ds(0, others)], q_send.at[0])
    await_(q_ref.at[:, pl.ds(0, features // PLANE)], local_sem.at[2])

    @pl.when(more)
    def _():
        await_(kv.at[:, :, rows(0, BACK)], halo_send.at[0])

    def drain(j, carry):
        @pl.when(j < plane)
        def _():
            await_(kv.at[j, :, rows(BACK, width)], land_send.at[0, j])

        @pl.when(j > plane)
        def _():
            await_(kv.at[j, :, rows(BACK, skip)], land_send.at[1, j])

        @pl.when(late & (j > plane))
        def _():
            await_(kv.at[j, :, rows(0, BACK)], land_send.at[2, j])

        return carry

    lax.fori_loop(0, planes, drain, 0)
    settle.wait()

    @pl.when(late)
    def _():
        settled.wait()
        await_(landed_ref.at[:, rows(0, (planes - 1) * width - BACK)], land_recv.at[0])

    @pl.when(plane == 0)
    def _():
        await_(landed_ref.at[:, rows(0, (planes - 1) * width)], land_recv.at[0])

    await_(q_ref.at[:, pl.ds(0, others)], out_send.at[0])
    await_(q_ref.at[:, pl.ds(0, others)], out_recv.at[0])


def wide_exchange(n, queries, keys, values, block_counts, last_tokens, pack_order):
    tokens, features = queries.shape
    here = tokens // BLOCK
    part = BLOCK // (n // HEADS)
    blocks = here * n
    kind = queries.dtype
    smem = pl.BlockSpec(memory_space=pltpu.SMEM)
    vmem = pl.BlockSpec(memory_space=pltpu.VMEM)
    anywhere = pl.BlockSpec(memory_space=pl.ANY)
    dma = pltpu.SemaphoreType.DMA
    return pl.pallas_call(
        functools.partial(exchange, n),
        out_shape=(
            jax.ShapeDtypeStruct((tokens, features), kind),
            jax.ShapeDtypeStruct((2, blocks * part, HEAD_DIM), kind),
        ),
        in_specs=[smem] * 3 + [anywhere] * 3,
        out_specs=(vmem, anywhere),
        scratch_shapes=[
            pltpu.VMEM((tokens, features), kind),
            pltpu.VMEM((2, tokens, features), kind),
            pltpu.VMEM((2, BACK * BLOCK, features), kind),
            pltpu.VMEM((2, 2 * BLOCK, features), kind),
            pltpu.VMEM((tokens, (BACK + here) * BLOCK), jnp.float32),
            dma((CHUNKS * 18,)),
            dma((BACK + 2, CHUNKS)),
            dma((2,)),
            dma((here,)),
            dma((3,)),
        ],
        compiler_params=pltpu.CompilerParams(
            collective_id=0, has_side_effects=True, vmem_limit_bytes=60 * 1024 * 1024
        ),
    )(block_counts, last_tokens, pack_order, queries, keys, values)


def local(n, queries, keys, values, block_counts, last_tokens, pack_order, decode_slot):
    tokens, features = queries.shape
    here = tokens // BLOCK
    splits = n // HEADS
    part = BLOCK // splits
    blocks = here * n
    kind = queries.dtype
    smem = pl.BlockSpec(memory_space=pltpu.SMEM)
    anywhere = pl.BlockSpec(memory_space=pl.ANY)
    dma = pltpu.SemaphoreType.DMA
    planes = n // PLANE
    if splits == 1 and here == 2 and planes > 1:
        attended, landed = pl.pallas_call(
            functools.partial(handoff, n),
            out_shape=(
                jax.ShapeDtypeStruct((tokens, features), kind),
                jax.ShapeDtypeStruct((2, blocks * part, HEAD_DIM), kind),
            ),
            in_specs=[smem] * 3 + [anywhere] * 3,
            out_specs=(anywhere, anywhere),
            scratch_shapes=[
                pltpu.VMEM((tokens, features), kind),
                pltpu.VMEM((2, tokens, features), kind),
                pltpu.VMEM((planes, 2, (BACK + PLANE * here) * BLOCK, HEAD_DIM), kind),
                pltpu.VMEM((planes, PLANE * tokens, HEAD_DIM), kind),
                pltpu.VMEM((planes, PLANE, tokens, HEAD_DIM), kind),
                pltpu.VMEM((PLANE, tokens, (BACK + here) * BLOCK), jnp.float32),
                dma((3,)),
                dma((3,)),
                dma((1,)),
                dma((PLANE - 1, planes)),
                dma((1,)),
                dma((PLANE - 1, planes)),
                dma((1,)),
                dma((planes, PLANE)),
                dma((3, planes)),
                dma((1,)),
                dma((1,)),
                dma((1,)),
            ],
            compiler_params=pltpu.CompilerParams(
                collective_id=0, has_side_effects=True, vmem_limit_bytes=60 * 1024 * 1024
            ),
        )(block_counts, last_tokens, pack_order, queries, keys, values)
    else:
        attended, landed = wide_exchange(
            n, queries, keys, values, block_counts, last_tokens, pack_order
        )
    cache = jax.ShapeDtypeStruct((1, blocks, part, HEAD_DIM), kind)
    attended, cache_keys, cache_values = pl.pallas_call(
        reorder,
        out_shape=(jax.ShapeDtypeStruct((tokens, features), kind), cache, cache),
        in_specs=[smem] * 3 + [anywhere] * 2,
        out_specs=(anywhere,) * 3,
        scratch_shapes=[
            pltpu.VMEM((2, blocks, part, HEAD_DIM), kind),
            pltpu.VMEM((tokens, features), kind),
            pltpu.SMEM(block_counts.shape, jnp.int32),
            pltpu.SMEM(block_counts.shape, jnp.int32),
            dma((3,)),
            dma((3,)),
        ],
    )(block_counts, pack_order, decode_slot, landed, attended)
    return attended, cache_keys, cache_values


def solution(mesh):
    rows = P(("groups", "seq"), None)
    small = P("groups")
    cache = P(("groups", "seq"), None, None, None)
    return jax.shard_map(
        functools.partial(local, mesh.shape["seq"]),
        mesh=mesh,
        in_specs=(rows, rows, rows, small, small, small, small),
        out_specs=(rows, cache, cache),
        check_vma=False,
    )
```

```python
import functools
import math

import jax
import jax.numpy as jnp
from jax import lax
from jax.experimental import pallas as pl
from jax.experimental.pallas import tpu as pltpu
from jax.sharding import PartitionSpec as P

HEADS = 16
HEAD_DIM = 128
BLOCK = 128
MAXB = 6
BACK = MAXB - 1
HIDDEN = -1e30
PLANE = 4
CHUNKS = 4
RELAY = BACK
ROUND = 2


def window_tables(counts_ref, tails_ref, order_ref, first, width):
    pairs = counts_ref.shape[0]
    prompts = order_ref.shape[0]

    def place(i, carry):
        start, docs, valids = carry
        prompt = order_ref[i]
        counted = counts_ref[lax.rem(prompt, pairs)]
        size = jnp.where(prompt < pairs, counted, 1)
        tail = tails_ref[prompt]
        end = start + size
        new_docs, new_valids = [], []
        for w in range(width):
            b = first + w
            inside = (start <= b) & (b < end)
            new_docs.append(jnp.where(inside, i, docs[w]))
            new_valids.append(
                jnp.where(inside, jnp.where(b + 1 == end, tail, BLOCK), valids[w])
            )
        return end, tuple(new_docs), tuple(new_valids)

    none = jnp.int32(-1)
    zero = jnp.int32(0)
    _, docs, valids = lax.fori_loop(
        0, prompts, place, (zero, (none,) * width, (zero,) * width)
    )
    return docs, valids


def exchange(
    n,
    counts_ref,
    tails_ref,
    order_ref,
    q_hbm,
    k_hbm,
    v_hbm,
    out_ref,
    landed_ref,
    q_ref,
    own,
    halo,
    relay,
    bias,
    halo_send,
    halo_recv,
    cache_sem,
    own_sem,
    load_sem,
):
    me = lax.axis_index("seq")
    role = lax.rem(me, PLANE)
    plane = me // PLANE
    planes = n // PLANE
    tokens, features = q_ref.shape
    here = tokens // BLOCK
    splits = n // HEADS
    part = BLOCK // splits
    wide = features // CHUNKS

    loads = [
        pltpu.make_async_copy(src, dst, load_sem.at[i])
        for i, (src, dst) in enumerate(
            ((k_hbm, own.at[0]), (v_hbm, own.at[1]), (q_hbm, q_ref))
        )
    ]
    for copy in loads:
        copy.start()

    barrier = pltpu.get_barrier_semaphore()

    def greet(r, carry):
        pl.semaphore_signal(
            barrier,
            inc=1,
            device_id={"seq": lax.rem(me + r, n)},
            device_id_type=pl.DeviceIdType.MESH,
        )
        return carry

    lax.fori_loop(1, n, greet, 0)
    loads[0].wait()
    loads[1].wait()
    pl.semaphore_wait(barrier, n - 1)

    pending = []

    def spot(block, c):
        return (
            slice(None),
            pl.ds(block * BLOCK, BLOCK),
            pl.ds(c * wide, wide),
        )

    def mine(block):
        return lambda c: own.at[spot(block, c)]

    def held(slot):
        if slot >= RELAY:
            return lambda c: relay.at[spot(slot - RELAY, c)]
        return lambda c: halo.at[spot(slot, c)]

    def start(cond, c, moves):
        copies = []
        for src, target, slot in moves:
            copy = pltpu.make_async_remote_copy(
                src_ref=src(c),
                dst_ref=held(slot)(c),
                send_sem=halo_send.at[len(pending)],
                recv_sem=halo_recv.at[slot, c],
                device_id={"seq": lax.rem(target + n, n)},
                device_id_type=pl.DeviceIdType.MESH,
            )
            pending.append((cond, copy))
            copies.append(copy)

        @pl.when(cond)
        def _():
            for copy in copies:
                copy.start()

    def await_slots(cond, c, slots):
        @pl.when(cond)
        def _():
            for slot in slots:
                ref = held(slot)(c)
                pltpu.make_async_copy(ref, ref, halo_recv.at[slot, c]).wait()

    more = plane < planes - 1
    late = plane > 0
    for c in range(CHUNKS):
        start((role == 3) & more, c, [(mine(0), me + 3, RELAY), (mine(1), me + 3, 0)])
        if c < ROUND:
            moves = [(mine(1), me - 2, RELAY + 1), (mine(0), me - 2, RELAY)]
        else:
            moves = [(mine(1), me + 2, 2), (mine(0), me + 2, 1)]
        start((role == 2) & more, c, moves)
        start((role == 1) & more, c, [(mine(1), me + 3, 0)])
        start(role == 1, c, [(mine(0), me + 1, 3), (mine(1), me + 1, 4)])
        start(role == 0, c, [(mine(1), me + 2, 2), (mine(0), me + 2, 1)])
        start(
            (role == 0) | (role == 2),
            c,
            [(mine(0), me + 1, 3), (mine(1), me + 1, 4)],
        )

    def piece(owner, block):
        head = owner // splits
        cols = pl.ds(pl.multiple_of(head * HEAD_DIM, HEAD_DIM), HEAD_DIM)
        if splits == 1:
            return own.at[:, :, cols]
        offset = pl.multiple_of(block * BLOCK + lax.rem(owner, splits) * part, part)
        return own.at[:, pl.ds(offset, part), cols]

    def place(block):
        if splits == 1:
            return landed_ref.at[:, pl.ds(pl.multiple_of(me * tokens, tokens), tokens)]
        return landed_ref.at[
            :, pl.ds(pl.multiple_of((me * here + block) * part, part), part)
        ]

    pieces = 1 if splits == 1 else here

    def give(s, carry):
        sign = 1 - 2 * lax.rem(s, 2)
        target = lax.rem(me + n // 2 + sign * ((s + 1) // 2), n)
        for block in range(pieces):
            pltpu.make_async_remote_copy(
                src_ref=piece(target, block),
                dst_ref=place(block),
                send_sem=cache_sem.at[0],
                recv_sem=cache_sem.at[1],
                device_id={"seq": target},
                device_id_type=pl.DeviceIdType.MESH,
            ).start()
        return carry

    cuts = [(n - 1) * i // CHUNKS for i in range(CHUNKS + 1)]

    docs, valids = window_tables(
        counts_ref, tails_ref, order_ref, me * here - BACK, BACK + here
    )
    row = lax.broadcasted_iota(jnp.int32, (BLOCK, BLOCK), 0)
    col = lax.broadcasted_iota(jnp.int32, (BLOCK, BLOCK), 1)
    for b in range(here):
        for w in range(BACK + here):
            if w > BACK + b:
                shade = jnp.full((BLOCK, BLOCK), HIDDEN, jnp.float32)
            else:
                limit = jnp.where(docs[w] == docs[BACK + b], valids[w], 0)
                seen = col < limit
                if w == BACK + b:
                    seen = seen & (col <= row)
                shade = jnp.where(seen, 0.0, HIDDEN)
            bias[b * BLOCK : (b + 1) * BLOCK, w * BLOCK : (w + 1) * BLOCK] = shade
    column = lax.broadcasted_iota(jnp.int32, (BLOCK, HEAD_DIM), 0)
    real = jnp.concatenate(
        [column < valids[BACK + b] for b in range(here)], axis=0
    )

    empty = jnp.zeros((BLOCK, features), halo.dtype)
    for slot, reach in ((0, 3), (1, 2), (2, 2), (3, 1), (4, 1)):

        @pl.when(me < reach)
        def _():
            for kv in range(2):
                halo[kv, slot * BLOCK : (slot + 1) * BLOCK, :] = empty

    loads[2].wait()

    factor = HEAD_DIM ** (-0.5) * math.log2(math.e)
    prior = BACK * BLOCK
    nt = (((1,), (1,)), ((), ()))

    def one_head(h, carry):
        cols = pl.ds(pl.multiple_of(h * HEAD_DIM, HEAD_DIM), HEAD_DIM)
        q = q_ref[:, cols]
        s1 = lax.dot_general(q, halo[0, :, cols], nt, preferred_element_type=jnp.float32)
        s2 = lax.dot_general(q, own[0, :, cols], nt, preferred_element_type=jnp.float32)
        s1 = s1 + bias[:, :prior]
        s2 = s2 + bias[:, prior:]
        peak = jnp.maximum(
            jnp.max(s1, axis=1, keepdims=True), jnp.max(s2, axis=1, keepdims=True)
        )
        w1 = jnp.exp2((s1 - peak) * factor)
        w2 = jnp.exp2((s2 - peak) * factor)
        total = jnp.sum(w1, axis=1, keepdims=True) + jnp.sum(w2, axis=1, keepdims=True)
        mixed = jnp.dot(
            w1.astype(jnp.bfloat16), halo[1, :, cols], preferred_element_type=jnp.float32
        ) + jnp.dot(
            w2.astype(jnp.bfloat16), own[1, :, cols], preferred_element_type=jnp.float32
        )
        out_ref[:, cols] = jnp.where(real, mixed / total, 0.0).astype(out_ref.dtype)
        return carry

    for c in range(CHUNKS):
        lax.fori_loop(cuts[c], cuts[c + 1], give, 0)
        if c < ROUND:
            await_slots((role == 0) & more, c, [RELAY, RELAY + 1])
            start(
                (role == 0) & more,
                c,
                [(held(RELAY + 1), me + PLANE, 2), (held(RELAY), me + PLANE, 1)],
            )
        await_slots((role == 2) & late, c, [RELAY, 0])
        start(
            (role == 2) & late, c, [(held(RELAY), me - 2 + n, 3), (held(0), me - 2 + n, 4)]
        )
        await_slots((role == 0) & late, c, [2, 3, 4])
        await_slots(role == 2, c, [2, 3, 4])
        start(
            (role == 2) | ((role == 0) & late),
            c,
            [(held(2), me + 1, 0), (held(3), me + 1, 1), (held(4), me + 1, 2)],
        )
        await_slots((role == 0) & late, c, [0, 1])
        await_slots(role == 1, c, [3, 4])
        await_slots((role == 1) & late, c, [0, 1, 2])
        await_slots(role == 2, c, [1])
        await_slots(role == 3, c, [0, 1, 2, 3, 4])
        each = HEADS // CHUNKS
        lax.fori_loop(c * each, (c + 1) * each, one_head, 0)

    copies = [
        pltpu.make_async_copy(piece(me, block), place(block), own_sem.at[block])
        for block in range(pieces)
    ]
    for copy in copies:
        copy.start()

    for cond, copy in pending:

        @pl.when(cond)
        def _():
            copy.wait_send()

    for copy in copies:
        copy.wait()
    others = landed_ref.shape[1] // n * (n - 1)
    ref = landed_ref.at[:, pl.ds(0, others)]
    pltpu.make_async_copy(ref, ref, cache_sem.at[0]).wait()
    pltpu.make_async_copy(ref, ref, cache_sem.at[1]).wait()


def reorder(
    counts_ref,
    order_ref,
    slot_ref,
    landed_ref,
    mixed_ref,
    attended_ref,
    keys_ref,
    values_ref,
    staged,
    passed,
    who,
    base,
    in_sem,
    out_sem,
):
    enter = pltpu.make_async_copy(mixed_ref, passed, in_sem.at[2])
    enter.start()
    pairs = counts_ref.shape[0]
    prompts = order_ref.shape[0]
    blocks, part = staged.shape[1:3]

    def invert(p, carry):
        who[slot_ref[p]] = p
        return carry

    lax.fori_loop(0, pairs, invert, 0)

    def lay(s, first):
        p = who[s]
        base[p] = first
        return first + counts_ref[p] + 1

    lax.fori_loop(0, pairs, lay, jnp.int32(0))

    def fetch(i, first):
        prompt = order_ref[i]
        pair = lax.rem(prompt, pairs)
        null = prompt >= pairs
        counted = counts_ref[pair]
        size = jnp.where(null, 1, counted)
        target = base[pair] + jnp.where(null, counted, 0)

        def one(w, carry):
            for kv in range(2):
                pltpu.make_async_copy(
                    landed_ref.at[kv, pl.ds((first + w) * part, part)],
                    staged.at[kv, target + w],
                    in_sem.at[kv],
                ).start()
            return carry

        lax.fori_loop(0, size, one, 0)
        return first + size

    lax.fori_loop(0, prompts, fetch, jnp.int32(0))
    enter.wait()
    outs = [pltpu.make_async_copy(passed, attended_ref, out_sem.at[2])]
    outs[0].start()
    for kv, ref in enumerate((keys_ref, values_ref)):
        pltpu.make_async_copy(staged.at[kv], staged.at[kv], in_sem.at[kv]).wait()
        copy = pltpu.make_async_copy(staged.at[kv], ref.at[0], out_sem.at[kv])
        copy.start()
        outs.append(copy)
    for copy in outs:
        copy.wait()


def handoff(
    n,
    counts_ref,
    tails_ref,
    order_ref,
    q_hbm,
    k_hbm,
    v_hbm,
    out_ref,
    landed_ref,
    q_ref,
    own,
    kv,
    qs,
    mixed_ref,
    bias,
    lower_q,
    lower_bias,
    part_out,
    part_in,
    size_out,
    size_in,
    load_sem,
    local_sem,
    kv_send,
    kv_recv,
    q_send,
    q_recv,
    halo_send,
    halo_recv,
    land_send,
    land_recv,
    out_send,
    out_recv,
    down_send,
    down_recv,
    up_send,
    up_recv,
):
    me = lax.axis_index("seq")
    role = lax.rem(me, PLANE)
    plane = me // PLANE
    planes = n // PLANE
    tokens, features = q_ref.shape
    here = tokens // BLOCK
    width = PLANE * here
    skip = width - BACK
    reach = BACK * BLOCK
    peers = (role + 1 - 2 * lax.rem(role, 2), lax.rem(role + 2, PLANE), PLANE - 1 - role)
    more = plane < planes - 1
    late = plane > 0
    base = plane * PLANE
    last = planes - 1
    orders = []
    for p in range(planes):
        above = list(range(last, p, -1))
        helping = [j for j in range(p + 1) if j + p < last and 2 * p >= planes - 2]
        rest = [j for j in range(p, -1, -1) if j not in helping]
        if p == last:
            above, helping, rest = [last - 1], list(range(last - 1)), [last]
        orders.append(above + helping + rest)
    def one_if(i, value):
        return (i + planes - value) // planes - (i + planes - value - 1) // planes

    picks = [
        sum(orders[p][t] * one_if(plane, p) for p in range(planes)) for t in range(planes)
    ]

    def turn(t):
        return sum(picks[other] * one_if(t, other) for other in range(planes))

    def hold(j):
        return ((plane == last) & (j < plane - 1)) | ((plane == 0) & (j < planes // 2))

    def back(j, p):
        return (j <= p) & (j + p < planes - 1) & (2 * p >= planes - 2)

    helpable = sorted({j for p in range(last) for j in range(p + 1) if j + p < last and 2 * p >= planes - 2})

    def helps(j):
        return more & back(j, plane)

    def helped(j):
        return late & back(j, plane - 1)

    def each(body):
        def step(t, carry):
            body(turn(t))
            return carry

        lax.fori_loop(0, planes, step, 0)

    def rows(first, count):
        return pl.ds(pl.multiple_of(first * BLOCK, BLOCK), count * BLOCK)

    def cols(head):
        return pl.ds(pl.multiple_of(head * HEAD_DIM, HEAD_DIM), HEAD_DIM)

    def remote(src, dst, send, recv, target):
        pltpu.make_async_remote_copy(
            src_ref=src,
            dst_ref=dst,
            send_sem=send,
            recv_sem=recv,
            device_id={"seq": target},
            device_id_type=pl.DeviceIdType.MESH,
        ).start()

    def await_(ref, sem):
        pltpu.make_async_copy(ref, ref, sem).wait()

    mine = rows(BACK + role * here, here)
    place = rows(role * here, here)

    loads = [
        pltpu.make_async_copy(src, dst, load_sem.at[i])
        for i, (src, dst) in enumerate(
            ((k_hbm, own.at[0]), (v_hbm, own.at[1]), (q_hbm, q_ref))
        )
    ]
    for load in loads:
        load.start()
    for j in range(planes):
        here_cols = cols(j * PLANE + role)
        for i, src in enumerate((k_hbm, v_hbm)):
            pltpu.make_async_copy(
                src.at[:, here_cols], kv.at[j, i, mine], local_sem.at[0]
            ).start()
    for j in range(planes):
        here_cols = cols(j * PLANE + role)
        pltpu.make_async_copy(
            q_hbm.at[:, here_cols], qs.at[j, place], local_sem.at[1]
        ).start()

    barrier = pltpu.get_barrier_semaphore()
    for peer in peers:
        pl.semaphore_signal(
            barrier,
            inc=1,
            device_id={"seq": base + peer},
            device_id_type=pl.DeviceIdType.MESH,
        )
    for step in range(1, planes):
        pl.semaphore_signal(
            barrier,
            inc=1,
            device_id={"seq": lax.rem(me + step * PLANE, n)},
            device_id_type=pl.DeviceIdType.MESH,
        )

    for j in range(planes):

        @pl.when((plane == 0) | helped(j))
        def _():
            for i in range(2):
                kv[j, i, :reach, :] = jnp.zeros((reach, HEAD_DIM), kv.dtype)

    with jax.named_scope("enter"):
        for load in loads:
            load.wait()
        pl.semaphore_wait(barrier, PLANE - 1 + planes - 1)

    def share(j):
        for k in (1, 2, 0):
            remote(
                own.at[:, :, cols(j * PLANE + peers[k])],
                kv.at[j, :, mine],
                kv_send.at[0],
                kv_recv.at[k, j],
                base + peers[k],
            )

    def share_q(j):
        for k in (1, 2, 0):
            remote(
                q_ref.at[:, cols(j * PLANE + peers[k])],
                qs.at[j, place],
                q_send.at[0],
                q_recv.at[k, j],
                base + peers[k],
            )

    def when_helped(body, truth):
        def step(j):
            @pl.when(helped(j) if truth else jnp.logical_not(helped(j)))
            def _():
                body(j)

        return step

    def descend(body):
        def step(t, carry):
            body(last - t)
            return carry

        lax.fori_loop(0, planes, step, 0)

    each(when_helped(share_q, True))
    each(share)
    descend(when_helped(share_q, False))

    def forward(j, rho):
        first = BACK + rho * here
        low = rho * here < skip
        high = rho * here + here > skip
        up = more & jnp.logical_not(helps(j))

        @pl.when(up & jnp.logical_not(low))
        def _():
            remote(
                kv.at[j, :, rows(first, here)],
                kv.at[j, :, rows(jnp.maximum(rho * here - skip, 0), here)],
                halo_send.at[j],
                halo_recv.at[j, rho],
                me + PLANE,
            )

        @pl.when(up & low & high)
        def _():
            remote(
                kv.at[j, :, rows(BACK + skip, BACK % here)],
                kv.at[j, :, rows(0, BACK % here)],
                halo_send.at[j],
                halo_recv.at[j, rho],
                me + PLANE,
            )

        @pl.when(late & (j > plane) & low & high)
        def _():
            remote(
                kv.at[j, :, rows(first, skip % here)],
                landed_ref.at[:, rows(plane * width + rho * here, skip % here)],
                land_send.at[1, j],
                land_recv.at[0],
                j * PLANE + role,
            )

        @pl.when(late & (j > plane) & jnp.logical_not(high))
        def _():
            remote(
                kv.at[j, :, rows(first, here)],
                landed_ref.at[:, rows(plane * width + rho * here, here)],
                land_send.at[1, j],
                land_recv.at[0],
                j * PLANE + role,
            )

        @pl.when(j < plane)
        def _():
            remote(
                kv.at[j, :, rows(first, here)],
                landed_ref.at[:, rows(plane * width + rho * here, here)],
                land_send.at[0, j],
                land_recv.at[0],
                j * PLANE + role,
            )

    def start_mine(j):
        @pl.when(jnp.logical_not(hold(j)))
        def _():
            forward(j, role)

    def take(k, j):
        await_(kv.at[j, :, rows(BACK + peers[k] * here, here)], kv_recv.at[k, j])

    def start_core(truth):
        def body(j):
            @pl.when(helped(j) if truth else jnp.logical_not(helped(j)))
            def _():
                take(0, j)

                @pl.when(jnp.logical_not(hold(j)))
                def _():
                    forward(j, peers[0])

        return body

    await_(kv.at[:, :, mine], local_sem.at[0])
    each(start_mine)

    with jax.named_scope("take_core"):
        each(start_core(False))

    with jax.named_scope("tables"):
        docs, valids = window_tables(
            counts_ref, tails_ref, order_ref, plane * width - BACK, BACK + width + BACK
        )
        row = lax.broadcasted_iota(jnp.int32, (BLOCK, BLOCK), 0)
        col = lax.broadcasted_iota(jnp.int32, (BLOCK, BLOCK), 1)
        hidden = jnp.full((BLOCK, BLOCK), HIDDEN, jnp.float32)

        def shade(source, target):
            limit = jnp.where(docs[source] == docs[target], valids[source], 0)
            seen = col < limit
            if source == target:
                seen = seen & (col <= row)
            return jnp.where(seen, 0.0, HIDDEN)

        for i in range(PLANE):
            for b in range(here):
                target = BACK + i * here + b
                for w in range(BACK + here):
                    source = i * here + w
                    spot = (slice(b * BLOCK, (b + 1) * BLOCK), slice(w * BLOCK, (w + 1) * BLOCK))
                    full = hidden if source > target else shade(source, target)
                    bias[(0, i) + spot] = full
                    bias[(1, i) + spot] = hidden if source < BACK else full
        for g in range(BACK):
            for c in range(BACK):
                lower_bias[g * BLOCK : (g + 1) * BLOCK, c * BLOCK : (c + 1) * BLOCK] = shade(
                    BACK + skip + c, BACK + width + g
                )
        column = lax.broadcasted_iota(jnp.int32, (BLOCK, HEAD_DIM), 0)

    def await_q(j):
        for k in range(PLANE - 1):
            await_(qs.at[j, rows(peers[k] * here, here)], q_recv.at[k, j])

    await_(qs.at[:, place], local_sem.at[1])

    def lower(j):
        await_q(j)
        remote(
            qs.at[j, pl.ds(0, reach)],
            lower_q.at[j],
            down_send.at[j],
            down_recv.at[j],
            me - PLANE,
        )

    with jax.named_scope("lower_q"):
        for h in helpable:

            @pl.when(helped(h))
            def _():
                lower(h)

    each(start_core(True))

    def await_halo(j):
        for rho in range(PLANE):
            count = min(here, (rho + 1) * here - skip)
            if count > 0:
                await_(
                    kv.at[j, :, rows(max(rho * here - skip, 0), count)],
                    halo_recv.at[j, rho],
                )

    below = rows(jnp.maximum(plane * width - BACK, 0), BACK)

    def relay(j):
        @pl.when(late & (j > plane))
        def _():
            await_halo(j)
            remote(
                kv.at[j, :, rows(0, BACK)],
                landed_ref.at[:, below],
                land_send.at[2, j],
                land_recv.at[0],
                j * PLANE + role,
            )

    factor = HEAD_DIM ** (-0.5) * math.log2(math.e)
    nt = (((1,), (1,)), ((), ()))
    span = (BACK + here) * BLOCK

    def soften(q, k, v, mask):
        s = lax.dot_general(q, k, nt, preferred_element_type=jnp.float32) + mask
        peak = jnp.max(s, axis=1, keepdims=True)
        w = jnp.exp2((s - peak) * factor)
        total = jnp.sum(w, axis=1, keepdims=True)
        mixed = jnp.dot(w.astype(jnp.bfloat16), v, preferred_element_type=jnp.float32)
        return mixed, peak * factor, total

    def help_out(j):
        await_(lower_q.at[j], down_recv.at[j])
        for first in range(0, BACK, here):
            count = min(here, BACK - first)
            lines = slice(first * BLOCK, (first + count) * BLOCK)
            window = pl.ds((BACK + skip + first) * BLOCK, (BACK - first) * BLOCK)
            mixed, peak, total = soften(
                lower_q[j, lines, :],
                kv[j, 0, window, :],
                kv[j, 1, window, :],
                lower_bias[lines, first * BLOCK :],
            )
            part_out[j, lines, :] = (mixed / total).astype(part_out.dtype)
            size = jnp.broadcast_to(peak + jnp.log2(total), (count * BLOCK, BLOCK))
            for b in range(count):
                turned = size[b * BLOCK : (b + 1) * BLOCK].T
                size_out[j, first + b] = turned[:8]

    def send_up(j):
        remote(part_out.at[j], part_in.at[j], up_send.at[0, j], up_recv.at[0, j], me + PLANE)
        remote(size_out.at[j], size_in.at[j], up_send.at[1, j], up_recv.at[1, j], me + PLANE)

    def release(j):
        @pl.when(hold(j))
        def _():
            forward(j, role)
            forward(j, peers[0])

    def far(t, carry):
        j = turn(t)
        with jax.named_scope("take_far"):
            for k in (1, 2):
                take(k, j)
                forward(j, peers[k])

        @pl.when(t == min(1, last))
        def _():
            each(release)

        for h in helpable:

            @pl.when(helps(h) & (j == h))
            def _():
                with jax.named_scope("help_out"):
                    help_out(h)

        for h in helpable:

            @pl.when(helps(h) & (j == h))
            def _():
                send_up(h)

        return carry

    lax.fori_loop(0, planes, far, 0)

    def climb(j, carry):
        @pl.when((plane == 0) & (j > 0))
        def _():
            remote(
                kv.at[j, :, rows(BACK, skip)],
                landed_ref.at[:, rows(0, skip)],
                land_send.at[1, j],
                land_recv.at[0],
                j * PLANE + role,
            )

        return carry

    lax.fori_loop(0, planes, climb, 0)

    with jax.named_scope("relay"):
        descend(relay)

    settle = pltpu.make_async_copy(
        kv.at[plane, :, rows(BACK, width)],
        landed_ref.at[:, rows(plane * width, width)],
        load_sem.at[0],
    )
    settle.start()

    def attend(j, i, variant):
        window = pl.ds(i * tokens, span)
        return soften(
            qs[j, pl.ds(i * tokens, tokens), :],
            kv[j, 0, window, :],
            kv[j, 1, window, :],
            bias[variant, i],
        )

    def finish(j, i, mixed, total):
        real = jnp.concatenate(
            [column < valids[BACK + i * here + b] for b in range(here)], axis=0
        )
        mixed_ref[j, i] = jnp.where(real, mixed / total, 0.0).astype(mixed_ref.dtype)

    def simple(j, i):
        mixed, _, total = attend(j, i, 0)
        finish(j, i, mixed, total)

    def give(j, i):
        target = out_ref.at[:, cols(j * PLANE + role)]

        @pl.when(role == i)
        def _():
            pltpu.make_async_copy(mixed_ref.at[j, i], target, local_sem.at[2]).start()

        @pl.when(role != i)
        def _():
            remote(mixed_ref.at[j, i], target, out_send.at[0], out_recv.at[0], base + i)

    top = PLANE - 1

    def own_blocks(t, carry):
        j = last - t
        with jax.named_scope("wait_q"):

            @pl.when(jnp.logical_not(helped(j)))
            def _():
                await_q(j)

        with jax.named_scope("top"):
            simple(j, top)

            @pl.when(t > 0)
            def _():
                give(jnp.minimum(j + 1, last), top)

        return carry

    lax.fori_loop(0, planes, own_blocks, 0)

    def reach_back(j):
        with jax.named_scope("wait_halo"):

            @pl.when(late & (j <= plane))
            def _():
                await_halo(j)

        with jax.named_scope("units"):
            for i in range(top - 1, -1, -1):
                simple(j, i)
                if i == top - 1:

                    @pl.when(j == last)
                    def _():
                        give(0, top)

                    @pl.when(j < last)
                    def _():
                        give(jnp.minimum(j + 1, last), 0)

                else:
                    give(j, i + 1)

    descend(when_helped(reach_back, False))

    settled = pltpu.make_async_copy(
        kv.at[plane, :, rows(0, BACK)], landed_ref.at[:, below], load_sem.at[1]
    )

    @pl.when(late)
    def _():
        settled.start()

    for j in range(planes):
        first = jnp.logical_not(helped(j))

        @pl.when(first & helped(j - 1) if j else first)
        def _():
            give(j, 0)

    def merge(j):
        with jax.named_scope("wait_part"):
            await_(part_in.at[j], up_recv.at[0, j])
            await_(size_in.at[j], up_recv.at[1, j])
        with jax.named_scope("merge"):
            for i in range(top - 1, -1, -1):
                mixed, peak, total = attend(j, i, 1)
                mixed = [mixed[b * BLOCK : (b + 1) * BLOCK] for b in range(here)]
                total = [
                    jnp.broadcast_to(total[b * BLOCK : (b + 1) * BLOCK], (BLOCK, BLOCK))
                    for b in range(here)
                ]
                for b in range(here):
                    g = i * here + b
                    if g < BACK:
                        size = jnp.broadcast_to(size_in[j, g, :1], (BLOCK, BLOCK)).T
                        mark = peak[b * BLOCK : (b + 1) * BLOCK]
                        high = jnp.maximum(mark, size)
                        mine_share = jnp.exp2(mark - high)
                        their_share = jnp.exp2(size - high)
                        theirs = part_in[j, g * BLOCK : (g + 1) * BLOCK, :]
                        mixed[b] = mixed[b] * mine_share + theirs.astype(jnp.float32) * their_share
                        total[b] = total[b] * mine_share + their_share
                finish(
                    j, i, jnp.concatenate(mixed, axis=0), jnp.concatenate(total, axis=0)
                )
                if i < top - 1:
                    give(j, i + 1)
        give(j, 0)

    for h in helpable:

        @pl.when(helped(h))
        def _():
            merge(h)

    with jax.named_scope("drain"):
        others = features // PLANE * (PLANE - 1)
        await_(own.at[:, :, pl.ds(0, others)], kv_send.at[0])
        await_(q_ref.at[:, pl.ds(0, others)], q_send.at[0])
        await_(q_ref.at[:, pl.ds(0, features // PLANE)], local_sem.at[2])

        def drain(j):
            @pl.when(more & jnp.logical_not(helps(j)))
            def _():
                await_(kv.at[j, :, rows(0, BACK)], halo_send.at[j])

            @pl.when(helps(j))
            def _():
                await_(part_out.at[j], up_send.at[0, j])
                await_(size_out.at[j], up_send.at[1, j])

            @pl.when(helped(j))
            def _():
                await_(lower_q.at[j], down_send.at[j])

            @pl.when(j < plane)
            def _():
                await_(kv.at[j, :, rows(BACK, width)], land_send.at[0, j])

            @pl.when(j > plane)
            def _():
                await_(kv.at[j, :, rows(BACK, skip)], land_send.at[1, j])

            @pl.when(late & (j > plane))
            def _():
                await_(kv.at[j, :, rows(0, BACK)], land_send.at[2, j])

        each(drain)
        settle.wait()
        await_(q_ref.at[:, pl.ds(0, others)], out_send.at[0])
        await_(q_ref.at[:, pl.ds(0, others)], out_recv.at[0])

    with jax.named_scope("land"):

        @pl.when(late)
        def _():
            settled.wait()
            await_(landed_ref.at[:, rows(0, (planes - 1) * width - BACK)], land_recv.at[0])

        @pl.when(plane == 0)
        def _():
            await_(landed_ref.at[:, rows(0, (planes - 1) * width)], land_recv.at[0])


def wide_exchange(n, queries, keys, values, block_counts, last_tokens, pack_order):
    tokens, features = queries.shape
    here = tokens // BLOCK
    part = BLOCK // (n // HEADS)
    blocks = here * n
    kind = queries.dtype
    smem = pl.BlockSpec(memory_space=pltpu.SMEM)
    vmem = pl.BlockSpec(memory_space=pltpu.VMEM)
    anywhere = pl.BlockSpec(memory_space=pl.ANY)
    dma = pltpu.SemaphoreType.DMA
    return pl.pallas_call(
        functools.partial(exchange, n),
        out_shape=(
            jax.ShapeDtypeStruct((tokens, features), kind),
            jax.ShapeDtypeStruct((2, blocks * part, HEAD_DIM), kind),
        ),
        in_specs=[smem] * 3 + [anywhere] * 3,
        out_specs=(vmem, anywhere),
        scratch_shapes=[
            pltpu.VMEM((tokens, features), kind),
            pltpu.VMEM((2, tokens, features), kind),
            pltpu.VMEM((2, BACK * BLOCK, features), kind),
            pltpu.VMEM((2, 2 * BLOCK, features), kind),
            pltpu.VMEM((tokens, (BACK + here) * BLOCK), jnp.float32),
            dma((CHUNKS * 18,)),
            dma((BACK + 2, CHUNKS)),
            dma((2,)),
            dma((here,)),
            dma((3,)),
        ],
        compiler_params=pltpu.CompilerParams(
            collective_id=0, has_side_effects=True, vmem_limit_bytes=60 * 1024 * 1024
        ),
    )(block_counts, last_tokens, pack_order, queries, keys, values)


def local(n, queries, keys, values, block_counts, last_tokens, pack_order, decode_slot):
    tokens, features = queries.shape
    here = tokens // BLOCK
    splits = n // HEADS
    part = BLOCK // splits
    blocks = here * n
    kind = queries.dtype
    smem = pl.BlockSpec(memory_space=pltpu.SMEM)
    anywhere = pl.BlockSpec(memory_space=pl.ANY)
    dma = pltpu.SemaphoreType.DMA
    planes = n // PLANE
    reach = BACK * BLOCK
    if splits == 1 and here == 2 and planes > 1:
        attended, landed = pl.pallas_call(
            functools.partial(handoff, n),
            out_shape=(
                jax.ShapeDtypeStruct((tokens, features), kind),
                jax.ShapeDtypeStruct((2, blocks * part, HEAD_DIM), kind),
            ),
            in_specs=[smem] * 3 + [anywhere] * 3,
            out_specs=(anywhere, anywhere),
            scratch_shapes=[
                pltpu.VMEM((tokens, features), kind),
                pltpu.VMEM((2, tokens, features), kind),
                pltpu.VMEM((planes, 2, (BACK + PLANE * here) * BLOCK, HEAD_DIM), kind),
                pltpu.VMEM((planes, PLANE * tokens, HEAD_DIM), kind),
                pltpu.VMEM((planes, PLANE, tokens, HEAD_DIM), kind),
                pltpu.VMEM((2, PLANE, tokens, (BACK + here) * BLOCK), jnp.float32),
                pltpu.VMEM((planes, reach, HEAD_DIM), kind),
                pltpu.VMEM((reach, reach), jnp.float32),
                pltpu.VMEM((planes, reach, HEAD_DIM), kind),
                pltpu.VMEM((planes, reach, HEAD_DIM), kind),
                pltpu.VMEM((planes, BACK, 8, BLOCK), jnp.float32),
                pltpu.VMEM((planes, BACK, 8, BLOCK), jnp.float32),
                dma((3,)),
                dma((3,)),
                dma((1,)),
                dma((PLANE - 1, planes)),
                dma((1,)),
                dma((PLANE - 1, planes)),
                dma((planes,)),
                dma((planes, PLANE)),
                dma((3, planes)),
                dma((1,)),
                dma((1,)),
                dma((1,)),
                dma((planes,)),
                dma((planes,)),
                dma((2, planes)),
                dma((2, planes)),
            ],
            compiler_params=pltpu.CompilerParams(
                collective_id=0, has_side_effects=True, vmem_limit_bytes=60 * 1024 * 1024
            ),
        )(block_counts, last_tokens, pack_order, queries, keys, values)
    else:
        attended, landed = wide_exchange(
            n, queries, keys, values, block_counts, last_tokens, pack_order
        )
    cache = jax.ShapeDtypeStruct((1, blocks, part, HEAD_DIM), kind)
    attended, cache_keys, cache_values = pl.pallas_call(
        reorder,
        out_shape=(jax.ShapeDtypeStruct((tokens, features), kind), cache, cache),
        in_specs=[smem] * 3 + [anywhere] * 2,
        out_specs=(anywhere,) * 3,
        scratch_shapes=[
            pltpu.VMEM((2, blocks, part, HEAD_DIM), kind),
            pltpu.VMEM((tokens, features), kind),
            pltpu.SMEM(block_counts.shape, jnp.int32),
            pltpu.SMEM(block_counts.shape, jnp.int32),
            dma((3,)),
            dma((3,)),
        ],
    )(block_counts, pack_order, decode_slot, landed, attended)
    return attended, cache_keys, cache_values


def solution(mesh):
    rows = P(("groups", "seq"), None)
    small = P("groups")
    cache = P(("groups", "seq"), None, None, None)
    return jax.shard_map(
        functools.partial(local, mesh.shape["seq"]),
        mesh=mesh,
        in_specs=(rows, rows, rows, small, small, small, small),
        out_specs=(rows, cache, cache),
        check_vma=False,
    )
```

```python
import functools
import math

import jax
import jax.numpy as jnp
from jax import lax
from jax.experimental import pallas as pl
from jax.experimental.pallas import tpu as pltpu
from jax.sharding import PartitionSpec as P

HEADS = 16
HEAD_DIM = 128
BLOCK = 128
MAXB = 6
BACK = MAXB - 1
HIDDEN = -1e30
PLANE = 4
CHUNKS = 4
RELAY = BACK
ROUND = 2


def window_tables(counts_ref, tails_ref, order_ref, first, width):
    pairs = counts_ref.shape[0]
    prompts = order_ref.shape[0]

    def place(i, carry):
        start, docs, valids = carry
        prompt = order_ref[i]
        counted = counts_ref[lax.rem(prompt, pairs)]
        size = jnp.where(prompt < pairs, counted, 1)
        tail = tails_ref[prompt]
        end = start + size
        new_docs, new_valids = [], []
        for w in range(width):
            b = first + w
            inside = (start <= b) & (b < end)
            new_docs.append(jnp.where(inside, i, docs[w]))
            new_valids.append(
                jnp.where(inside, jnp.where(b + 1 == end, tail, BLOCK), valids[w])
            )
        return end, tuple(new_docs), tuple(new_valids)

    none = jnp.int32(-1)
    zero = jnp.int32(0)
    _, docs, valids = lax.fori_loop(
        0, prompts, place, (zero, (none,) * width, (zero,) * width)
    )
    return docs, valids


def exchange(
    n,
    counts_ref,
    tails_ref,
    order_ref,
    q_hbm,
    k_hbm,
    v_hbm,
    out_ref,
    landed_ref,
    q_ref,
    own,
    halo,
    relay,
    bias,
    halo_send,
    halo_recv,
    cache_sem,
    own_sem,
    load_sem,
):
    me = lax.axis_index("seq")
    role = lax.rem(me, PLANE)
    plane = me // PLANE
    planes = n // PLANE
    tokens, features = q_ref.shape
    here = tokens // BLOCK
    splits = n // HEADS
    part = BLOCK // splits
    wide = features // CHUNKS

    loads = [
        pltpu.make_async_copy(src, dst, load_sem.at[i])
        for i, (src, dst) in enumerate(
            ((k_hbm, own.at[0]), (v_hbm, own.at[1]), (q_hbm, q_ref))
        )
    ]
    for copy in loads:
        copy.start()

    barrier = pltpu.get_barrier_semaphore()

    def greet(r, carry):
        pl.semaphore_signal(
            barrier,
            inc=1,
            device_id={"seq": lax.rem(me + r, n)},
            device_id_type=pl.DeviceIdType.MESH,
        )
        return carry

    lax.fori_loop(1, n, greet, 0)
    loads[0].wait()
    loads[1].wait()
    pl.semaphore_wait(barrier, n - 1)

    pending = []

    def spot(block, c):
        return (
            slice(None),
            pl.ds(block * BLOCK, BLOCK),
            pl.ds(c * wide, wide),
        )

    def mine(block):
        return lambda c: own.at[spot(block, c)]

    def held(slot):
        if slot >= RELAY:
            return lambda c: relay.at[spot(slot - RELAY, c)]
        return lambda c: halo.at[spot(slot, c)]

    def start(cond, c, moves):
        copies = []
        for src, target, slot in moves:
            copy = pltpu.make_async_remote_copy(
                src_ref=src(c),
                dst_ref=held(slot)(c),
                send_sem=halo_send.at[len(pending)],
                recv_sem=halo_recv.at[slot, c],
                device_id={"seq": lax.rem(target + n, n)},
                device_id_type=pl.DeviceIdType.MESH,
            )
            pending.append((cond, copy))
            copies.append(copy)

        @pl.when(cond)
        def _():
            for copy in copies:
                copy.start()

    def await_slots(cond, c, slots):
        @pl.when(cond)
        def _():
            for slot in slots:
                ref = held(slot)(c)
                pltpu.make_async_copy(ref, ref, halo_recv.at[slot, c]).wait()

    more = plane < planes - 1
    late = plane > 0
    for c in range(CHUNKS):
        start((role == 3) & more, c, [(mine(0), me + 3, RELAY), (mine(1), me + 3, 0)])
        if c < ROUND:
            moves = [(mine(1), me - 2, RELAY + 1), (mine(0), me - 2, RELAY)]
        else:
            moves = [(mine(1), me + 2, 2), (mine(0), me + 2, 1)]
        start((role == 2) & more, c, moves)
        start((role == 1) & more, c, [(mine(1), me + 3, 0)])
        start(role == 1, c, [(mine(0), me + 1, 3), (mine(1), me + 1, 4)])
        start(role == 0, c, [(mine(1), me + 2, 2), (mine(0), me + 2, 1)])
        start(
            (role == 0) | (role == 2),
            c,
            [(mine(0), me + 1, 3), (mine(1), me + 1, 4)],
        )

    def piece(owner, block):
        head = owner // splits
        cols = pl.ds(pl.multiple_of(head * HEAD_DIM, HEAD_DIM), HEAD_DIM)
        if splits == 1:
            return own.at[:, :, cols]
        offset = pl.multiple_of(block * BLOCK + lax.rem(owner, splits) * part, part)
        return own.at[:, pl.ds(offset, part), cols]

    def place(block):
        if splits == 1:
            return landed_ref.at[:, pl.ds(pl.multiple_of(me * tokens, tokens), tokens)]
        return landed_ref.at[
            :, pl.ds(pl.multiple_of((me * here + block) * part, part), part)
        ]

    pieces = 1 if splits == 1 else here

    def give(s, carry):
        sign = 1 - 2 * lax.rem(s, 2)
        target = lax.rem(me + n // 2 + sign * ((s + 1) // 2), n)
        for block in range(pieces):
            pltpu.make_async_remote_copy(
                src_ref=piece(target, block),
                dst_ref=place(block),
                send_sem=cache_sem.at[0],
                recv_sem=cache_sem.at[1],
                device_id={"seq": target},
                device_id_type=pl.DeviceIdType.MESH,
            ).start()
        return carry

    cuts = [(n - 1) * i // CHUNKS for i in range(CHUNKS + 1)]

    docs, valids = window_tables(
        counts_ref, tails_ref, order_ref, me * here - BACK, BACK + here
    )
    row = lax.broadcasted_iota(jnp.int32, (BLOCK, BLOCK), 0)
    col = lax.broadcasted_iota(jnp.int32, (BLOCK, BLOCK), 1)
    for b in range(here):
        for w in range(BACK + here):
            if w > BACK + b:
                shade = jnp.full((BLOCK, BLOCK), HIDDEN, jnp.float32)
            else:
                limit = jnp.where(docs[w] == docs[BACK + b], valids[w], 0)
                seen = col < limit
                if w == BACK + b:
                    seen = seen & (col <= row)
                shade = jnp.where(seen, 0.0, HIDDEN)
            bias[b * BLOCK : (b + 1) * BLOCK, w * BLOCK : (w + 1) * BLOCK] = shade
    column = lax.broadcasted_iota(jnp.int32, (BLOCK, HEAD_DIM), 0)
    real = jnp.concatenate(
        [column < valids[BACK + b] for b in range(here)], axis=0
    )

    empty = jnp.zeros((BLOCK, features), halo.dtype)
    for slot, reach in ((0, 3), (1, 2), (2, 2), (3, 1), (4, 1)):

        @pl.when(me < reach)
        def _():
            for kv in range(2):
                halo[kv, slot * BLOCK : (slot + 1) * BLOCK, :] = empty

    loads[2].wait()

    factor = HEAD_DIM ** (-0.5) * math.log2(math.e)
    prior = BACK * BLOCK
    nt = (((1,), (1,)), ((), ()))

    def one_head(h, carry):
        cols = pl.ds(pl.multiple_of(h * HEAD_DIM, HEAD_DIM), HEAD_DIM)
        q = q_ref[:, cols]
        s1 = lax.dot_general(q, halo[0, :, cols], nt, preferred_element_type=jnp.float32)
        s2 = lax.dot_general(q, own[0, :, cols], nt, preferred_element_type=jnp.float32)
        s1 = s1 + bias[:, :prior]
        s2 = s2 + bias[:, prior:]
        peak = jnp.maximum(
            jnp.max(s1, axis=1, keepdims=True), jnp.max(s2, axis=1, keepdims=True)
        )
        w1 = jnp.exp2((s1 - peak) * factor)
        w2 = jnp.exp2((s2 - peak) * factor)
        total = jnp.sum(w1, axis=1, keepdims=True) + jnp.sum(w2, axis=1, keepdims=True)
        mixed = jnp.dot(
            w1.astype(jnp.bfloat16), halo[1, :, cols], preferred_element_type=jnp.float32
        ) + jnp.dot(
            w2.astype(jnp.bfloat16), own[1, :, cols], preferred_element_type=jnp.float32
        )
        out_ref[:, cols] = jnp.where(real, mixed / total, 0.0).astype(out_ref.dtype)
        return carry

    for c in range(CHUNKS):
        lax.fori_loop(cuts[c], cuts[c + 1], give, 0)
        if c < ROUND:
            await_slots((role == 0) & more, c, [RELAY, RELAY + 1])
            start(
                (role == 0) & more,
                c,
                [(held(RELAY + 1), me + PLANE, 2), (held(RELAY), me + PLANE, 1)],
            )
        await_slots((role == 2) & late, c, [RELAY, 0])
        start(
            (role == 2) & late, c, [(held(RELAY), me - 2 + n, 3), (held(0), me - 2 + n, 4)]
        )
        await_slots((role == 0) & late, c, [2, 3, 4])
        await_slots(role == 2, c, [2, 3, 4])
        start(
            (role == 2) | ((role == 0) & late),
            c,
            [(held(2), me + 1, 0), (held(3), me + 1, 1), (held(4), me + 1, 2)],
        )
        await_slots((role == 0) & late, c, [0, 1])
        await_slots(role == 1, c, [3, 4])
        await_slots((role == 1) & late, c, [0, 1, 2])
        await_slots(role == 2, c, [1])
        await_slots(role == 3, c, [0, 1, 2, 3, 4])
        each = HEADS // CHUNKS
        lax.fori_loop(c * each, (c + 1) * each, one_head, 0)

    copies = [
        pltpu.make_async_copy(piece(me, block), place(block), own_sem.at[block])
        for block in range(pieces)
    ]
    for copy in copies:
        copy.start()

    for cond, copy in pending:

        @pl.when(cond)
        def _():
            copy.wait_send()

    for copy in copies:
        copy.wait()
    others = landed_ref.shape[1] // n * (n - 1)
    ref = landed_ref.at[:, pl.ds(0, others)]
    pltpu.make_async_copy(ref, ref, cache_sem.at[0]).wait()
    pltpu.make_async_copy(ref, ref, cache_sem.at[1]).wait()


def decode_places(counts_ref, order_ref, slot_ref, who, base, put):
    pairs = counts_ref.shape[0]
    prompts = order_ref.shape[0]

    def invert(p, carry):
        who[slot_ref[p]] = p
        return carry

    lax.fori_loop(0, pairs, invert, 0)

    def lay(s, first):
        p = who[s]
        base[p] = first
        return first + counts_ref[p] + 1

    lax.fori_loop(0, pairs, lay, jnp.int32(0))

    def fetch(i, first):
        prompt = order_ref[i]
        pair = lax.rem(prompt, pairs)
        null = prompt >= pairs
        counted = counts_ref[pair]
        size = jnp.where(null, 1, counted)
        target = base[pair] + jnp.where(null, counted, 0)

        def one(w, carry):
            put(first + w, target + w)
            return carry

        lax.fori_loop(0, size, one, 0)
        return first + size

    lax.fori_loop(0, prompts, fetch, jnp.int32(0))


def reorder(
    counts_ref,
    order_ref,
    slot_ref,
    landed_ref,
    keys_ref,
    values_ref,
    staged,
    who,
    base,
    in_sem,
    out_sem,
):
    part = staged.shape[2]

    def put(source, target):
        for kv in range(2):
            pltpu.make_async_copy(
                landed_ref.at[kv, pl.ds(source * part, part)],
                staged.at[kv, target],
                in_sem.at[kv],
            ).start()

    decode_places(counts_ref, order_ref, slot_ref, who, base, put)
    outs = []
    for kv, ref in enumerate((keys_ref, values_ref)):
        pltpu.make_async_copy(staged.at[kv], staged.at[kv], in_sem.at[kv]).wait()
        copy = pltpu.make_async_copy(staged.at[kv], ref.at[0], out_sem.at[kv])
        copy.start()
        outs.append(copy)
    for copy in outs:
        copy.wait()


def publish(
    counts_ref,
    order_ref,
    slot_ref,
    landed_ref,
    mixed_ref,
    attended_ref,
    keys_ref,
    values_ref,
    who,
    base,
    out_sem,
):
    leave = pltpu.make_async_copy(mixed_ref, attended_ref, out_sem.at[2])
    leave.start()
    refs = (keys_ref, values_ref)
    part = keys_ref.shape[2]

    def put(source, target):
        for kv, ref in enumerate(refs):
            pltpu.make_async_copy(
                landed_ref.at[kv, pl.ds(source * part, part)], ref.at[0, target], out_sem.at[kv]
            ).start()

    decode_places(counts_ref, order_ref, slot_ref, who, base, put)
    leave.wait()
    for kv, ref in enumerate(refs):
        pltpu.make_async_copy(ref.at[0], ref.at[0], out_sem.at[kv]).wait()


def handoff(
    n,
    counts_ref,
    tails_ref,
    order_ref,
    q_hbm,
    k_hbm,
    v_hbm,
    out_ref,
    landed_ref,
    q_ref,
    own,
    kv,
    qs,
    mixed_ref,
    bias,
    lower_q,
    lower_bias,
    part_out,
    part_in,
    size_out,
    size_in,
    load_sem,
    local_sem,
    kv_send,
    kv_recv,
    q_send,
    q_recv,
    halo_send,
    halo_recv,
    land_send,
    land_recv,
    out_send,
    out_recv,
    down_send,
    down_recv,
    up_send,
    up_recv,
):
    me = lax.axis_index("seq")
    role = lax.rem(me, PLANE)
    plane = me // PLANE
    planes = n // PLANE
    tokens, features = q_ref.shape
    here = tokens // BLOCK
    width = PLANE * here
    skip = width - BACK
    reach = BACK * BLOCK
    peers = (role + 1 - 2 * lax.rem(role, 2), lax.rem(role + 2, PLANE), PLANE - 1 - role)
    more = plane < planes - 1
    late = plane > 0
    base = plane * PLANE
    last = planes - 1
    orders = []
    for p in range(planes):
        above = list(range(last, p, -1))
        helping = [j for j in range(p + 1) if j + p < last and 2 * p >= planes - 2]
        rest = [j for j in range(p, -1, -1) if j not in helping]
        if p == last:
            above, helping, rest = [last - 1], list(range(last - 1)), [last]
        orders.append(above + helping + rest)
    def one_if(i, value):
        return (i + planes - value) // planes - (i + planes - value - 1) // planes

    picks = [
        sum(orders[p][t] * one_if(plane, p) for p in range(planes)) for t in range(planes)
    ]

    def turn(t):
        return sum(picks[other] * one_if(t, other) for other in range(planes))

    def hold(j):
        return ((plane == last) & (j < plane - 1)) | ((plane == 0) & (j < planes // 2))

    def back(j, p):
        return (j <= p) & (j + p < planes - 1) & (2 * p >= planes - 2)

    helpable = sorted({j for p in range(last) for j in range(p + 1) if j + p < last and 2 * p >= planes - 2})

    def helps(j):
        return more & back(j, plane)

    def helped(j):
        return late & back(j, plane - 1)

    def each(body):
        def step(t, carry):
            body(turn(t))
            return carry

        lax.fori_loop(0, planes, step, 0)

    def rows(first, count):
        return pl.ds(pl.multiple_of(first * BLOCK, BLOCK), count * BLOCK)

    def cols(head):
        return pl.ds(pl.multiple_of(head * HEAD_DIM, HEAD_DIM), HEAD_DIM)

    def remote(src, dst, send, recv, target):
        pltpu.make_async_remote_copy(
            src_ref=src,
            dst_ref=dst,
            send_sem=send,
            recv_sem=recv,
            device_id={"seq": target},
            device_id_type=pl.DeviceIdType.MESH,
        ).start()

    def await_(ref, sem):
        pltpu.make_async_copy(ref, ref, sem).wait()

    mine = rows(BACK + role * here, here)
    place = rows(role * here, here)

    loads = [
        pltpu.make_async_copy(src, dst, load_sem.at[i])
        for i, (src, dst) in enumerate(
            ((k_hbm, own.at[0]), (v_hbm, own.at[1]), (q_hbm, q_ref))
        )
    ]
    barrier = pltpu.get_barrier_semaphore()
    for peer in peers:
        pl.semaphore_signal(
            barrier,
            inc=1,
            device_id={"seq": base + peer},
            device_id_type=pl.DeviceIdType.MESH,
        )
    for step in range(1, planes):
        pl.semaphore_signal(
            barrier,
            inc=1,
            device_id={"seq": lax.rem(me + step * PLANE, n)},
            device_id_type=pl.DeviceIdType.MESH,
        )
    for j in range(planes):
        here_cols = cols(j * PLANE + role)
        for i, src in enumerate((k_hbm, v_hbm)):
            pltpu.make_async_copy(
                src.at[:, here_cols], kv.at[j, i, mine], local_sem.at[0]
            ).start()
    for load in loads:
        load.start()
    for j in range(planes):
        here_cols = cols(j * PLANE + role)
        pltpu.make_async_copy(
            q_hbm.at[:, here_cols], qs.at[j, place], local_sem.at[1]
        ).start()

    for j in range(planes):

        @pl.when((plane == 0) | helped(j))
        def _():
            for i in range(2):
                kv[j, i, :reach, :] = jnp.zeros((reach, HEAD_DIM), kv.dtype)

    def share(j):
        for k in (1, 2, 0):
            remote(
                own.at[:, :, cols(j * PLANE + peers[k])],
                kv.at[j, :, mine],
                kv_send.at[0],
                kv_recv.at[k, j],
                base + peers[k],
            )

    def share_q(j):
        for k in (1, 2, 0):
            remote(
                q_ref.at[:, cols(j * PLANE + peers[k])],
                qs.at[j, place],
                q_send.at[0],
                q_recv.at[k, j],
                base + peers[k],
            )

    def when_helped(body, truth):
        def step(j):
            @pl.when(helped(j) if truth else jnp.logical_not(helped(j)))
            def _():
                body(j)

        return step

    def descend(body):
        def step(t, carry):
            body(last - t)
            return carry

        lax.fori_loop(0, planes, step, 0)

    def forward(j, rho):
        first = BACK + rho * here
        low = rho * here < skip
        high = rho * here + here > skip
        up = more & jnp.logical_not(helps(j))

        @pl.when(up & jnp.logical_not(low))
        def _():
            remote(
                kv.at[j, :, rows(first, here)],
                kv.at[j, :, rows(jnp.maximum(rho * here - skip, 0), here)],
                halo_send.at[j],
                halo_recv.at[j, rho],
                me + PLANE,
            )

        @pl.when(up & low & high)
        def _():
            remote(
                kv.at[j, :, rows(BACK + skip, BACK % here)],
                kv.at[j, :, rows(0, BACK % here)],
                halo_send.at[j],
                halo_recv.at[j, rho],
                me + PLANE,
            )

        @pl.when(late & (j > plane) & low & high)
        def _():
            remote(
                kv.at[j, :, rows(first, skip % here)],
                landed_ref.at[:, rows(plane * width + rho * here, skip % here)],
                land_send.at[1, j],
                land_recv.at[0],
                j * PLANE + role,
            )

        @pl.when(late & (j > plane) & jnp.logical_not(high))
        def _():
            remote(
                kv.at[j, :, rows(first, here)],
                landed_ref.at[:, rows(plane * width + rho * here, here)],
                land_send.at[1, j],
                land_recv.at[0],
                j * PLANE + role,
            )

        @pl.when(j < plane)
        def _():
            remote(
                kv.at[j, :, rows(first, here)],
                landed_ref.at[:, rows(plane * width + rho * here, here)],
                land_send.at[0, j],
                land_recv.at[0],
                j * PLANE + role,
            )

    def start_mine(j):
        @pl.when(jnp.logical_not(hold(j)))
        def _():
            forward(j, role)

    def take(k, j):
        await_(kv.at[j, :, rows(BACK + peers[k] * here, here)], kv_recv.at[k, j])

    def start_core(truth):
        def body(j):
            @pl.when(helped(j) if truth else jnp.logical_not(helped(j)))
            def _():
                take(0, j)

                @pl.when(jnp.logical_not(hold(j)))
                def _():
                    forward(j, peers[0])

        return body

    with jax.named_scope("enter_local"):
        await_(kv.at[:, :, mine], local_sem.at[0])
    with jax.named_scope("enter_barrier"):
        pl.semaphore_wait(barrier, PLANE - 1 + planes - 1)
    with jax.named_scope("start_mine"):
        each(start_mine)
    with jax.named_scope("enter_loads"):
        for load in loads:
            load.wait()
    with jax.named_scope("share"):
        each(when_helped(share_q, True))
        each(share)
        descend(when_helped(share_q, False))

    with jax.named_scope("take_core"):
        each(start_core(False))

    with jax.named_scope("tables"):
        docs, valids = window_tables(
            counts_ref, tails_ref, order_ref, plane * width - BACK, BACK + width + BACK
        )
        row = lax.broadcasted_iota(jnp.int32, (BLOCK, BLOCK), 0)
        col = lax.broadcasted_iota(jnp.int32, (BLOCK, BLOCK), 1)
        hidden = jnp.full((BLOCK, BLOCK), HIDDEN, jnp.float32)

        def shade(source, target):
            limit = jnp.where(docs[source] == docs[target], valids[source], 0)
            seen = col < limit
            if source == target:
                seen = seen & (col <= row)
            return jnp.where(seen, 0.0, HIDDEN)

        for i in range(PLANE):
            for b in range(here):
                target = BACK + i * here + b
                for w in range(BACK + here):
                    source = i * here + w
                    spot = (slice(b * BLOCK, (b + 1) * BLOCK), slice(w * BLOCK, (w + 1) * BLOCK))
                    full = hidden if source > target else shade(source, target)
                    bias[(0, i) + spot] = full
                    bias[(1, i) + spot] = hidden if source < BACK else full
        for g in range(BACK):
            for c in range(BACK):
                lower_bias[g * BLOCK : (g + 1) * BLOCK, c * BLOCK : (c + 1) * BLOCK] = shade(
                    BACK + skip + c, BACK + width + g
                )
        column = lax.broadcasted_iota(jnp.int32, (BLOCK, HEAD_DIM), 0)

    def await_q(j):
        for k in range(PLANE - 1):
            await_(qs.at[j, rows(peers[k] * here, here)], q_recv.at[k, j])

    await_(qs.at[:, place], local_sem.at[1])

    def lower(j):
        await_q(j)
        remote(
            qs.at[j, pl.ds(0, reach)],
            lower_q.at[j],
            down_send.at[j],
            down_recv.at[j],
            me - PLANE,
        )

    with jax.named_scope("lower_q"):
        for h in helpable:

            @pl.when(helped(h))
            def _():
                lower(h)

    each(start_core(True))

    def await_halo(j):
        for rho in range(PLANE):
            count = min(here, (rho + 1) * here - skip)
            if count > 0:
                await_(
                    kv.at[j, :, rows(max(rho * here - skip, 0), count)],
                    halo_recv.at[j, rho],
                )

    below = rows(jnp.maximum(plane * width - BACK, 0), BACK)

    def relay(j):
        @pl.when(late & (j > plane))
        def _():
            await_halo(j)
            remote(
                kv.at[j, :, rows(0, BACK)],
                landed_ref.at[:, below],
                land_send.at[2, j],
                land_recv.at[0],
                j * PLANE + role,
            )

    factor = HEAD_DIM ** (-0.5) * math.log2(math.e)
    nt = (((1,), (1,)), ((), ()))
    span = (BACK + here) * BLOCK

    def soften(q, k, v, mask):
        s = lax.dot_general(q, k, nt, preferred_element_type=jnp.float32) + mask
        peak = jnp.max(s, axis=1, keepdims=True)
        w = jnp.exp2((s - peak) * factor)
        total = jnp.sum(w, axis=1, keepdims=True)
        mixed = jnp.dot(w.astype(jnp.bfloat16), v, preferred_element_type=jnp.float32)
        return mixed, peak * factor, total

    def help_out(j):
        await_(lower_q.at[j], down_recv.at[j])
        for first in range(0, BACK, here):
            count = min(here, BACK - first)
            lines = slice(first * BLOCK, (first + count) * BLOCK)
            window = pl.ds((BACK + skip + first) * BLOCK, (BACK - first) * BLOCK)
            mixed, peak, total = soften(
                lower_q[j, lines, :],
                kv[j, 0, window, :],
                kv[j, 1, window, :],
                lower_bias[lines, first * BLOCK :],
            )
            part_out[j, lines, :] = (mixed / total).astype(part_out.dtype)
            size = jnp.broadcast_to(peak + jnp.log2(total), (count * BLOCK, BLOCK))
            for b in range(count):
                turned = size[b * BLOCK : (b + 1) * BLOCK].T
                size_out[j, first + b] = turned[:8]

    def send_up(j):
        remote(part_out.at[j], part_in.at[j], up_send.at[0, j], up_recv.at[0, j], me + PLANE)
        remote(size_out.at[j], size_in.at[j], up_send.at[1, j], up_recv.at[1, j], me + PLANE)

    def release(j):
        @pl.when(hold(j))
        def _():
            forward(j, role)
            forward(j, peers[0])

    def far(t, carry):
        j = turn(t)
        with jax.named_scope("take_far"):
            for k in (1, 2):
                take(k, j)
                forward(j, peers[k])

        @pl.when(t == min(1, last))
        def _():
            each(release)

        for h in helpable:

            @pl.when(helps(h) & (j == h))
            def _():
                with jax.named_scope("help_out"):
                    help_out(h)

        for h in helpable:

            @pl.when(helps(h) & (j == h))
            def _():
                send_up(h)

        return carry

    lax.fori_loop(0, planes, far, 0)

    def climb(j, carry):
        @pl.when((plane == 0) & (j > 0))
        def _():
            remote(
                kv.at[j, :, rows(BACK, skip)],
                landed_ref.at[:, rows(0, skip)],
                land_send.at[1, j],
                land_recv.at[0],
                j * PLANE + role,
            )

        return carry

    lax.fori_loop(0, planes, climb, 0)

    with jax.named_scope("relay"):
        descend(relay)

    settle = pltpu.make_async_copy(
        kv.at[plane, :, rows(BACK, width)],
        landed_ref.at[:, rows(plane * width, width)],
        load_sem.at[0],
    )
    settle.start()

    def attend(j, i, variant):
        window = pl.ds(i * tokens, span)
        return soften(
            qs[j, pl.ds(i * tokens, tokens), :],
            kv[j, 0, window, :],
            kv[j, 1, window, :],
            bias[variant, i],
        )

    def finish(j, i, mixed, total):
        real = jnp.concatenate(
            [column < valids[BACK + i * here + b] for b in range(here)], axis=0
        )
        mixed_ref[j, i] = jnp.where(real, mixed / total, 0.0).astype(mixed_ref.dtype)

    def simple(j, i):
        mixed, _, total = attend(j, i, 0)
        finish(j, i, mixed, total)

    def give(j, i):
        target = out_ref.at[:, cols(j * PLANE + role)]

        @pl.when(role == i)
        def _():
            pltpu.make_async_copy(mixed_ref.at[j, i], target, local_sem.at[2]).start()

        @pl.when(role != i)
        def _():
            remote(mixed_ref.at[j, i], target, out_send.at[0], out_recv.at[0], base + i)

    top = PLANE - 1

    def own_blocks(t, carry):
        j = last - t
        with jax.named_scope("wait_q"):

            @pl.when(jnp.logical_not(helped(j)))
            def _():
                await_q(j)

        with jax.named_scope("top"):
            simple(j, top)

            @pl.when(t > 0)
            def _():
                give(jnp.minimum(j + 1, last), top)

        return carry

    lax.fori_loop(0, planes, own_blocks, 0)

    def reach_back(j):
        with jax.named_scope("wait_halo"):

            @pl.when(late & (j <= plane))
            def _():
                await_halo(j)

        with jax.named_scope("units"):
            for i in range(top - 1, -1, -1):
                simple(j, i)
                if i == top - 1:

                    @pl.when(j == last)
                    def _():
                        give(0, top)

                    @pl.when(j < last)
                    def _():
                        give(jnp.minimum(j + 1, last), 0)

                else:
                    give(j, i + 1)

    descend(when_helped(reach_back, False))

    settled = pltpu.make_async_copy(
        kv.at[plane, :, rows(0, BACK)], landed_ref.at[:, below], load_sem.at[1]
    )

    @pl.when(late)
    def _():
        settled.start()

    for j in range(planes):
        first = jnp.logical_not(helped(j))

        @pl.when(first & helped(j - 1) if j else first)
        def _():
            give(j, 0)

    def merge(j):
        with jax.named_scope("wait_part"):
            await_(part_in.at[j], up_recv.at[0, j])
            await_(size_in.at[j], up_recv.at[1, j])
        with jax.named_scope("merge"):
            for i in range(top - 1, -1, -1):
                mixed, peak, total = attend(j, i, 1)
                mixed = [mixed[b * BLOCK : (b + 1) * BLOCK] for b in range(here)]
                total = [
                    jnp.broadcast_to(total[b * BLOCK : (b + 1) * BLOCK], (BLOCK, BLOCK))
                    for b in range(here)
                ]
                for b in range(here):
                    g = i * here + b
                    if g < BACK:
                        size = jnp.broadcast_to(size_in[j, g, :1], (BLOCK, BLOCK)).T
                        mark = peak[b * BLOCK : (b + 1) * BLOCK]
                        high = jnp.maximum(mark, size)
                        mine_share = jnp.exp2(mark - high)
                        their_share = jnp.exp2(size - high)
                        theirs = part_in[j, g * BLOCK : (g + 1) * BLOCK, :]
                        mixed[b] = mixed[b] * mine_share + theirs.astype(jnp.float32) * their_share
                        total[b] = total[b] * mine_share + their_share
                finish(
                    j, i, jnp.concatenate(mixed, axis=0), jnp.concatenate(total, axis=0)
                )
                if i < top - 1:
                    give(j, i + 1)
        give(j, 0)

    for h in helpable:

        @pl.when(helped(h))
        def _():
            merge(h)

    with jax.named_scope("drain"):
        others = features // PLANE * (PLANE - 1)
        await_(own.at[:, :, pl.ds(0, others)], kv_send.at[0])
        await_(q_ref.at[:, pl.ds(0, others)], q_send.at[0])
        await_(q_ref.at[:, pl.ds(0, features // PLANE)], local_sem.at[2])

        def drain(j):
            @pl.when(more & jnp.logical_not(helps(j)))
            def _():
                await_(kv.at[j, :, rows(0, BACK)], halo_send.at[j])

            @pl.when(helps(j))
            def _():
                await_(part_out.at[j], up_send.at[0, j])
                await_(size_out.at[j], up_send.at[1, j])

            @pl.when(helped(j))
            def _():
                await_(lower_q.at[j], down_send.at[j])

            @pl.when(j < plane)
            def _():
                await_(kv.at[j, :, rows(BACK, width)], land_send.at[0, j])

            @pl.when(j > plane)
            def _():
                await_(kv.at[j, :, rows(BACK, skip)], land_send.at[1, j])

            @pl.when(late & (j > plane))
            def _():
                await_(kv.at[j, :, rows(0, BACK)], land_send.at[2, j])

        each(drain)
        settle.wait()
        await_(q_ref.at[:, pl.ds(0, others)], out_send.at[0])
        await_(q_ref.at[:, pl.ds(0, others)], out_recv.at[0])

    with jax.named_scope("land"):

        @pl.when(late)
        def _():
            settled.wait()
            await_(landed_ref.at[:, rows(0, (planes - 1) * width - BACK)], land_recv.at[0])

        @pl.when(plane == 0)
        def _():
            await_(landed_ref.at[:, rows(0, (planes - 1) * width)], land_recv.at[0])


def wide_exchange(n, queries, keys, values, block_counts, last_tokens, pack_order):
    tokens, features = queries.shape
    here = tokens // BLOCK
    part = BLOCK // (n // HEADS)
    blocks = here * n
    kind = queries.dtype
    smem = pl.BlockSpec(memory_space=pltpu.SMEM)
    vmem = pl.BlockSpec(memory_space=pltpu.VMEM)
    anywhere = pl.BlockSpec(memory_space=pl.ANY)
    dma = pltpu.SemaphoreType.DMA
    return pl.pallas_call(
        functools.partial(exchange, n),
        out_shape=(
            jax.ShapeDtypeStruct((tokens, features), kind),
            jax.ShapeDtypeStruct((2, blocks * part, HEAD_DIM), kind),
        ),
        in_specs=[smem] * 3 + [anywhere] * 3,
        out_specs=(vmem, anywhere),
        scratch_shapes=[
            pltpu.VMEM((tokens, features), kind),
            pltpu.VMEM((2, tokens, features), kind),
            pltpu.VMEM((2, BACK * BLOCK, features), kind),
            pltpu.VMEM((2, 2 * BLOCK, features), kind),
            pltpu.VMEM((tokens, (BACK + here) * BLOCK), jnp.float32),
            dma((CHUNKS * 18,)),
            dma((BACK + 2, CHUNKS)),
            dma((2,)),
            dma((here,)),
            dma((3,)),
        ],
        compiler_params=pltpu.CompilerParams(
            collective_id=0, has_side_effects=True, vmem_limit_bytes=60 * 1024 * 1024
        ),
    )(block_counts, last_tokens, pack_order, queries, keys, values)


def local(n, queries, keys, values, block_counts, last_tokens, pack_order, decode_slot):
    tokens, features = queries.shape
    here = tokens // BLOCK
    splits = n // HEADS
    part = BLOCK // splits
    blocks = here * n
    kind = queries.dtype
    smem = pl.BlockSpec(memory_space=pltpu.SMEM)
    anywhere = pl.BlockSpec(memory_space=pl.ANY)
    dma = pltpu.SemaphoreType.DMA
    planes = n // PLANE
    reach = BACK * BLOCK
    cache = jax.ShapeDtypeStruct((1, blocks, part, HEAD_DIM), kind)
    if splits == 1 and here == 2 and planes > 1:
        attended, landed = pl.pallas_call(
            functools.partial(handoff, n),
            out_shape=(
                pltpu.VMEM((tokens, features), kind),
                pltpu.VMEM((2, blocks * part, HEAD_DIM), kind),
            ),
            in_specs=[smem] * 3 + [anywhere] * 3,
            out_specs=(anywhere, anywhere),
            scratch_shapes=[
                pltpu.VMEM((tokens, features), kind),
                pltpu.VMEM((2, tokens, features), kind),
                pltpu.VMEM((planes, 2, (BACK + PLANE * here) * BLOCK, HEAD_DIM), kind),
                pltpu.VMEM((planes, PLANE * tokens, HEAD_DIM), kind),
                pltpu.VMEM((planes, PLANE, tokens, HEAD_DIM), kind),
                pltpu.VMEM((2, PLANE, tokens, (BACK + here) * BLOCK), jnp.float32),
                pltpu.VMEM((planes, reach, HEAD_DIM), kind),
                pltpu.VMEM((reach, reach), jnp.float32),
                pltpu.VMEM((planes, reach, HEAD_DIM), kind),
                pltpu.VMEM((planes, reach, HEAD_DIM), kind),
                pltpu.VMEM((planes, BACK, 8, BLOCK), jnp.float32),
                pltpu.VMEM((planes, BACK, 8, BLOCK), jnp.float32),
                dma((3,)),
                dma((3,)),
                dma((1,)),
                dma((PLANE - 1, planes)),
                dma((1,)),
                dma((PLANE - 1, planes)),
                dma((planes,)),
                dma((planes, PLANE)),
                dma((3, planes)),
                dma((1,)),
                dma((1,)),
                dma((1,)),
                dma((planes,)),
                dma((planes,)),
                dma((2, planes)),
                dma((2, planes)),
            ],
            compiler_params=pltpu.CompilerParams(
                collective_id=0, has_side_effects=True, vmem_limit_bytes=60 * 1024 * 1024
            ),
        )(block_counts, last_tokens, pack_order, queries, keys, values)
        return pl.pallas_call(
            publish,
            out_shape=(jax.ShapeDtypeStruct((tokens, features), kind), cache, cache),
            in_specs=[smem] * 3 + [anywhere] * 2,
            out_specs=(anywhere,) * 3,
            scratch_shapes=[
                pltpu.SMEM(block_counts.shape, jnp.int32),
                pltpu.SMEM(block_counts.shape, jnp.int32),
                dma((3,)),
            ],
        )(
            block_counts,
            pack_order,
            decode_slot,
            pltpu.with_memory_space_constraint(landed, pltpu.VMEM),
            pltpu.with_memory_space_constraint(attended, pltpu.VMEM),
        )
    attended, landed = wide_exchange(
        n, queries, keys, values, block_counts, last_tokens, pack_order
    )
    cache_keys, cache_values = pl.pallas_call(
        reorder,
        out_shape=(cache, cache),
        in_specs=[smem] * 3 + [anywhere],
        out_specs=(anywhere, anywhere),
        scratch_shapes=[
            pltpu.VMEM((2, blocks, part, HEAD_DIM), kind),
            pltpu.SMEM(block_counts.shape, jnp.int32),
            pltpu.SMEM(block_counts.shape, jnp.int32),
            dma((2,)),
            dma((2,)),
        ],
    )(block_counts, pack_order, decode_slot, landed)
    return attended, cache_keys, cache_values


def solution(mesh):
    rows = P(("groups", "seq"), None)
    small = P("groups")
    cache = P(("groups", "seq"), None, None, None)
    return jax.shard_map(
        functools.partial(local, mesh.shape["seq"]),
        mesh=mesh,
        in_specs=(rows, rows, rows, small, small, small, small),
        out_specs=(rows, cache, cache),
        check_vma=False,
    )
```

```python
import functools
import math

import jax
import jax.numpy as jnp
from jax import lax
from jax.experimental import pallas as pl
from jax.experimental.pallas import tpu as pltpu
from jax.sharding import PartitionSpec as P

HEADS = 16
HEAD_DIM = 128
BLOCK = 128
MAXB = 6
BACK = MAXB - 1
HIDDEN = -1e30
PLANE = 4
CHUNKS = 4
RELAY = BACK
ROUND = 2


def window_tables(counts_ref, tails_ref, order_ref, first, width):
    pairs = counts_ref.shape[0]
    prompts = order_ref.shape[0]

    def place(i, carry):
        start, docs, valids = carry
        prompt = order_ref[i]
        counted = counts_ref[lax.rem(prompt, pairs)]
        size = jnp.where(prompt < pairs, counted, 1)
        tail = tails_ref[prompt]
        end = start + size
        new_docs, new_valids = [], []
        for w in range(width):
            b = first + w
            inside = (start <= b) & (b < end)
            new_docs.append(jnp.where(inside, i, docs[w]))
            new_valids.append(
                jnp.where(inside, jnp.where(b + 1 == end, tail, BLOCK), valids[w])
            )
        return end, tuple(new_docs), tuple(new_valids)

    none = jnp.int32(-1)
    zero = jnp.int32(0)
    _, docs, valids = lax.fori_loop(
        0, prompts, place, (zero, (none,) * width, (zero,) * width)
    )
    return docs, valids


def exchange(
    n,
    counts_ref,
    tails_ref,
    order_ref,
    q_hbm,
    k_hbm,
    v_hbm,
    out_ref,
    landed_ref,
    q_ref,
    own,
    halo,
    relay,
    bias,
    halo_send,
    halo_recv,
    cache_sem,
    own_sem,
    load_sem,
):
    me = lax.axis_index("seq")
    role = lax.rem(me, PLANE)
    plane = me // PLANE
    planes = n // PLANE
    tokens, features = q_ref.shape
    here = tokens // BLOCK
    splits = n // HEADS
    part = BLOCK // splits
    wide = features // CHUNKS

    loads = [
        pltpu.make_async_copy(src, dst, load_sem.at[i])
        for i, (src, dst) in enumerate(
            ((k_hbm, own.at[0]), (v_hbm, own.at[1]), (q_hbm, q_ref))
        )
    ]
    for copy in loads:
        copy.start()

    barrier = pltpu.get_barrier_semaphore()

    def greet(r, carry):
        pl.semaphore_signal(
            barrier,
            inc=1,
            device_id={"seq": lax.rem(me + r, n)},
            device_id_type=pl.DeviceIdType.MESH,
        )
        return carry

    lax.fori_loop(1, n, greet, 0)
    loads[0].wait()
    loads[1].wait()
    pl.semaphore_wait(barrier, n - 1)

    pending = []

    def spot(block, c):
        return (
            slice(None),
            pl.ds(block * BLOCK, BLOCK),
            pl.ds(c * wide, wide),
        )

    def mine(block):
        return lambda c: own.at[spot(block, c)]

    def held(slot):
        if slot >= RELAY:
            return lambda c: relay.at[spot(slot - RELAY, c)]
        return lambda c: halo.at[spot(slot, c)]

    def start(cond, c, moves):
        copies = []
        for src, target, slot in moves:
            copy = pltpu.make_async_remote_copy(
                src_ref=src(c),
                dst_ref=held(slot)(c),
                send_sem=halo_send.at[len(pending)],
                recv_sem=halo_recv.at[slot, c],
                device_id={"seq": lax.rem(target + n, n)},
                device_id_type=pl.DeviceIdType.MESH,
            )
            pending.append((cond, copy))
            copies.append(copy)

        @pl.when(cond)
        def _():
            for copy in copies:
                copy.start()

    def await_slots(cond, c, slots):
        @pl.when(cond)
        def _():
            for slot in slots:
                ref = held(slot)(c)
                pltpu.make_async_copy(ref, ref, halo_recv.at[slot, c]).wait()

    more = plane < planes - 1
    late = plane > 0
    for c in range(CHUNKS):
        start((role == 3) & more, c, [(mine(0), me + 3, RELAY), (mine(1), me + 3, 0)])
        if c < ROUND:
            moves = [(mine(1), me - 2, RELAY + 1), (mine(0), me - 2, RELAY)]
        else:
            moves = [(mine(1), me + 2, 2), (mine(0), me + 2, 1)]
        start((role == 2) & more, c, moves)
        start((role == 1) & more, c, [(mine(1), me + 3, 0)])
        start(role == 1, c, [(mine(0), me + 1, 3), (mine(1), me + 1, 4)])
        start(role == 0, c, [(mine(1), me + 2, 2), (mine(0), me + 2, 1)])
        start(
            (role == 0) | (role == 2),
            c,
            [(mine(0), me + 1, 3), (mine(1), me + 1, 4)],
        )

    def piece(owner, block):
        head = owner // splits
        cols = pl.ds(pl.multiple_of(head * HEAD_DIM, HEAD_DIM), HEAD_DIM)
        if splits == 1:
            return own.at[:, :, cols]
        offset = pl.multiple_of(block * BLOCK + lax.rem(owner, splits) * part, part)
        return own.at[:, pl.ds(offset, part), cols]

    def place(block):
        if splits == 1:
            return landed_ref.at[:, pl.ds(pl.multiple_of(me * tokens, tokens), tokens)]
        return landed_ref.at[
            :, pl.ds(pl.multiple_of((me * here + block) * part, part), part)
        ]

    pieces = 1 if splits == 1 else here

    def give(s, carry):
        sign = 1 - 2 * lax.rem(s, 2)
        target = lax.rem(me + n // 2 + sign * ((s + 1) // 2), n)
        for block in range(pieces):
            pltpu.make_async_remote_copy(
                src_ref=piece(target, block),
                dst_ref=place(block),
                send_sem=cache_sem.at[0],
                recv_sem=cache_sem.at[1],
                device_id={"seq": target},
                device_id_type=pl.DeviceIdType.MESH,
            ).start()
        return carry

    cuts = [(n - 1) * i // CHUNKS for i in range(CHUNKS + 1)]

    docs, valids = window_tables(
        counts_ref, tails_ref, order_ref, me * here - BACK, BACK + here
    )
    row = lax.broadcasted_iota(jnp.int32, (BLOCK, BLOCK), 0)
    col = lax.broadcasted_iota(jnp.int32, (BLOCK, BLOCK), 1)
    for b in range(here):
        for w in range(BACK + here):
            if w > BACK + b:
                shade = jnp.full((BLOCK, BLOCK), HIDDEN, jnp.float32)
            else:
                limit = jnp.where(docs[w] == docs[BACK + b], valids[w], 0)
                seen = col < limit
                if w == BACK + b:
                    seen = seen & (col <= row)
                shade = jnp.where(seen, 0.0, HIDDEN)
            bias[b * BLOCK : (b + 1) * BLOCK, w * BLOCK : (w + 1) * BLOCK] = shade
    column = lax.broadcasted_iota(jnp.int32, (BLOCK, HEAD_DIM), 0)
    real = jnp.concatenate(
        [column < valids[BACK + b] for b in range(here)], axis=0
    )

    empty = jnp.zeros((BLOCK, features), halo.dtype)
    for slot, reach in ((0, 3), (1, 2), (2, 2), (3, 1), (4, 1)):

        @pl.when(me < reach)
        def _():
            for kv in range(2):
                halo[kv, slot * BLOCK : (slot + 1) * BLOCK, :] = empty

    loads[2].wait()

    factor = HEAD_DIM ** (-0.5) * math.log2(math.e)
    prior = BACK * BLOCK
    nt = (((1,), (1,)), ((), ()))

    def one_head(h, carry):
        cols = pl.ds(pl.multiple_of(h * HEAD_DIM, HEAD_DIM), HEAD_DIM)
        q = q_ref[:, cols]
        s1 = lax.dot_general(q, halo[0, :, cols], nt, preferred_element_type=jnp.float32)
        s2 = lax.dot_general(q, own[0, :, cols], nt, preferred_element_type=jnp.float32)
        s1 = s1 + bias[:, :prior]
        s2 = s2 + bias[:, prior:]
        peak = jnp.maximum(
            jnp.max(s1, axis=1, keepdims=True), jnp.max(s2, axis=1, keepdims=True)
        )
        w1 = jnp.exp2((s1 - peak) * factor)
        w2 = jnp.exp2((s2 - peak) * factor)
        total = jnp.sum(w1, axis=1, keepdims=True) + jnp.sum(w2, axis=1, keepdims=True)
        mixed = jnp.dot(
            w1.astype(jnp.bfloat16), halo[1, :, cols], preferred_element_type=jnp.float32
        ) + jnp.dot(
            w2.astype(jnp.bfloat16), own[1, :, cols], preferred_element_type=jnp.float32
        )
        out_ref[:, cols] = jnp.where(real, mixed / total, 0.0).astype(out_ref.dtype)
        return carry

    for c in range(CHUNKS):
        lax.fori_loop(cuts[c], cuts[c + 1], give, 0)
        if c < ROUND:
            await_slots((role == 0) & more, c, [RELAY, RELAY + 1])
            start(
                (role == 0) & more,
                c,
                [(held(RELAY + 1), me + PLANE, 2), (held(RELAY), me + PLANE, 1)],
            )
        await_slots((role == 2) & late, c, [RELAY, 0])
        start(
            (role == 2) & late, c, [(held(RELAY), me - 2 + n, 3), (held(0), me - 2 + n, 4)]
        )
        await_slots((role == 0) & late, c, [2, 3, 4])
        await_slots(role == 2, c, [2, 3, 4])
        start(
            (role == 2) | ((role == 0) & late),
            c,
            [(held(2), me + 1, 0), (held(3), me + 1, 1), (held(4), me + 1, 2)],
        )
        await_slots((role == 0) & late, c, [0, 1])
        await_slots(role == 1, c, [3, 4])
        await_slots((role == 1) & late, c, [0, 1, 2])
        await_slots(role == 2, c, [1])
        await_slots(role == 3, c, [0, 1, 2, 3, 4])
        each = HEADS // CHUNKS
        lax.fori_loop(c * each, (c + 1) * each, one_head, 0)

    copies = [
        pltpu.make_async_copy(piece(me, block), place(block), own_sem.at[block])
        for block in range(pieces)
    ]
    for copy in copies:
        copy.start()

    for cond, copy in pending:

        @pl.when(cond)
        def _():
            copy.wait_send()

    for copy in copies:
        copy.wait()
    others = landed_ref.shape[1] // n * (n - 1)
    ref = landed_ref.at[:, pl.ds(0, others)]
    pltpu.make_async_copy(ref, ref, cache_sem.at[0]).wait()
    pltpu.make_async_copy(ref, ref, cache_sem.at[1]).wait()


def decode_places(counts_ref, order_ref, slot_ref, who, base, put):
    pairs = counts_ref.shape[0]
    prompts = order_ref.shape[0]

    def invert(p, carry):
        who[slot_ref[p]] = p
        return carry

    lax.fori_loop(0, pairs, invert, 0)

    def lay(s, first):
        p = who[s]
        base[p] = first
        return first + counts_ref[p] + 1

    lax.fori_loop(0, pairs, lay, jnp.int32(0))

    def fetch(i, first):
        prompt = order_ref[i]
        pair = lax.rem(prompt, pairs)
        null = prompt >= pairs
        counted = counts_ref[pair]
        size = jnp.where(null, 1, counted)
        target = base[pair] + jnp.where(null, counted, 0)

        def one(w, carry):
            put(first + w, target + w)
            return carry

        lax.fori_loop(0, size, one, 0)
        return first + size

    lax.fori_loop(0, prompts, fetch, jnp.int32(0))


def reorder(
    counts_ref,
    order_ref,
    slot_ref,
    landed_ref,
    keys_ref,
    values_ref,
    staged,
    who,
    base,
    in_sem,
    out_sem,
):
    part = staged.shape[2]

    def put(source, target):
        for kv in range(2):
            pltpu.make_async_copy(
                landed_ref.at[kv, pl.ds(source * part, part)],
                staged.at[kv, target],
                in_sem.at[kv],
            ).start()

    decode_places(counts_ref, order_ref, slot_ref, who, base, put)
    outs = []
    for kv, ref in enumerate((keys_ref, values_ref)):
        pltpu.make_async_copy(staged.at[kv], staged.at[kv], in_sem.at[kv]).wait()
        copy = pltpu.make_async_copy(staged.at[kv], ref.at[0], out_sem.at[kv])
        copy.start()
        outs.append(copy)
    for copy in outs:
        copy.wait()


def publish(places_ref, landed_ref, mixed_ref, attended_ref, keys_ref, values_ref, out_sem):
    leave = pltpu.make_async_copy(mixed_ref, attended_ref, out_sem.at[2])
    leave.start()
    refs = (keys_ref, values_ref)
    part = keys_ref.shape[2]

    def put(b, carry):
        for kv, ref in enumerate(refs):
            pltpu.make_async_copy(
                landed_ref.at[kv, pl.ds(pl.multiple_of(b * part, part), part)],
                ref.at[0, places_ref[b]],
                out_sem.at[kv],
            ).start()
        return carry

    lax.fori_loop(0, places_ref.shape[0], put, 0)
    leave.wait()
    for kv, ref in enumerate(refs):
        pltpu.make_async_copy(ref.at[0], ref.at[0], out_sem.at[kv]).wait()


def handoff(
    n,
    counts_hbm,
    tails_hbm,
    order_hbm,
    slot_hbm,
    q_hbm,
    k_hbm,
    v_hbm,
    out_ref,
    landed_ref,
    places_ref,
    counts_ref,
    tails_ref,
    order_ref,
    slot_ref,
    q_ref,
    own,
    kv,
    qs,
    mixed_ref,
    bias,
    lower_q,
    lower_bias,
    part_out,
    part_in,
    size_out,
    size_in,
    small_sem,
    load_sem,
    local_sem,
    kv_send,
    kv_recv,
    q_send,
    q_recv,
    halo_send,
    halo_recv,
    land_send,
    land_recv,
    out_send,
    out_recv,
    down_send,
    down_recv,
    up_send,
    up_recv,
):
    me = lax.axis_index("seq")
    role = lax.rem(me, PLANE)
    plane = me // PLANE
    planes = n // PLANE
    tokens, features = q_ref.shape
    here = tokens // BLOCK
    width = PLANE * here
    skip = width - BACK
    reach = BACK * BLOCK
    peers = (role + 1 - 2 * lax.rem(role, 2), lax.rem(role + 2, PLANE), PLANE - 1 - role)
    more = plane < planes - 1
    late = plane > 0
    base = plane * PLANE
    last = planes - 1
    orders = []
    for p in range(planes):
        above = list(range(last, p, -1))
        helping = [j for j in range(p + 1) if j + p < last and 2 * p >= planes - 2]
        rest = [j for j in range(p, -1, -1) if j not in helping]
        if p == last:
            above, helping, rest = [last - 1], list(range(last - 1)), [last]
        orders.append(above + helping + rest)
    def one_if(i, value):
        return (i + planes - value) // planes - (i + planes - value - 1) // planes

    picks = [
        sum(orders[p][t] * one_if(plane, p) for p in range(planes)) for t in range(planes)
    ]

    def turn(t):
        return sum(picks[other] * one_if(t, other) for other in range(planes))

    def hold(j):
        return ((plane == last) & (j < plane - 1)) | ((plane == 0) & (j < planes // 2))

    def back(j, p):
        return (j <= p) & (j + p < planes - 1) & (2 * p >= planes - 2)

    helpable = sorted({j for p in range(last) for j in range(p + 1) if j + p < last and 2 * p >= planes - 2})

    def helps(j):
        return more & back(j, plane)

    def helped(j):
        return late & back(j, plane - 1)

    def each(body):
        def step(t, carry):
            body(turn(t))
            return carry

        lax.fori_loop(0, planes, step, 0)

    def rows(first, count):
        return pl.ds(pl.multiple_of(first * BLOCK, BLOCK), count * BLOCK)

    def cols(head):
        return pl.ds(pl.multiple_of(head * HEAD_DIM, HEAD_DIM), HEAD_DIM)

    def remote(src, dst, send, recv, target):
        pltpu.make_async_remote_copy(
            src_ref=src,
            dst_ref=dst,
            send_sem=send,
            recv_sem=recv,
            device_id={"seq": target},
            device_id_type=pl.DeviceIdType.MESH,
        ).start()

    def await_(ref, sem):
        pltpu.make_async_copy(ref, ref, sem).wait()

    mine = rows(BACK + role * here, here)
    place = rows(role * here, here)

    loads = [
        pltpu.make_async_copy(src, dst, load_sem.at[i])
        for i, (src, dst) in enumerate(
            ((k_hbm, own.at[0]), (v_hbm, own.at[1]), (q_hbm, q_ref))
        )
    ]
    barrier = pltpu.get_barrier_semaphore()
    for peer in peers:
        pl.semaphore_signal(
            barrier,
            inc=1,
            device_id={"seq": base + peer},
            device_id_type=pl.DeviceIdType.MESH,
        )
    for step in range(1, planes):
        pl.semaphore_signal(
            barrier,
            inc=1,
            device_id={"seq": lax.rem(me + step * PLANE, n)},
            device_id_type=pl.DeviceIdType.MESH,
        )
    for j in range(planes):
        here_cols = cols(j * PLANE + role)
        for i, src in enumerate((k_hbm, v_hbm)):
            pltpu.make_async_copy(
                src.at[:, here_cols], kv.at[j, i, mine], local_sem.at[0]
            ).start()
    for load in loads:
        load.start()
    smalls = [
        pltpu.make_async_copy(src, dst, small_sem.at[i])
        for i, (src, dst) in enumerate(
            (
                (counts_hbm, counts_ref),
                (tails_hbm, tails_ref),
                (order_hbm, order_ref),
                (slot_hbm, slot_ref),
            )
        )
    ]
    for small in smalls:
        small.start()
    for j in range(planes):
        here_cols = cols(j * PLANE + role)
        pltpu.make_async_copy(
            q_hbm.at[:, here_cols], qs.at[j, place], local_sem.at[1]
        ).start()

    for j in range(planes):

        @pl.when((plane == 0) | helped(j))
        def _():
            for i in range(2):
                kv[j, i, :reach, :] = jnp.zeros((reach, HEAD_DIM), kv.dtype)

    def share(j):
        for k in (1, 2, 0):
            remote(
                own.at[:, :, cols(j * PLANE + peers[k])],
                kv.at[j, :, mine],
                kv_send.at[0],
                kv_recv.at[k, j],
                base + peers[k],
            )

    def share_q(j):
        for k in (1, 2, 0):
            remote(
                q_ref.at[:, cols(j * PLANE + peers[k])],
                qs.at[j, place],
                q_send.at[0],
                q_recv.at[k, j],
                base + peers[k],
            )

    def when_helped(body, truth):
        def step(j):
            @pl.when(helped(j) if truth else jnp.logical_not(helped(j)))
            def _():
                body(j)

        return step

    def descend(body):
        def step(t, carry):
            body(last - t)
            return carry

        lax.fori_loop(0, planes, step, 0)

    def forward(j, rho):
        first = BACK + rho * here
        low = rho * here < skip
        high = rho * here + here > skip
        up = more & jnp.logical_not(helps(j))

        @pl.when(up & jnp.logical_not(low))
        def _():
            remote(
                kv.at[j, :, rows(first, here)],
                kv.at[j, :, rows(jnp.maximum(rho * here - skip, 0), here)],
                halo_send.at[j],
                halo_recv.at[j, rho],
                me + PLANE,
            )

        @pl.when(up & low & high)
        def _():
            remote(
                kv.at[j, :, rows(BACK + skip, BACK % here)],
                kv.at[j, :, rows(0, BACK % here)],
                halo_send.at[j],
                halo_recv.at[j, rho],
                me + PLANE,
            )

        @pl.when(late & (j > plane) & low & high)
        def _():
            remote(
                kv.at[j, :, rows(first, skip % here)],
                landed_ref.at[:, rows(plane * width + rho * here, skip % here)],
                land_send.at[1, j],
                land_recv.at[0],
                j * PLANE + role,
            )

        @pl.when(late & (j > plane) & jnp.logical_not(high))
        def _():
            remote(
                kv.at[j, :, rows(first, here)],
                landed_ref.at[:, rows(plane * width + rho * here, here)],
                land_send.at[1, j],
                land_recv.at[0],
                j * PLANE + role,
            )

        @pl.when(j < plane)
        def _():
            remote(
                kv.at[j, :, rows(first, here)],
                landed_ref.at[:, rows(plane * width + rho * here, here)],
                land_send.at[0, j],
                land_recv.at[0],
                j * PLANE + role,
            )

    def start_mine(j):
        @pl.when(jnp.logical_not(hold(j)))
        def _():
            forward(j, role)

    def take(k, j):
        await_(kv.at[j, :, rows(BACK + peers[k] * here, here)], kv_recv.at[k, j])

    def start_core(truth):
        def body(j):
            later = helped(j) & (j > 0)

            @pl.when(later if truth else jnp.logical_not(later))
            def _():
                take(0, j)

                @pl.when(jnp.logical_not(hold(j)))
                def _():
                    forward(j, peers[0])

        return body

    with jax.named_scope("enter_local"):
        await_(kv.at[:, :, mine], local_sem.at[0])
    with jax.named_scope("enter_barrier"):
        pl.semaphore_wait(barrier, PLANE - 1 + planes - 1)
    with jax.named_scope("start_mine"):
        each(start_mine)
    with jax.named_scope("enter_loads"):
        for load in loads:
            load.wait()
    with jax.named_scope("share"):
        each(when_helped(share_q, True))
        each(share)
        descend(when_helped(share_q, False))

    with jax.named_scope("take_core"):
        each(start_core(False))

    with jax.named_scope("tables"):
        for small in smalls:
            small.wait()
        docs, valids = window_tables(
            counts_ref, tails_ref, order_ref, plane * width - BACK, BACK + width + BACK
        )
        row = lax.broadcasted_iota(jnp.int32, (BLOCK, BLOCK), 0)
        col = lax.broadcasted_iota(jnp.int32, (BLOCK, BLOCK), 1)
        hidden = jnp.full((BLOCK, BLOCK), HIDDEN, jnp.float32)

        def shade(source, target):
            limit = jnp.where(docs[source] == docs[target], valids[source], 0)
            seen = col < limit
            if source == target:
                seen = seen & (col <= row)
            return jnp.where(seen, 0.0, HIDDEN)

        for i in range(PLANE):
            for b in range(here):
                target = BACK + i * here + b
                for w in range(BACK + here):
                    source = i * here + w
                    spot = (slice(b * BLOCK, (b + 1) * BLOCK), slice(w * BLOCK, (w + 1) * BLOCK))
                    full = hidden if source > target else shade(source, target)
                    bias[(0, i) + spot] = full
                    bias[(1, i) + spot] = hidden if source < BACK else full
        for g in range(BACK):
            for c in range(BACK):
                lower_bias[g * BLOCK : (g + 1) * BLOCK, c * BLOCK : (c + 1) * BLOCK] = shade(
                    BACK + skip + c, BACK + width + g
                )
        column = lax.broadcasted_iota(jnp.int32, (BLOCK, HEAD_DIM), 0)

    def await_q(j):
        for k in range(PLANE - 1):
            await_(qs.at[j, rows(peers[k] * here, here)], q_recv.at[k, j])

    await_(qs.at[:, place], local_sem.at[1])

    def lower(j):
        await_q(j)
        remote(
            qs.at[j, pl.ds(0, reach)],
            lower_q.at[j],
            down_send.at[j],
            down_recv.at[j],
            me - PLANE,
        )

    with jax.named_scope("lower_q"):
        for h in helpable:

            @pl.when(helped(h))
            def _():
                lower(h)

    each(start_core(True))

    def await_halo(j):
        for rho in range(PLANE):
            count = min(here, (rho + 1) * here - skip)
            if count > 0:
                await_(
                    kv.at[j, :, rows(max(rho * here - skip, 0), count)],
                    halo_recv.at[j, rho],
                )

    below = rows(jnp.maximum(plane * width - BACK, 0), BACK)

    def relay(j):
        @pl.when(late & (j > plane))
        def _():
            await_halo(j)
            remote(
                kv.at[j, :, rows(0, BACK)],
                landed_ref.at[:, below],
                land_send.at[2, j],
                land_recv.at[0],
                j * PLANE + role,
            )

    def map_places():
        pairs = counts_ref.shape[0]
        blocks = places_ref.shape[0]

        def empty(b, carry):
            places_ref[b] = 0
            return carry

        lax.fori_loop(0, blocks, empty, 0)

        def fill(i, first):
            prompt = order_ref[i]
            pair = lax.rem(prompt, pairs)
            null = prompt >= pairs
            counted = counts_ref[pair]
            end = first + jnp.where(null, 1, counted)
            slot = slot_ref[pair]

            def earlier(p, total):
                return total + jnp.where(slot_ref[p] < slot, counts_ref[p] + 1, 0)

            target = lax.fori_loop(0, pairs, earlier, jnp.where(null, counted, 0)) - first

            def mark(b, carry):
                inside = (first <= b) & (b < end)
                places_ref[b] = jnp.where(inside, target + b, places_ref[b])
                return carry

            lax.fori_loop(0, blocks, mark, 0)
            return end

        lax.fori_loop(0, order_ref.shape[0], fill, jnp.int32(0))

    with jax.named_scope("map_places"):
        map_places()

    factor = HEAD_DIM ** (-0.5) * math.log2(math.e)
    nt = (((1,), (1,)), ((), ()))
    span = (BACK + here) * BLOCK

    def soften(q, k, v, mask):
        s = lax.dot_general(q, k, nt, preferred_element_type=jnp.float32) + mask
        peak = jnp.max(s, axis=1, keepdims=True)
        w = jnp.exp2((s - peak) * factor)
        total = jnp.sum(w, axis=1, keepdims=True)
        mixed = jnp.dot(w.astype(jnp.bfloat16), v, preferred_element_type=jnp.float32)
        return mixed, peak * factor, total

    def help_out(j):
        await_(lower_q.at[j], down_recv.at[j])
        for first in range(0, BACK, here):
            count = min(here, BACK - first)
            lines = slice(first * BLOCK, (first + count) * BLOCK)
            window = pl.ds((BACK + skip + first) * BLOCK, (BACK - first) * BLOCK)
            mixed, peak, total = soften(
                lower_q[j, lines, :],
                kv[j, 0, window, :],
                kv[j, 1, window, :],
                lower_bias[lines, first * BLOCK :],
            )
            part_out[j, lines, :] = (mixed / total).astype(part_out.dtype)
            size = jnp.broadcast_to(peak + jnp.log2(total), (count * BLOCK, BLOCK))
            for b in range(count):
                turned = size[b * BLOCK : (b + 1) * BLOCK].T
                size_out[j, first + b] = turned[:8]

    def send_up(j):
        remote(part_out.at[j], part_in.at[j], up_send.at[0, j], up_recv.at[0, j], me + PLANE)
        remote(size_out.at[j], size_in.at[j], up_send.at[1, j], up_recv.at[1, j], me + PLANE)

    def release(j):
        @pl.when(hold(j))
        def _():
            forward(j, role)
            forward(j, peers[0])

    def far(t, carry):
        j = turn(t)
        with jax.named_scope("take_far"):
            for k in (1, 2):
                take(k, j)
                forward(j, peers[k])

        @pl.when(t == min(1, last))
        def _():
            each(release)

        for h in helpable:

            @pl.when(helps(h) & (j == h))
            def _():
                with jax.named_scope("help_out"):
                    help_out(h)

        for h in helpable:

            @pl.when(helps(h) & (j == h))
            def _():
                send_up(h)

        return carry

    lax.fori_loop(0, planes, far, 0)

    def climb(j, carry):
        @pl.when((plane == 0) & (j > 0))
        def _():
            remote(
                kv.at[j, :, rows(BACK, skip)],
                landed_ref.at[:, rows(0, skip)],
                land_send.at[1, j],
                land_recv.at[0],
                j * PLANE + role,
            )

        return carry

    lax.fori_loop(0, planes, climb, 0)

    with jax.named_scope("relay"):
        descend(relay)

    settle = pltpu.make_async_copy(
        kv.at[plane, :, rows(BACK, width)],
        landed_ref.at[:, rows(plane * width, width)],
        load_sem.at[0],
    )
    settle.start()

    def attend(j, i, variant):
        window = pl.ds(i * tokens, span)
        return soften(
            qs[j, pl.ds(i * tokens, tokens), :],
            kv[j, 0, window, :],
            kv[j, 1, window, :],
            bias[variant, i],
        )

    def finish(j, i, mixed, total):
        real = jnp.concatenate(
            [column < valids[BACK + i * here + b] for b in range(here)], axis=0
        )
        mixed_ref[j, i] = jnp.where(real, mixed / total, 0.0).astype(mixed_ref.dtype)

    def simple(j, i):
        mixed, _, total = attend(j, i, 0)
        finish(j, i, mixed, total)

    def give(j, i):
        target = out_ref.at[:, cols(j * PLANE + role)]

        @pl.when(role == i)
        def _():
            pltpu.make_async_copy(mixed_ref.at[j, i], target, local_sem.at[2]).start()

        @pl.when(role != i)
        def _():
            remote(mixed_ref.at[j, i], target, out_send.at[0], out_recv.at[0], base + i)

    top = PLANE - 1

    def own_blocks(t, carry):
        j = last - t
        with jax.named_scope("wait_q"):

            @pl.when(jnp.logical_not(helped(j)))
            def _():
                await_q(j)

        with jax.named_scope("top"):
            simple(j, top)

            @pl.when(t > 0)
            def _():
                give(jnp.minimum(j + 1, last), top)

        return carry

    lax.fori_loop(0, planes, own_blocks, 0)

    def reach_back(j):
        with jax.named_scope("wait_halo"):

            @pl.when(late & (j <= plane))
            def _():
                await_halo(j)

        with jax.named_scope("units"):
            for i in range(top - 1, -1, -1):
                simple(j, i)
                if i == top - 1:

                    @pl.when(j == last)
                    def _():
                        give(0, top)

                    @pl.when(j < last)
                    def _():
                        give(jnp.minimum(j + 1, last), 0)

                else:
                    give(j, i + 1)

    descend(when_helped(reach_back, False))

    settled = pltpu.make_async_copy(
        kv.at[plane, :, rows(0, BACK)], landed_ref.at[:, below], load_sem.at[1]
    )

    @pl.when(late)
    def _():
        settled.start()

    for j in range(planes):
        first = jnp.logical_not(helped(j))

        @pl.when(first & helped(j - 1) if j else first)
        def _():
            give(j, 0)

    def merge(j):
        with jax.named_scope("wait_part"):
            await_(part_in.at[j], up_recv.at[0, j])
            await_(size_in.at[j], up_recv.at[1, j])
        with jax.named_scope("merge"):
            for i in range(top - 1, -1, -1):
                mixed, peak, total = attend(j, i, 1)
                mixed = [mixed[b * BLOCK : (b + 1) * BLOCK] for b in range(here)]
                total = [
                    jnp.broadcast_to(total[b * BLOCK : (b + 1) * BLOCK], (BLOCK, BLOCK))
                    for b in range(here)
                ]
                for b in range(here):
                    g = i * here + b
                    if g < BACK:
                        size = jnp.broadcast_to(size_in[j, g, :1], (BLOCK, BLOCK)).T
                        mark = peak[b * BLOCK : (b + 1) * BLOCK]
                        high = jnp.maximum(mark, size)
                        mine_share = jnp.exp2(mark - high)
                        their_share = jnp.exp2(size - high)
                        theirs = part_in[j, g * BLOCK : (g + 1) * BLOCK, :]
                        mixed[b] = mixed[b] * mine_share + theirs.astype(jnp.float32) * their_share
                        total[b] = total[b] * mine_share + their_share
                finish(
                    j, i, jnp.concatenate(mixed, axis=0), jnp.concatenate(total, axis=0)
                )
                if i < top - 1:
                    give(j, i + 1)
        give(j, 0)

    for h in helpable:

        @pl.when(helped(h))
        def _():
            merge(h)

    with jax.named_scope("drain"):
        others = features // PLANE * (PLANE - 1)
        await_(own.at[:, :, pl.ds(0, others)], kv_send.at[0])
        await_(q_ref.at[:, pl.ds(0, others)], q_send.at[0])
        await_(q_ref.at[:, pl.ds(0, features // PLANE)], local_sem.at[2])

        def drain(j):
            @pl.when(more & jnp.logical_not(helps(j)))
            def _():
                await_(kv.at[j, :, rows(0, BACK)], halo_send.at[j])

            @pl.when(helps(j))
            def _():
                await_(part_out.at[j], up_send.at[0, j])
                await_(size_out.at[j], up_send.at[1, j])

            @pl.when(helped(j))
            def _():
                await_(lower_q.at[j], down_send.at[j])

            @pl.when(j < plane)
            def _():
                await_(kv.at[j, :, rows(BACK, width)], land_send.at[0, j])

            @pl.when(j > plane)
            def _():
                await_(kv.at[j, :, rows(BACK, skip)], land_send.at[1, j])

            @pl.when(late & (j > plane))
            def _():
                await_(kv.at[j, :, rows(0, BACK)], land_send.at[2, j])

        each(drain)
        settle.wait()
        await_(q_ref.at[:, pl.ds(0, others)], out_send.at[0])
        await_(q_ref.at[:, pl.ds(0, others)], out_recv.at[0])

    with jax.named_scope("land"):

        @pl.when(late)
        def _():
            settled.wait()
            await_(landed_ref.at[:, rows(0, (planes - 1) * width - BACK)], land_recv.at[0])

        @pl.when(plane == 0)
        def _():
            await_(landed_ref.at[:, rows(0, (planes - 1) * width)], land_recv.at[0])


def wide_exchange(n, queries, keys, values, block_counts, last_tokens, pack_order):
    tokens, features = queries.shape
    here = tokens // BLOCK
    part = BLOCK // (n // HEADS)
    blocks = here * n
    kind = queries.dtype
    smem = pl.BlockSpec(memory_space=pltpu.SMEM)
    vmem = pl.BlockSpec(memory_space=pltpu.VMEM)
    anywhere = pl.BlockSpec(memory_space=pl.ANY)
    dma = pltpu.SemaphoreType.DMA
    return pl.pallas_call(
        functools.partial(exchange, n),
        out_shape=(
            jax.ShapeDtypeStruct((tokens, features), kind),
            jax.ShapeDtypeStruct((2, blocks * part, HEAD_DIM), kind),
        ),
        in_specs=[smem] * 3 + [anywhere] * 3,
        out_specs=(vmem, anywhere),
        scratch_shapes=[
            pltpu.VMEM((tokens, features), kind),
            pltpu.VMEM((2, tokens, features), kind),
            pltpu.VMEM((2, BACK * BLOCK, features), kind),
            pltpu.VMEM((2, 2 * BLOCK, features), kind),
            pltpu.VMEM((tokens, (BACK + here) * BLOCK), jnp.float32),
            dma((CHUNKS * 18,)),
            dma((BACK + 2, CHUNKS)),
            dma((2,)),
            dma((here,)),
            dma((3,)),
        ],
        compiler_params=pltpu.CompilerParams(
            collective_id=0, has_side_effects=True, vmem_limit_bytes=60 * 1024 * 1024
        ),
    )(block_counts, last_tokens, pack_order, queries, keys, values)


def local(n, queries, keys, values, block_counts, last_tokens, pack_order, decode_slot):
    tokens, features = queries.shape
    here = tokens // BLOCK
    splits = n // HEADS
    part = BLOCK // splits
    blocks = here * n
    kind = queries.dtype
    smem = pl.BlockSpec(memory_space=pltpu.SMEM)
    anywhere = pl.BlockSpec(memory_space=pl.ANY)
    dma = pltpu.SemaphoreType.DMA
    planes = n // PLANE
    reach = BACK * BLOCK
    cache = jax.ShapeDtypeStruct((1, blocks, part, HEAD_DIM), kind)
    if splits == 1 and here == 2 and planes > 1:
        attended, landed, places = pl.pallas_call(
            functools.partial(handoff, n),
            out_shape=(
                pltpu.VMEM((tokens, features), kind),
                pltpu.VMEM((2, blocks * part, HEAD_DIM), kind),
                pltpu.SMEM((blocks,), jnp.int32),
            ),
            in_specs=[anywhere] * 7,
            out_specs=(anywhere, anywhere, smem),
            scratch_shapes=[
                pltpu.SMEM(block_counts.shape, jnp.int32),
                pltpu.SMEM(last_tokens.shape, jnp.int32),
                pltpu.SMEM(pack_order.shape, jnp.int32),
                pltpu.SMEM(decode_slot.shape, jnp.int32),
                pltpu.VMEM((tokens, features), kind),
                pltpu.VMEM((2, tokens, features), kind),
                pltpu.VMEM((planes, 2, (BACK + PLANE * here) * BLOCK, HEAD_DIM), kind),
                pltpu.VMEM((planes, PLANE * tokens, HEAD_DIM), kind),
                pltpu.VMEM((planes, PLANE, tokens, HEAD_DIM), kind),
                pltpu.VMEM((2, PLANE, tokens, (BACK + here) * BLOCK), jnp.float32),
                pltpu.VMEM((planes, reach, HEAD_DIM), kind),
                pltpu.VMEM((reach, reach), jnp.float32),
                pltpu.VMEM((planes, reach, HEAD_DIM), kind),
                pltpu.VMEM((planes, reach, HEAD_DIM), kind),
                pltpu.VMEM((planes, BACK, 8, BLOCK), jnp.float32),
                pltpu.VMEM((planes, BACK, 8, BLOCK), jnp.float32),
                dma((4,)),
                dma((3,)),
                dma((3,)),
                dma((1,)),
                dma((PLANE - 1, planes)),
                dma((1,)),
                dma((PLANE - 1, planes)),
                dma((planes,)),
                dma((planes, PLANE)),
                dma((3, planes)),
                dma((1,)),
                dma((1,)),
                dma((1,)),
                dma((planes,)),
                dma((planes,)),
                dma((2, planes)),
                dma((2, planes)),
            ],
            compiler_params=pltpu.CompilerParams(
                collective_id=0, has_side_effects=True, vmem_limit_bytes=60 * 1024 * 1024
            ),
        )(block_counts, last_tokens, pack_order, decode_slot, queries, keys, values)
        return pl.pallas_call(
            publish,
            out_shape=(jax.ShapeDtypeStruct((tokens, features), kind), cache, cache),
            in_specs=[smem] + [anywhere] * 2,
            out_specs=(anywhere,) * 3,
            scratch_shapes=[dma((3,))],
        )(
            pltpu.with_memory_space_constraint(places, pltpu.SMEM),
            pltpu.with_memory_space_constraint(landed, pltpu.VMEM),
            pltpu.with_memory_space_constraint(attended, pltpu.VMEM),
        )
    attended, landed = wide_exchange(
        n, queries, keys, values, block_counts, last_tokens, pack_order
    )
    cache_keys, cache_values = pl.pallas_call(
        reorder,
        out_shape=(cache, cache),
        in_specs=[smem] * 3 + [anywhere],
        out_specs=(anywhere, anywhere),
        scratch_shapes=[
            pltpu.VMEM((2, blocks, part, HEAD_DIM), kind),
            pltpu.SMEM(block_counts.shape, jnp.int32),
            pltpu.SMEM(block_counts.shape, jnp.int32),
            dma((2,)),
            dma((2,)),
        ],
    )(block_counts, pack_order, decode_slot, landed)
    return attended, cache_keys, cache_values


def solution(mesh):
    rows = P(("groups", "seq"), None)
    small = P("groups")
    cache = P(("groups", "seq"), None, None, None)
    return jax.shard_map(
        functools.partial(local, mesh.shape["seq"]),
        mesh=mesh,
        in_specs=(rows, rows, rows, small, small, small, small),
        out_specs=(rows, cache, cache),
        check_vma=False,
    )
```

```python
import functools
import math

import jax
import jax.numpy as jnp
from jax import lax
from jax.experimental import pallas as pl
from jax.experimental.pallas import tpu as pltpu
from jax.sharding import PartitionSpec as P

HEADS = 16
HEAD_DIM = 128
BLOCK = 128
MAXB = 6
BACK = MAXB - 1
HIDDEN = -1e30
PLANE = 4
CHUNKS = 4
RELAY = BACK
ROUND = 2
NEAR = 2
FEW = MAXB - NEAR - 1


def window_tables(counts_ref, tails_ref, order_ref, first, width):
    pairs = counts_ref.shape[0]
    prompts = order_ref.shape[0]

    def place(i, carry):
        start, docs, valids = carry
        prompt = order_ref[i]
        counted = counts_ref[lax.rem(prompt, pairs)]
        size = jnp.where(prompt < pairs, counted, 1)
        tail = tails_ref[prompt]
        end = start + size
        new_docs, new_valids = [], []
        for w in range(width):
            b = first + w
            inside = (start <= b) & (b < end)
            new_docs.append(jnp.where(inside, i, docs[w]))
            new_valids.append(
                jnp.where(inside, jnp.where(b + 1 == end, tail, BLOCK), valids[w])
            )
        return end, tuple(new_docs), tuple(new_valids)

    none = jnp.int32(-1)
    zero = jnp.int32(0)
    _, docs, valids = lax.fori_loop(
        0, prompts, place, (zero, (none,) * width, (zero,) * width)
    )
    return docs, valids


def exchange(
    n,
    counts_ref,
    tails_ref,
    order_ref,
    q_hbm,
    k_hbm,
    v_hbm,
    out_ref,
    landed_ref,
    q_ref,
    own,
    halo,
    relay,
    bias,
    halo_send,
    halo_recv,
    cache_sem,
    own_sem,
    load_sem,
):
    me = lax.axis_index("seq")
    role = lax.rem(me, PLANE)
    plane = me // PLANE
    planes = n // PLANE
    tokens, features = q_ref.shape
    here = tokens // BLOCK
    splits = n // HEADS
    part = BLOCK // splits
    wide = features // CHUNKS

    loads = [
        pltpu.make_async_copy(src, dst, load_sem.at[i])
        for i, (src, dst) in enumerate(
            ((k_hbm, own.at[0]), (v_hbm, own.at[1]), (q_hbm, q_ref))
        )
    ]
    for copy in loads:
        copy.start()

    barrier = pltpu.get_barrier_semaphore()

    def greet(r, carry):
        pl.semaphore_signal(
            barrier,
            inc=1,
            device_id={"seq": lax.rem(me + r, n)},
            device_id_type=pl.DeviceIdType.MESH,
        )
        return carry

    lax.fori_loop(1, n, greet, 0)
    loads[0].wait()
    loads[1].wait()
    pl.semaphore_wait(barrier, n - 1)

    pending = []

    def spot(block, c):
        return (
            slice(None),
            pl.ds(block * BLOCK, BLOCK),
            pl.ds(c * wide, wide),
        )

    def mine(block):
        return lambda c: own.at[spot(block, c)]

    def held(slot):
        if slot >= RELAY:
            return lambda c: relay.at[spot(slot - RELAY, c)]
        return lambda c: halo.at[spot(slot, c)]

    def start(cond, c, moves):
        copies = []
        for src, target, slot in moves:
            copy = pltpu.make_async_remote_copy(
                src_ref=src(c),
                dst_ref=held(slot)(c),
                send_sem=halo_send.at[len(pending)],
                recv_sem=halo_recv.at[slot, c],
                device_id={"seq": lax.rem(target + n, n)},
                device_id_type=pl.DeviceIdType.MESH,
            )
            pending.append((cond, copy))
            copies.append(copy)

        @pl.when(cond)
        def _():
            for copy in copies:
                copy.start()

    def await_slots(cond, c, slots):
        @pl.when(cond)
        def _():
            for slot in slots:
                ref = held(slot)(c)
                pltpu.make_async_copy(ref, ref, halo_recv.at[slot, c]).wait()

    more = plane < planes - 1
    late = plane > 0
    for c in range(CHUNKS):
        start((role == 3) & more, c, [(mine(0), me + 3, RELAY), (mine(1), me + 3, 0)])
        if c < ROUND:
            moves = [(mine(1), me - 2, RELAY + 1), (mine(0), me - 2, RELAY)]
        else:
            moves = [(mine(1), me + 2, 2), (mine(0), me + 2, 1)]
        start((role == 2) & more, c, moves)
        start((role == 1) & more, c, [(mine(1), me + 3, 0)])
        start(role == 1, c, [(mine(0), me + 1, 3), (mine(1), me + 1, 4)])
        start(role == 0, c, [(mine(1), me + 2, 2), (mine(0), me + 2, 1)])
        start(
            (role == 0) | (role == 2),
            c,
            [(mine(0), me + 1, 3), (mine(1), me + 1, 4)],
        )

    def piece(owner, block):
        head = owner // splits
        cols = pl.ds(pl.multiple_of(head * HEAD_DIM, HEAD_DIM), HEAD_DIM)
        if splits == 1:
            return own.at[:, :, cols]
        offset = pl.multiple_of(block * BLOCK + lax.rem(owner, splits) * part, part)
        return own.at[:, pl.ds(offset, part), cols]

    def place(block):
        if splits == 1:
            return landed_ref.at[:, pl.ds(pl.multiple_of(me * tokens, tokens), tokens)]
        return landed_ref.at[
            :, pl.ds(pl.multiple_of((me * here + block) * part, part), part)
        ]

    pieces = 1 if splits == 1 else here

    def give(s, carry):
        sign = 1 - 2 * lax.rem(s, 2)
        target = lax.rem(me + n // 2 + sign * ((s + 1) // 2), n)
        for block in range(pieces):
            pltpu.make_async_remote_copy(
                src_ref=piece(target, block),
                dst_ref=place(block),
                send_sem=cache_sem.at[0],
                recv_sem=cache_sem.at[1],
                device_id={"seq": target},
                device_id_type=pl.DeviceIdType.MESH,
            ).start()
        return carry

    cuts = [(n - 1) * i // CHUNKS for i in range(CHUNKS + 1)]

    docs, valids = window_tables(
        counts_ref, tails_ref, order_ref, me * here - BACK, BACK + here
    )
    row = lax.broadcasted_iota(jnp.int32, (BLOCK, BLOCK), 0)
    col = lax.broadcasted_iota(jnp.int32, (BLOCK, BLOCK), 1)
    for b in range(here):
        for w in range(BACK + here):
            if w > BACK + b:
                shade = jnp.full((BLOCK, BLOCK), HIDDEN, jnp.float32)
            else:
                limit = jnp.where(docs[w] == docs[BACK + b], valids[w], 0)
                seen = col < limit
                if w == BACK + b:
                    seen = seen & (col <= row)
                shade = jnp.where(seen, 0.0, HIDDEN)
            bias[b * BLOCK : (b + 1) * BLOCK, w * BLOCK : (w + 1) * BLOCK] = shade
    column = lax.broadcasted_iota(jnp.int32, (BLOCK, HEAD_DIM), 0)
    real = jnp.concatenate(
        [column < valids[BACK + b] for b in range(here)], axis=0
    )

    empty = jnp.zeros((BLOCK, features), halo.dtype)
    for slot, reach in ((0, 3), (1, 2), (2, 2), (3, 1), (4, 1)):

        @pl.when(me < reach)
        def _():
            for kv in range(2):
                halo[kv, slot * BLOCK : (slot + 1) * BLOCK, :] = empty

    loads[2].wait()

    factor = HEAD_DIM ** (-0.5) * math.log2(math.e)
    prior = BACK * BLOCK
    nt = (((1,), (1,)), ((), ()))

    def one_head(h, carry):
        cols = pl.ds(pl.multiple_of(h * HEAD_DIM, HEAD_DIM), HEAD_DIM)
        q = q_ref[:, cols]
        s1 = lax.dot_general(q, halo[0, :, cols], nt, preferred_element_type=jnp.float32)
        s2 = lax.dot_general(q, own[0, :, cols], nt, preferred_element_type=jnp.float32)
        s1 = s1 + bias[:, :prior]
        s2 = s2 + bias[:, prior:]
        peak = jnp.maximum(
            jnp.max(s1, axis=1, keepdims=True), jnp.max(s2, axis=1, keepdims=True)
        )
        w1 = jnp.exp2((s1 - peak) * factor)
        w2 = jnp.exp2((s2 - peak) * factor)
        total = jnp.sum(w1, axis=1, keepdims=True) + jnp.sum(w2, axis=1, keepdims=True)
        mixed = jnp.dot(
            w1.astype(jnp.bfloat16), halo[1, :, cols], preferred_element_type=jnp.float32
        ) + jnp.dot(
            w2.astype(jnp.bfloat16), own[1, :, cols], preferred_element_type=jnp.float32
        )
        out_ref[:, cols] = jnp.where(real, mixed / total, 0.0).astype(out_ref.dtype)
        return carry

    for c in range(CHUNKS):
        lax.fori_loop(cuts[c], cuts[c + 1], give, 0)
        if c < ROUND:
            await_slots((role == 0) & more, c, [RELAY, RELAY + 1])
            start(
                (role == 0) & more,
                c,
                [(held(RELAY + 1), me + PLANE, 2), (held(RELAY), me + PLANE, 1)],
            )
        await_slots((role == 2) & late, c, [RELAY, 0])
        start(
            (role == 2) & late, c, [(held(RELAY), me - 2 + n, 3), (held(0), me - 2 + n, 4)]
        )
        await_slots((role == 0) & late, c, [2, 3, 4])
        await_slots(role == 2, c, [2, 3, 4])
        start(
            (role == 2) | ((role == 0) & late),
            c,
            [(held(2), me + 1, 0), (held(3), me + 1, 1), (held(4), me + 1, 2)],
        )
        await_slots((role == 0) & late, c, [0, 1])
        await_slots(role == 1, c, [3, 4])
        await_slots((role == 1) & late, c, [0, 1, 2])
        await_slots(role == 2, c, [1])
        await_slots(role == 3, c, [0, 1, 2, 3, 4])
        each = HEADS // CHUNKS
        lax.fori_loop(c * each, (c + 1) * each, one_head, 0)

    copies = [
        pltpu.make_async_copy(piece(me, block), place(block), own_sem.at[block])
        for block in range(pieces)
    ]
    for copy in copies:
        copy.start()

    for cond, copy in pending:

        @pl.when(cond)
        def _():
            copy.wait_send()

    for copy in copies:
        copy.wait()
    others = landed_ref.shape[1] // n * (n - 1)
    ref = landed_ref.at[:, pl.ds(0, others)]
    pltpu.make_async_copy(ref, ref, cache_sem.at[0]).wait()
    pltpu.make_async_copy(ref, ref, cache_sem.at[1]).wait()


def decode_places(counts_ref, order_ref, slot_ref, who, base, put):
    pairs = counts_ref.shape[0]
    prompts = order_ref.shape[0]

    def invert(p, carry):
        who[slot_ref[p]] = p
        return carry

    lax.fori_loop(0, pairs, invert, 0)

    def lay(s, first):
        p = who[s]
        base[p] = first
        return first + counts_ref[p] + 1

    lax.fori_loop(0, pairs, lay, jnp.int32(0))

    def fetch(i, first):
        prompt = order_ref[i]
        pair = lax.rem(prompt, pairs)
        null = prompt >= pairs
        counted = counts_ref[pair]
        size = jnp.where(null, 1, counted)
        target = base[pair] + jnp.where(null, counted, 0)

        def one(w, carry):
            put(first + w, target + w)
            return carry

        lax.fori_loop(0, size, one, 0)
        return first + size

    lax.fori_loop(0, prompts, fetch, jnp.int32(0))


def reorder(
    counts_ref,
    order_ref,
    slot_ref,
    landed_ref,
    keys_ref,
    values_ref,
    staged,
    who,
    base,
    in_sem,
    out_sem,
):
    part = staged.shape[2]

    def put(source, target):
        for kv in range(2):
            pltpu.make_async_copy(
                landed_ref.at[kv, pl.ds(source * part, part)],
                staged.at[kv, target],
                in_sem.at[kv],
            ).start()

    decode_places(counts_ref, order_ref, slot_ref, who, base, put)
    outs = []
    for kv, ref in enumerate((keys_ref, values_ref)):
        pltpu.make_async_copy(staged.at[kv], staged.at[kv], in_sem.at[kv]).wait()
        copy = pltpu.make_async_copy(staged.at[kv], ref.at[0], out_sem.at[kv])
        copy.start()
        outs.append(copy)
    for copy in outs:
        copy.wait()


def publish(places_ref, landed_ref, mixed_ref, attended_ref, keys_ref, values_ref, out_sem):
    leave = pltpu.make_async_copy(mixed_ref, attended_ref, out_sem.at[2])
    leave.start()
    refs = (keys_ref, values_ref)
    part = keys_ref.shape[2]

    def put(b, carry):
        for kv, ref in enumerate(refs):
            pltpu.make_async_copy(
                landed_ref.at[kv, pl.ds(pl.multiple_of(b * part, part), part)],
                ref.at[0, places_ref[b]],
                out_sem.at[kv],
            ).start()
        return carry

    lax.fori_loop(0, places_ref.shape[0], put, 0)
    leave.wait()
    for kv, ref in enumerate(refs):
        pltpu.make_async_copy(ref.at[0], ref.at[0], out_sem.at[kv]).wait()


def handoff(
    n,
    counts_hbm,
    tails_hbm,
    order_hbm,
    slot_hbm,
    q_hbm,
    k_hbm,
    v_hbm,
    out_ref,
    landed_ref,
    places_ref,
    counts_ref,
    tails_ref,
    order_ref,
    slot_ref,
    q_ref,
    own,
    kv,
    qs,
    mixed_ref,
    bias,
    lower_q,
    lower_bias,
    slot_out,
    size_out,
    size_in,
    small_sem,
    load_sem,
    local_sem,
    kv_send,
    kv_recv,
    q_send,
    q_recv,
    halo_send,
    halo_recv,
    land_send,
    land_recv,
    out_send,
    out_recv,
    down_send,
    down_recv,
    up_send,
    up_recv,
):
    me = lax.axis_index("seq")
    role = lax.rem(me, PLANE)
    plane = me // PLANE
    planes = n // PLANE
    tokens, features = q_ref.shape
    here = tokens // BLOCK
    width = PLANE * here
    skip = width - BACK
    reach = BACK * BLOCK
    few_rows = FEW * BLOCK
    far_rows = (BACK - NEAR) * BLOCK
    peers = (role + 1 - 2 * lax.rem(role, 2), lax.rem(role + 2, PLANE), PLANE - 1 - role)
    more = plane < planes - 1
    late = plane > 0
    base = plane * PLANE
    last = planes - 1
    orders = []
    for p in range(planes):
        above = list(range(last, p, -1))
        helping = [j for j in range(p + 1) if 2 * j < planes and 2 * p >= planes - 2]
        rest = [j for j in range(p, -1, -1) if j not in helping]
        if p == last:
            above, helping, rest = [last - 1], list(range(last - 1)), [last]
        orders.append(above + helping + rest)
    def one_if(i, value):
        return (i + planes - value) // planes - (i + planes - value - 1) // planes

    picks = [
        sum(orders[p][t] * one_if(plane, p) for p in range(planes)) for t in range(planes)
    ]

    def turn(t):
        return sum(picks[other] * one_if(t, other) for other in range(planes))

    def hold(j):
        return ((plane == last) & (j < plane - 1)) | ((plane == 0) & (j < planes // 2))

    def back(j, p):
        return (j <= p) & (2 * j < planes) & (2 * p >= planes - 2)

    helpable = [j for j in range(last) if 2 * j < planes]

    def helps(j):
        return more & back(j, plane)

    def helped(j):
        return late & back(j, plane - 1)

    def each(body):
        def step(t, carry):
            body(turn(t))
            return carry

        lax.fori_loop(0, planes, step, 0)

    def rows(first, count):
        return pl.ds(pl.multiple_of(first * BLOCK, BLOCK), count * BLOCK)

    def cols(head):
        return pl.ds(pl.multiple_of(head * HEAD_DIM, HEAD_DIM), HEAD_DIM)

    def remote(src, dst, send, recv, target):
        pltpu.make_async_remote_copy(
            src_ref=src,
            dst_ref=dst,
            send_sem=send,
            recv_sem=recv,
            device_id={"seq": target},
            device_id_type=pl.DeviceIdType.MESH,
        ).start()

    def await_(ref, sem):
        pltpu.make_async_copy(ref, ref, sem).wait()

    mine = rows(BACK + role * here, here)
    place = rows(role * here, here)

    loads = [
        pltpu.make_async_copy(src, dst, load_sem.at[i])
        for i, (src, dst) in enumerate(
            ((k_hbm, own.at[0]), (v_hbm, own.at[1]), (q_hbm, q_ref))
        )
    ]
    barrier = pltpu.get_barrier_semaphore()
    for peer in peers:
        pl.semaphore_signal(
            barrier,
            inc=1,
            device_id={"seq": base + peer},
            device_id_type=pl.DeviceIdType.MESH,
        )
    for step in range(1, planes):
        pl.semaphore_signal(
            barrier,
            inc=1,
            device_id={"seq": lax.rem(me + step * PLANE, n)},
            device_id_type=pl.DeviceIdType.MESH,
        )
    for j in range(planes):
        here_cols = cols(j * PLANE + role)
        for i, src in enumerate((k_hbm, v_hbm)):
            pltpu.make_async_copy(
                src.at[:, here_cols], kv.at[j, i, mine], local_sem.at[0]
            ).start()
    for load in loads:
        load.start()
    smalls = [
        pltpu.make_async_copy(src, dst, small_sem.at[i])
        for i, (src, dst) in enumerate(
            (
                (counts_hbm, counts_ref),
                (tails_hbm, tails_ref),
                (order_hbm, order_ref),
                (slot_hbm, slot_ref),
            )
        )
    ]
    for small in smalls:
        small.start()
    for j in range(planes):
        here_cols = cols(j * PLANE + role)
        pltpu.make_async_copy(
            q_hbm.at[:, here_cols], qs.at[j, place], local_sem.at[1]
        ).start()

    for j in range(planes):

        @pl.when(helped(j))
        def _():
            for i in range(2):
                kv[j, i, :far_rows, :] = jnp.zeros((far_rows, HEAD_DIM), kv.dtype)

        @pl.when(plane == 0)
        def _():
            for i in range(2):
                kv[j, i, :reach, :] = jnp.zeros((reach, HEAD_DIM), kv.dtype)

    def share(j):
        for k in (1, 2, 0):
            remote(
                own.at[:, :, cols(j * PLANE + peers[k])],
                kv.at[j, :, mine],
                kv_send.at[0],
                kv_recv.at[k, j],
                base + peers[k],
            )

    def share_q(early):
        def body(j):
            soon = helped(j) & (role * here < FEW)

            @pl.when(soon if early else jnp.logical_not(soon))
            def _():
                for k in (1, 2, 0):
                    remote(
                        q_ref.at[:, cols(j * PLANE + peers[k])],
                        qs.at[j, place],
                        q_send.at[0],
                        q_recv.at[k, j],
                        base + peers[k],
                    )

        return body

    def when_helped(body, truth):
        def step(j):
            @pl.when(helped(j) if truth else jnp.logical_not(helped(j)))
            def _():
                body(j)

        return step

    def descend(body):
        def step(t, carry):
            body(last - t)
            return carry

        lax.fori_loop(0, planes, step, 0)

    def forward(j, rho):
        first = BACK + rho * here
        low = rho * here < skip
        high = rho * here + here > skip
        up = more & jnp.logical_not(helps(j))

        @pl.when(up & jnp.logical_not(low))
        def _():
            remote(
                kv.at[j, :, rows(first, here)],
                kv.at[j, :, rows(jnp.maximum(rho * here - skip, 0), here)],
                halo_send.at[j],
                halo_recv.at[j, rho],
                me + PLANE,
            )

        @pl.when(up & low & high)
        def _():
            remote(
                kv.at[j, :, rows(BACK + skip, BACK % here)],
                kv.at[j, :, rows(0, BACK % here)],
                halo_send.at[j],
                halo_recv.at[j, rho],
                me + PLANE,
            )

        @pl.when(late & (j > plane) & low & high)
        def _():
            remote(
                kv.at[j, :, rows(first, skip % here)],
                landed_ref.at[:, rows(plane * width + rho * here, skip % here)],
                land_send.at[1, j],
                land_recv.at[0],
                j * PLANE + role,
            )

        @pl.when(late & (j > plane) & jnp.logical_not(high))
        def _():
            remote(
                kv.at[j, :, rows(first, here)],
                landed_ref.at[:, rows(plane * width + rho * here, here)],
                land_send.at[1, j],
                land_recv.at[0],
                j * PLANE + role,
            )

        @pl.when(j < plane)
        def _():
            remote(
                kv.at[j, :, rows(first, here)],
                landed_ref.at[:, rows(plane * width + rho * here, here)],
                land_send.at[0, j],
                land_recv.at[0],
                j * PLANE + role,
            )

    def start_mine(j):
        @pl.when(jnp.logical_not(hold(j)))
        def _():
            forward(j, role)

    def take(k, j):
        await_(kv.at[j, :, rows(BACK + peers[k] * here, here)], kv_recv.at[k, j])

    def start_core(truth):
        def body(j):
            later = helped(j) & (j > 0)

            @pl.when(later if truth else jnp.logical_not(later))
            def _():
                take(0, j)

                @pl.when(jnp.logical_not(hold(j)))
                def _():
                    forward(j, peers[0])

        return body

    with jax.named_scope("enter_local"):
        await_(kv.at[:, :, mine], local_sem.at[0])
    with jax.named_scope("enter_barrier"):
        pl.semaphore_wait(barrier, PLANE - 1 + planes - 1)
    with jax.named_scope("start_mine"):
        each(start_mine)
    with jax.named_scope("enter_loads"):
        for load in loads:
            load.wait()
    with jax.named_scope("share"):
        each(share_q(True))
        each(share)
        descend(share_q(False))

    with jax.named_scope("take_core"):
        each(start_core(False))

    with jax.named_scope("tables"):
        for small in smalls:
            small.wait()
        docs, valids = window_tables(
            counts_ref, tails_ref, order_ref, plane * width - BACK, BACK + width + BACK
        )
        row = lax.broadcasted_iota(jnp.int32, (BLOCK, BLOCK), 0)
        col = lax.broadcasted_iota(jnp.int32, (BLOCK, BLOCK), 1)
        hidden = jnp.full((BLOCK, BLOCK), HIDDEN, jnp.float32)

        def near(first):
            return docs[first] != docs[first - NEAR - 1]

        def shade(source, target, shown=True):
            same = (docs[source] == docs[target]) & shown
            limit = jnp.where(same, valids[source], 0)
            seen = col < limit
            if source == target:
                seen = seen & (col <= row)
            return jnp.where(seen, 0.0, HIDDEN)

        for i in range(PLANE):
            for b in range(here):
                target = BACK + i * here + b
                for w in range(BACK + here):
                    source = i * here + w
                    spot = (slice(b * BLOCK, (b + 1) * BLOCK), slice(w * BLOCK, (w + 1) * BLOCK))
                    full = hidden if source > target else shade(source, target)
                    bias[(0, i) + spot] = full
                    if source < BACK - NEAR:
                        bias[(1, i) + spot] = hidden
                    elif source < BACK and source <= target:
                        bias[(1, i) + spot] = shade(source, target, near(BACK))
                    else:
                        bias[(1, i) + spot] = full
        for g in range(FEW):
            for c in range(BACK):
                lower_bias[g * BLOCK : (g + 1) * BLOCK, c * BLOCK : (c + 1) * BLOCK] = shade(
                    BACK + skip + c, BACK + width + g
                )
        column = lax.broadcasted_iota(jnp.int32, (BLOCK, HEAD_DIM), 0)

    def await_q(j, early):
        for k in range(PLANE - 1):
            soon = helped(j) & (peers[k] * here < FEW)

            @pl.when(soon if early else jnp.logical_not(soon))
            def _():
                await_(qs.at[j, rows(peers[k] * here, here)], q_recv.at[k, j])

    await_(qs.at[:, place], local_sem.at[1])

    def lower(j):
        await_q(j, True)
        remote(
            qs.at[j, pl.ds(0, few_rows)],
            lower_q.at[j],
            down_send.at[j],
            down_recv.at[j],
            me - PLANE,
        )

    with jax.named_scope("lower_q"):
        for h in helpable:

            @pl.when(helped(h))
            def _():
                lower(h)

    each(start_core(True))

    def await_halo(j):
        for rho in range(PLANE):
            count = min(here, (rho + 1) * here - skip)
            if count > 0:
                await_(
                    kv.at[j, :, rows(max(rho * here - skip, 0), count)],
                    halo_recv.at[j, rho],
                )

    below = rows(jnp.maximum(plane * width - BACK, 0), BACK)

    def relay(j):
        @pl.when(late & (j > plane))
        def _():
            await_halo(j)
            remote(
                kv.at[j, :, rows(0, BACK)],
                landed_ref.at[:, below],
                land_send.at[2, j],
                land_recv.at[0],
                j * PLANE + role,
            )

    def map_places():
        pairs = counts_ref.shape[0]
        blocks = places_ref.shape[0]

        def empty(b, carry):
            places_ref[b] = 0
            return carry

        lax.fori_loop(0, blocks, empty, 0)

        def fill(i, first):
            prompt = order_ref[i]
            pair = lax.rem(prompt, pairs)
            null = prompt >= pairs
            counted = counts_ref[pair]
            end = first + jnp.where(null, 1, counted)
            slot = slot_ref[pair]

            def earlier(p, total):
                return total + jnp.where(slot_ref[p] < slot, counts_ref[p] + 1, 0)

            target = lax.fori_loop(0, pairs, earlier, jnp.where(null, counted, 0)) - first

            def mark(chunk, carry):
                for step in range(8):
                    b = chunk * 8 + step
                    inside = (first <= b) & (b < end)
                    places_ref[b] = jnp.where(inside, target + b, places_ref[b])
                return carry

            lax.fori_loop(0, blocks // 8, mark, 0)
            return end

        lax.fori_loop(0, order_ref.shape[0], fill, jnp.int32(0))

    factor = HEAD_DIM ** (-0.5) * math.log2(math.e)
    nt = (((1,), (1,)), ((), ()))
    span = (BACK + here) * BLOCK

    def soften(q, k, v, mask):
        s = lax.dot_general(q, k, nt, preferred_element_type=jnp.float32) + mask
        peak = jnp.max(s, axis=1, keepdims=True)
        w = jnp.exp2((s - peak) * factor)
        total = jnp.sum(w, axis=1, keepdims=True)
        mixed = jnp.dot(w.astype(jnp.bfloat16), v, preferred_element_type=jnp.float32)
        return mixed, peak * factor, total

    def help_out(j):
        await_(lower_q.at[j], down_recv.at[j])
        send_near = near(BACK + width)
        for first in range(0, FEW, here):
            count = min(here, FEW - first)
            lines = slice(first * BLOCK, (first + count) * BLOCK)
            window = pl.ds((BACK + skip + first) * BLOCK, (BACK - first) * BLOCK)
            mixed, peak, total = soften(
                lower_q[j, lines, :],
                kv[j, 0, window, :],
                kv[j, 1, window, :],
                lower_bias[lines, first * BLOCK :],
            )
            size = jnp.broadcast_to(peak + jnp.log2(total), (count * BLOCK, BLOCK))
            for b in range(count):
                g = first + b
                turned = size[b * BLOCK : (b + 1) * BLOCK].T
                size_out[j, g] = jnp.where(send_near, HIDDEN, turned[:8])
            mixed = (mixed / total).astype(slot_out.dtype)
            for b in range(count):
                side, line = divmod(first + b, NEAR)
                spot = pl.ds(line * BLOCK, BLOCK)
                block = kv[j, side, pl.ds((BACK + width - NEAR + line) * BLOCK, BLOCK), :]
                slot_out[j, side, spot, :] = jnp.where(
                    send_near, block, mixed[b * BLOCK : (b + 1) * BLOCK]
                )
        for g in range(FEW, 2 * NEAR):
            side, line = divmod(g, NEAR)
            slot_out[j, side, pl.ds(line * BLOCK, BLOCK), :] = kv[
                j, side, pl.ds((BACK + width - NEAR + line) * BLOCK, BLOCK), :
            ]

    def send_up(j):
        remote(
            slot_out.at[j],
            kv.at[j, :, rows(BACK - NEAR, NEAR)],
            up_send.at[0, j],
            up_recv.at[0, j],
            me + PLANE,
        )
        remote(size_out.at[j], size_in.at[j], up_send.at[1, j], up_recv.at[1, j], me + PLANE)

    def release(j):
        @pl.when(hold(j))
        def _():
            forward(j, role)
            forward(j, peers[0])

    def far(t, carry):
        j = turn(t)
        with jax.named_scope("take_far"):
            for k in (1, 2):
                take(k, j)
                forward(j, peers[k])

        @pl.when(t == min(1, last))
        def _():
            each(release)

        for h in helpable:

            @pl.when(helps(h) & (j == h))
            def _():
                with jax.named_scope("help_out"):
                    help_out(h)

        for h in helpable:

            @pl.when(helps(h) & (j == h))
            def _():
                send_up(h)

        return carry

    lax.fori_loop(0, planes, far, 0)

    def climb(j, carry):
        @pl.when((plane == 0) & (j > 0))
        def _():
            remote(
                kv.at[j, :, rows(BACK, skip)],
                landed_ref.at[:, rows(0, skip)],
                land_send.at[1, j],
                land_recv.at[0],
                j * PLANE + role,
            )

        return carry

    lax.fori_loop(0, planes, climb, 0)

    with jax.named_scope("relay"):
        descend(relay)

    settle = pltpu.make_async_copy(
        kv.at[plane, :, rows(BACK, width)],
        landed_ref.at[:, rows(plane * width, width)],
        load_sem.at[0],
    )
    settle.start()

    def attend(j, i, variant):
        window = pl.ds(i * tokens, span)
        return soften(
            qs[j, pl.ds(i * tokens, tokens), :],
            kv[j, 0, window, :],
            kv[j, 1, window, :],
            bias[variant, i],
        )

    def finish(j, i, mixed, total):
        real = jnp.concatenate(
            [column < valids[BACK + i * here + b] for b in range(here)], axis=0
        )
        mixed_ref[j, i] = jnp.where(real, mixed / total, 0.0).astype(mixed_ref.dtype)

    def simple(j, i):
        mixed, _, total = attend(j, i, 0)
        finish(j, i, mixed, total)

    def give(j, i):
        target = out_ref.at[:, cols(j * PLANE + role)]

        @pl.when(role == i)
        def _():
            pltpu.make_async_copy(mixed_ref.at[j, i], target, local_sem.at[2]).start()

        @pl.when(role != i)
        def _():
            remote(mixed_ref.at[j, i], target, out_send.at[0], out_recv.at[0], base + i)

    top = PLANE - 1

    def own_blocks(t, carry):
        j = last - t
        with jax.named_scope("wait_q"):
            await_q(j, False)

        with jax.named_scope("top"):
            simple(j, top)

            @pl.when(t > 0)
            def _():
                give(jnp.minimum(j + 1, last), top)

        return carry

    lax.fori_loop(0, planes, own_blocks, 0)

    def reach_back(j):
        with jax.named_scope("wait_halo"):

            @pl.when(late & (j <= plane))
            def _():
                await_halo(j)

        with jax.named_scope("units"):
            for i in range(top - 1, -1, -1):
                simple(j, i)
                if i == top - 1:

                    @pl.when(j == last)
                    def _():
                        give(0, top)

                    @pl.when(j < last)
                    def _():
                        give(jnp.minimum(j + 1, last), 0)

                else:
                    give(j, i + 1)

    descend(when_helped(reach_back, False))

    settled = pltpu.make_async_copy(
        kv.at[plane, :, rows(0, BACK)], landed_ref.at[:, below], load_sem.at[1]
    )

    @pl.when(late)
    def _():
        settled.start()

    for j in range(planes):
        first = jnp.logical_not(helped(j))

        @pl.when(first & helped(j - 1) if j else first)
        def _():
            give(j, 0)

    def merge(j):
        with jax.named_scope("wait_part"):
            await_(kv.at[j, :, rows(BACK - NEAR, NEAR)], up_recv.at[0, j])
            await_(size_in.at[j], up_recv.at[1, j])
        with jax.named_scope("merge"):
            for i in range(top - 1, -1, -1):
                mixed, peak, total = attend(j, i, 1)
                mixed = [mixed[b * BLOCK : (b + 1) * BLOCK] for b in range(here)]
                total = [
                    jnp.broadcast_to(total[b * BLOCK : (b + 1) * BLOCK], (BLOCK, BLOCK))
                    for b in range(here)
                ]
                for b in range(here):
                    g = i * here + b
                    if g < FEW:
                        size = jnp.broadcast_to(size_in[j, g, :1], (BLOCK, BLOCK)).T
                        mark = peak[b * BLOCK : (b + 1) * BLOCK]
                        high = jnp.maximum(mark, size)
                        mine_share = jnp.exp2(mark - high)
                        their_share = jnp.exp2(size - high)
                        side, line = divmod(g, NEAR)
                        line = (BACK - NEAR + line) * BLOCK
                        theirs = kv[j, side, line : line + BLOCK, :]
                        mixed[b] = mixed[b] * mine_share + theirs.astype(jnp.float32) * their_share
                        total[b] = total[b] * mine_share + their_share
                finish(
                    j, i, jnp.concatenate(mixed, axis=0), jnp.concatenate(total, axis=0)
                )
                if i < top - 1:
                    give(j, i + 1)
        give(j, 0)

    for h in helpable:

        @pl.when(helped(h))
        def _():
            merge(h)

    with jax.named_scope("map_places"):
        map_places()

    with jax.named_scope("drain"):
        others = features // PLANE * (PLANE - 1)
        await_(own.at[:, :, pl.ds(0, others)], kv_send.at[0])
        await_(q_ref.at[:, pl.ds(0, others)], q_send.at[0])
        await_(q_ref.at[:, pl.ds(0, features // PLANE)], local_sem.at[2])

        def drain(j):
            @pl.when(more & jnp.logical_not(helps(j)))
            def _():
                await_(kv.at[j, :, rows(0, BACK)], halo_send.at[j])

            @pl.when(helps(j))
            def _():
                await_(slot_out.at[j], up_send.at[0, j])
                await_(size_out.at[j], up_send.at[1, j])

            @pl.when(helped(j))
            def _():
                await_(lower_q.at[j], down_send.at[j])

            @pl.when(j < plane)
            def _():
                await_(kv.at[j, :, rows(BACK, width)], land_send.at[0, j])

            @pl.when(j > plane)
            def _():
                await_(kv.at[j, :, rows(BACK, skip)], land_send.at[1, j])

            @pl.when(late & (j > plane))
            def _():
                await_(kv.at[j, :, rows(0, BACK)], land_send.at[2, j])

        each(drain)
        settle.wait()
        await_(q_ref.at[:, pl.ds(0, others)], out_send.at[0])
        await_(q_ref.at[:, pl.ds(0, others)], out_recv.at[0])

    with jax.named_scope("land"):

        @pl.when(late)
        def _():
            settled.wait()
            await_(landed_ref.at[:, rows(0, (planes - 1) * width - BACK)], land_recv.at[0])

        @pl.when(plane == 0)
        def _():
            await_(landed_ref.at[:, rows(0, (planes - 1) * width)], land_recv.at[0])


def wide_exchange(n, queries, keys, values, block_counts, last_tokens, pack_order):
    tokens, features = queries.shape
    here = tokens // BLOCK
    part = BLOCK // (n // HEADS)
    blocks = here * n
    kind = queries.dtype
    smem = pl.BlockSpec(memory_space=pltpu.SMEM)
    vmem = pl.BlockSpec(memory_space=pltpu.VMEM)
    anywhere = pl.BlockSpec(memory_space=pl.ANY)
    dma = pltpu.SemaphoreType.DMA
    return pl.pallas_call(
        functools.partial(exchange, n),
        out_shape=(
            jax.ShapeDtypeStruct((tokens, features), kind),
            jax.ShapeDtypeStruct((2, blocks * part, HEAD_DIM), kind),
        ),
        in_specs=[smem] * 3 + [anywhere] * 3,
        out_specs=(vmem, anywhere),
        scratch_shapes=[
            pltpu.VMEM((tokens, features), kind),
            pltpu.VMEM((2, tokens, features), kind),
            pltpu.VMEM((2, BACK * BLOCK, features), kind),
            pltpu.VMEM((2, 2 * BLOCK, features), kind),
            pltpu.VMEM((tokens, (BACK + here) * BLOCK), jnp.float32),
            dma((CHUNKS * 18,)),
            dma((BACK + 2, CHUNKS)),
            dma((2,)),
            dma((here,)),
            dma((3,)),
        ],
        compiler_params=pltpu.CompilerParams(
            collective_id=0, has_side_effects=True, vmem_limit_bytes=60 * 1024 * 1024
        ),
    )(block_counts, last_tokens, pack_order, queries, keys, values)


def local(n, queries, keys, values, block_counts, last_tokens, pack_order, decode_slot):
    tokens, features = queries.shape
    here = tokens // BLOCK
    splits = n // HEADS
    part = BLOCK // splits
    blocks = here * n
    kind = queries.dtype
    smem = pl.BlockSpec(memory_space=pltpu.SMEM)
    anywhere = pl.BlockSpec(memory_space=pl.ANY)
    dma = pltpu.SemaphoreType.DMA
    planes = n // PLANE
    few = FEW * BLOCK
    cache = jax.ShapeDtypeStruct((1, blocks, part, HEAD_DIM), kind)
    if splits == 1 and here == 2 and planes > 1:
        attended, landed, places = pl.pallas_call(
            functools.partial(handoff, n),
            out_shape=(
                pltpu.VMEM((tokens, features), kind),
                pltpu.VMEM((2, blocks * part, HEAD_DIM), kind),
                pltpu.SMEM((blocks,), jnp.int32),
            ),
            in_specs=[anywhere] * 7,
            out_specs=(anywhere, anywhere, smem),
            scratch_shapes=[
                pltpu.SMEM(block_counts.shape, jnp.int32),
                pltpu.SMEM(last_tokens.shape, jnp.int32),
                pltpu.SMEM(pack_order.shape, jnp.int32),
                pltpu.SMEM(decode_slot.shape, jnp.int32),
                pltpu.VMEM((tokens, features), kind),
                pltpu.VMEM((2, tokens, features), kind),
                pltpu.VMEM((planes, 2, (BACK + PLANE * here) * BLOCK, HEAD_DIM), kind),
                pltpu.VMEM((planes, PLANE * tokens, HEAD_DIM), kind),
                pltpu.VMEM((planes, PLANE, tokens, HEAD_DIM), kind),
                pltpu.VMEM((2, PLANE, tokens, (BACK + here) * BLOCK), jnp.float32),
                pltpu.VMEM((planes, few, HEAD_DIM), kind),
                pltpu.VMEM((few, BACK * BLOCK), jnp.float32),
                pltpu.VMEM((planes, 2, NEAR * BLOCK, HEAD_DIM), kind),
                pltpu.VMEM((planes, FEW, 8, BLOCK), jnp.float32),
                pltpu.VMEM((planes, FEW, 8, BLOCK), jnp.float32),
                dma((4,)),
                dma((3,)),
                dma((3,)),
                dma((1,)),
                dma((PLANE - 1, planes)),
                dma((1,)),
                dma((PLANE - 1, planes)),
                dma((planes,)),
                dma((planes, PLANE)),
                dma((3, planes)),
                dma((1,)),
                dma((1,)),
                dma((1,)),
                dma((planes,)),
                dma((planes,)),
                dma((2, planes)),
                dma((2, planes)),
            ],
            compiler_params=pltpu.CompilerParams(
                collective_id=0, has_side_effects=True, vmem_limit_bytes=60 * 1024 * 1024
            ),
        )(block_counts, last_tokens, pack_order, decode_slot, queries, keys, values)
        return pl.pallas_call(
            publish,
            out_shape=(jax.ShapeDtypeStruct((tokens, features), kind), cache, cache),
            in_specs=[smem] + [anywhere] * 2,
            out_specs=(anywhere,) * 3,
            scratch_shapes=[dma((3,))],
        )(
            pltpu.with_memory_space_constraint(places, pltpu.SMEM),
            pltpu.with_memory_space_constraint(landed, pltpu.VMEM),
            pltpu.with_memory_space_constraint(attended, pltpu.VMEM),
        )
    attended, landed = wide_exchange(
        n, queries, keys, values, block_counts, last_tokens, pack_order
    )
    cache_keys, cache_values = pl.pallas_call(
        reorder,
        out_shape=(cache, cache),
        in_specs=[smem] * 3 + [anywhere],
        out_specs=(anywhere, anywhere),
        scratch_shapes=[
            pltpu.VMEM((2, blocks, part, HEAD_DIM), kind),
            pltpu.SMEM(block_counts.shape, jnp.int32),
            pltpu.SMEM(block_counts.shape, jnp.int32),
            dma((2,)),
            dma((2,)),
        ],
    )(block_counts, pack_order, decode_slot, landed)
    return attended, cache_keys, cache_values


def solution(mesh):
    rows = P(("groups", "seq"), None)
    small = P("groups")
    cache = P(("groups", "seq"), None, None, None)
    return jax.shard_map(
        functools.partial(local, mesh.shape["seq"]),
        mesh=mesh,
        in_specs=(rows, rows, rows, small, small, small, small),
        out_specs=(rows, cache, cache),
        check_vma=False,
    )
```

```python
import functools
import math

import jax
import jax.numpy as jnp
from jax import lax
from jax.experimental import pallas as pl
from jax.experimental.pallas import tpu as pltpu
from jax.sharding import PartitionSpec as P

HEADS = 16
HEAD_DIM = 128
BLOCK = 128
MAXB = 6
BACK = MAXB - 1
HIDDEN = -1e30
PLANE = 4
CHUNKS = 4
RELAY = BACK
ROUND = 2
NEAR = 2
FEW = MAXB - NEAR - 1


def window_tables(counts_ref, tails_ref, order_ref, first, width):
    pairs = counts_ref.shape[0]
    prompts = order_ref.shape[0]

    def place(i, carry):
        start, docs, valids = carry
        prompt = order_ref[i]
        counted = counts_ref[lax.rem(prompt, pairs)]
        size = jnp.where(prompt < pairs, counted, 1)
        tail = tails_ref[prompt]
        end = start + size
        new_docs, new_valids = [], []
        for w in range(width):
            b = first + w
            inside = (start <= b) & (b < end)
            new_docs.append(jnp.where(inside, i, docs[w]))
            new_valids.append(
                jnp.where(inside, jnp.where(b + 1 == end, tail, BLOCK), valids[w])
            )
        return end, tuple(new_docs), tuple(new_valids)

    none = jnp.int32(-1)
    zero = jnp.int32(0)
    _, docs, valids = lax.fori_loop(
        0, prompts, place, (zero, (none,) * width, (zero,) * width)
    )
    return docs, valids


def exchange(
    n,
    counts_ref,
    tails_ref,
    order_ref,
    q_hbm,
    k_hbm,
    v_hbm,
    out_ref,
    landed_ref,
    q_ref,
    own,
    halo,
    relay,
    bias,
    halo_send,
    halo_recv,
    cache_sem,
    own_sem,
    load_sem,
):
    me = lax.axis_index("seq")
    role = lax.rem(me, PLANE)
    plane = me // PLANE
    planes = n // PLANE
    tokens, features = q_ref.shape
    here = tokens // BLOCK
    splits = n // HEADS
    part = BLOCK // splits
    wide = features // CHUNKS

    loads = [
        pltpu.make_async_copy(src, dst, load_sem.at[i])
        for i, (src, dst) in enumerate(
            ((k_hbm, own.at[0]), (v_hbm, own.at[1]), (q_hbm, q_ref))
        )
    ]
    for copy in loads:
        copy.start()

    barrier = pltpu.get_barrier_semaphore()

    def greet(r, carry):
        pl.semaphore_signal(
            barrier,
            inc=1,
            device_id={"seq": lax.rem(me + r, n)},
            device_id_type=pl.DeviceIdType.MESH,
        )
        return carry

    lax.fori_loop(1, n, greet, 0)
    loads[0].wait()
    loads[1].wait()
    pl.semaphore_wait(barrier, n - 1)

    pending = []

    def spot(block, c):
        return (
            slice(None),
            pl.ds(block * BLOCK, BLOCK),
            pl.ds(c * wide, wide),
        )

    def mine(block):
        return lambda c: own.at[spot(block, c)]

    def held(slot):
        if slot >= RELAY:
            return lambda c: relay.at[spot(slot - RELAY, c)]
        return lambda c: halo.at[spot(slot, c)]

    def start(cond, c, moves):
        copies = []
        for src, target, slot in moves:
            copy = pltpu.make_async_remote_copy(
                src_ref=src(c),
                dst_ref=held(slot)(c),
                send_sem=halo_send.at[len(pending)],
                recv_sem=halo_recv.at[slot, c],
                device_id={"seq": lax.rem(target + n, n)},
                device_id_type=pl.DeviceIdType.MESH,
            )
            pending.append((cond, copy))
            copies.append(copy)

        @pl.when(cond)
        def _():
            for copy in copies:
                copy.start()

    def await_slots(cond, c, slots):
        @pl.when(cond)
        def _():
            for slot in slots:
                ref = held(slot)(c)
                pltpu.make_async_copy(ref, ref, halo_recv.at[slot, c]).wait()

    more = plane < planes - 1
    late = plane > 0
    for c in range(CHUNKS):
        start((role == 3) & more, c, [(mine(0), me + 3, RELAY), (mine(1), me + 3, 0)])
        if c < ROUND:
            moves = [(mine(1), me - 2, RELAY + 1), (mine(0), me - 2, RELAY)]
        else:
            moves = [(mine(1), me + 2, 2), (mine(0), me + 2, 1)]
        start((role == 2) & more, c, moves)
        start((role == 1) & more, c, [(mine(1), me + 3, 0)])
        start(role == 1, c, [(mine(0), me + 1, 3), (mine(1), me + 1, 4)])
        start(role == 0, c, [(mine(1), me + 2, 2), (mine(0), me + 2, 1)])
        start(
            (role == 0) | (role == 2),
            c,
            [(mine(0), me + 1, 3), (mine(1), me + 1, 4)],
        )

    def piece(owner, block):
        head = owner // splits
        cols = pl.ds(pl.multiple_of(head * HEAD_DIM, HEAD_DIM), HEAD_DIM)
        if splits == 1:
            return own.at[:, :, cols]
        offset = pl.multiple_of(block * BLOCK + lax.rem(owner, splits) * part, part)
        return own.at[:, pl.ds(offset, part), cols]

    def place(block):
        if splits == 1:
            return landed_ref.at[:, pl.ds(pl.multiple_of(me * tokens, tokens), tokens)]
        return landed_ref.at[
            :, pl.ds(pl.multiple_of((me * here + block) * part, part), part)
        ]

    pieces = 1 if splits == 1 else here

    def give(s, carry):
        sign = 1 - 2 * lax.rem(s, 2)
        target = lax.rem(me + n // 2 + sign * ((s + 1) // 2), n)
        for block in range(pieces):
            pltpu.make_async_remote_copy(
                src_ref=piece(target, block),
                dst_ref=place(block),
                send_sem=cache_sem.at[0],
                recv_sem=cache_sem.at[1],
                device_id={"seq": target},
                device_id_type=pl.DeviceIdType.MESH,
            ).start()
        return carry

    cuts = [(n - 1) * i // CHUNKS for i in range(CHUNKS + 1)]

    docs, valids = window_tables(
        counts_ref, tails_ref, order_ref, me * here - BACK, BACK + here
    )
    row = lax.broadcasted_iota(jnp.int32, (BLOCK, BLOCK), 0)
    col = lax.broadcasted_iota(jnp.int32, (BLOCK, BLOCK), 1)
    for b in range(here):
        for w in range(BACK + here):
            if w > BACK + b:
                shade = jnp.full((BLOCK, BLOCK), HIDDEN, jnp.float32)
            else:
                limit = jnp.where(docs[w] == docs[BACK + b], valids[w], 0)
                seen = col < limit
                if w == BACK + b:
                    seen = seen & (col <= row)
                shade = jnp.where(seen, 0.0, HIDDEN)
            bias[b * BLOCK : (b + 1) * BLOCK, w * BLOCK : (w + 1) * BLOCK] = shade
    column = lax.broadcasted_iota(jnp.int32, (BLOCK, HEAD_DIM), 0)
    real = jnp.concatenate(
        [column < valids[BACK + b] for b in range(here)], axis=0
    )

    empty = jnp.zeros((BLOCK, features), halo.dtype)
    for slot, reach in ((0, 3), (1, 2), (2, 2), (3, 1), (4, 1)):

        @pl.when(me < reach)
        def _():
            for kv in range(2):
                halo[kv, slot * BLOCK : (slot + 1) * BLOCK, :] = empty

    loads[2].wait()

    factor = HEAD_DIM ** (-0.5) * math.log2(math.e)
    prior = BACK * BLOCK
    nt = (((1,), (1,)), ((), ()))

    def one_head(h, carry):
        cols = pl.ds(pl.multiple_of(h * HEAD_DIM, HEAD_DIM), HEAD_DIM)
        q = q_ref[:, cols]
        s1 = lax.dot_general(q, halo[0, :, cols], nt, preferred_element_type=jnp.float32)
        s2 = lax.dot_general(q, own[0, :, cols], nt, preferred_element_type=jnp.float32)
        s1 = s1 + bias[:, :prior]
        s2 = s2 + bias[:, prior:]
        peak = jnp.maximum(
            jnp.max(s1, axis=1, keepdims=True), jnp.max(s2, axis=1, keepdims=True)
        )
        w1 = jnp.exp2((s1 - peak) * factor)
        w2 = jnp.exp2((s2 - peak) * factor)
        total = jnp.sum(w1, axis=1, keepdims=True) + jnp.sum(w2, axis=1, keepdims=True)
        mixed = jnp.dot(
            w1.astype(jnp.bfloat16), halo[1, :, cols], preferred_element_type=jnp.float32
        ) + jnp.dot(
            w2.astype(jnp.bfloat16), own[1, :, cols], preferred_element_type=jnp.float32
        )
        out_ref[:, cols] = jnp.where(real, mixed / total, 0.0).astype(out_ref.dtype)
        return carry

    for c in range(CHUNKS):
        lax.fori_loop(cuts[c], cuts[c + 1], give, 0)
        if c < ROUND:
            await_slots((role == 0) & more, c, [RELAY, RELAY + 1])
            start(
                (role == 0) & more,
                c,
                [(held(RELAY + 1), me + PLANE, 2), (held(RELAY), me + PLANE, 1)],
            )
        await_slots((role == 2) & late, c, [RELAY, 0])
        start(
            (role == 2) & late, c, [(held(RELAY), me - 2 + n, 3), (held(0), me - 2 + n, 4)]
        )
        await_slots((role == 0) & late, c, [2, 3, 4])
        await_slots(role == 2, c, [2, 3, 4])
        start(
            (role == 2) | ((role == 0) & late),
            c,
            [(held(2), me + 1, 0), (held(3), me + 1, 1), (held(4), me + 1, 2)],
        )
        await_slots((role == 0) & late, c, [0, 1])
        await_slots(role == 1, c, [3, 4])
        await_slots((role == 1) & late, c, [0, 1, 2])
        await_slots(role == 2, c, [1])
        await_slots(role == 3, c, [0, 1, 2, 3, 4])
        each = HEADS // CHUNKS
        lax.fori_loop(c * each, (c + 1) * each, one_head, 0)

    copies = [
        pltpu.make_async_copy(piece(me, block), place(block), own_sem.at[block])
        for block in range(pieces)
    ]
    for copy in copies:
        copy.start()

    for cond, copy in pending:

        @pl.when(cond)
        def _():
            copy.wait_send()

    for copy in copies:
        copy.wait()
    others = landed_ref.shape[1] // n * (n - 1)
    ref = landed_ref.at[:, pl.ds(0, others)]
    pltpu.make_async_copy(ref, ref, cache_sem.at[0]).wait()
    pltpu.make_async_copy(ref, ref, cache_sem.at[1]).wait()


def decode_places(counts_ref, order_ref, slot_ref, who, base, put):
    pairs = counts_ref.shape[0]
    prompts = order_ref.shape[0]

    def invert(p, carry):
        who[slot_ref[p]] = p
        return carry

    lax.fori_loop(0, pairs, invert, 0)

    def lay(s, first):
        p = who[s]
        base[p] = first
        return first + counts_ref[p] + 1

    lax.fori_loop(0, pairs, lay, jnp.int32(0))

    def fetch(i, first):
        prompt = order_ref[i]
        pair = lax.rem(prompt, pairs)
        null = prompt >= pairs
        counted = counts_ref[pair]
        size = jnp.where(null, 1, counted)
        target = base[pair] + jnp.where(null, counted, 0)

        def one(w, carry):
            put(first + w, target + w)
            return carry

        lax.fori_loop(0, size, one, 0)
        return first + size

    lax.fori_loop(0, prompts, fetch, jnp.int32(0))


def reorder(
    counts_ref,
    order_ref,
    slot_ref,
    landed_ref,
    keys_ref,
    values_ref,
    staged,
    who,
    base,
    in_sem,
    out_sem,
):
    part = staged.shape[2]

    def put(source, target):
        for kv in range(2):
            pltpu.make_async_copy(
                landed_ref.at[kv, pl.ds(source * part, part)],
                staged.at[kv, target],
                in_sem.at[kv],
            ).start()

    decode_places(counts_ref, order_ref, slot_ref, who, base, put)
    outs = []
    for kv, ref in enumerate((keys_ref, values_ref)):
        pltpu.make_async_copy(staged.at[kv], staged.at[kv], in_sem.at[kv]).wait()
        copy = pltpu.make_async_copy(staged.at[kv], ref.at[0], out_sem.at[kv])
        copy.start()
        outs.append(copy)
    for copy in outs:
        copy.wait()


def publish(places_ref, landed_ref, mixed_ref, attended_ref, keys_ref, values_ref, out_sem):
    leave = pltpu.make_async_copy(mixed_ref, attended_ref, out_sem.at[2])
    leave.start()
    refs = (keys_ref, values_ref)
    part = keys_ref.shape[2]

    for b in range(places_ref.shape[0]):
        place = places_ref[b]
        for kv, ref in enumerate(refs):
            pltpu.make_async_copy(
                landed_ref.at[kv, b * part : (b + 1) * part], ref.at[0, place], out_sem.at[kv]
            ).start()
    leave.wait()
    for kv, ref in enumerate(refs):
        pltpu.make_async_copy(ref.at[0], ref.at[0], out_sem.at[kv]).wait()


def handoff(
    n,
    counts_hbm,
    tails_hbm,
    order_hbm,
    slot_hbm,
    q_hbm,
    k_hbm,
    v_hbm,
    out_ref,
    landed_ref,
    places_ref,
    counts_ref,
    tails_ref,
    order_ref,
    slot_ref,
    q_ref,
    own,
    kv,
    qs,
    mixed_ref,
    bias,
    lower_q,
    lower_bias,
    slot_out,
    size_out,
    size_in,
    load_sem,
    local_sem,
    leave_sem,
    share_send,
    kv_recv,
    q_recv,
    halo_send,
    halo_recv,
    land_send,
    arrive_recv,
    down_send,
    down_recv,
    up_send,
    up_recv,
):
    me = lax.axis_index("seq")
    role = lax.rem(me, PLANE)
    plane = me // PLANE
    planes = n // PLANE
    tokens, features = q_ref.shape
    here = tokens // BLOCK
    width = PLANE * here
    skip = width - BACK
    reach = BACK * BLOCK
    few_rows = FEW * BLOCK
    far_rows = (BACK - NEAR) * BLOCK
    peers = (role + 1 - 2 * lax.rem(role, 2), lax.rem(role + 2, PLANE), PLANE - 1 - role)
    more = plane < planes - 1
    late = plane > 0
    base = plane * PLANE
    last = planes - 1
    orders = []
    for p in range(planes):
        above = list(range(last, p, -1))
        helping = [j for j in range(p + 1) if 2 * j < planes and 2 * p >= planes - 2]
        rest = [j for j in range(p, -1, -1) if j not in helping]
        if p == last:
            above, helping, rest = [last - 1], list(range(last - 1)), [last]
        orders.append(above + helping + rest)
    def one_if(i, value):
        return (i + planes - value) // planes - (i + planes - value - 1) // planes

    picks = [
        sum(orders[p][t] * one_if(plane, p) for p in range(planes)) for t in range(planes)
    ]

    def turn(t):
        return sum(picks[other] * one_if(t, other) for other in range(planes))

    def hold(j):
        return ((plane == last) & (j < plane - 1)) | ((plane == 0) & (j < planes // 2))

    def back(j, p):
        return (j <= p) & (2 * j < planes) & (2 * p >= planes - 2)

    helpable = [j for j in range(last) if 2 * j < planes]

    def helps(j):
        return more & back(j, plane)

    def helped(j):
        return late & back(j, plane - 1)

    def each(body):
        def step(t, carry):
            body(turn(t))
            return carry

        lax.fori_loop(0, planes, step, 0)

    def rows(first, count):
        return pl.ds(pl.multiple_of(first * BLOCK, BLOCK), count * BLOCK)

    def cols(head):
        return pl.ds(pl.multiple_of(head * HEAD_DIM, HEAD_DIM), HEAD_DIM)

    def remote(src, dst, send, recv, target):
        pltpu.make_async_remote_copy(
            src_ref=src,
            dst_ref=dst,
            send_sem=send,
            recv_sem=recv,
            device_id={"seq": target},
            device_id_type=pl.DeviceIdType.MESH,
        ).start()

    def await_(ref, sem):
        pltpu.make_async_copy(ref, ref, sem).wait()

    mine = rows(BACK + role * here, here)
    place = rows(role * here, here)

    loads = [
        pltpu.make_async_copy(src, dst, load_sem.at[i])
        for src, dst, i in ((k_hbm, own.at[0], 0), (v_hbm, own.at[1], 0), (q_hbm, q_ref, 1))
    ]
    barrier = pltpu.get_barrier_semaphore()
    for peer in peers:
        pl.semaphore_signal(
            barrier,
            inc=1,
            device_id={"seq": base + peer},
            device_id_type=pl.DeviceIdType.MESH,
        )
    for step in range(1, planes):
        pl.semaphore_signal(
            barrier,
            inc=1,
            device_id={"seq": lax.rem(me + step * PLANE, n)},
            device_id_type=pl.DeviceIdType.MESH,
        )
    for j in range(planes):
        here_cols = cols(j * PLANE + role)
        for i, src in enumerate((k_hbm, v_hbm)):
            pltpu.make_async_copy(
                src.at[:, here_cols], kv.at[j, i, mine], local_sem.at[0]
            ).start()
    for load in loads:
        load.start()
    smalls = [
        pltpu.make_async_copy(src, dst, load_sem.at[2 + i])
        for i, (src, dst) in enumerate(
            (
                (counts_hbm, counts_ref),
                (tails_hbm, tails_ref),
                (order_hbm, order_ref),
                (slot_hbm, slot_ref),
            )
        )
    ]
    for small in smalls:
        small.start()
    for j in range(planes):
        here_cols = cols(j * PLANE + role)
        pltpu.make_async_copy(
            q_hbm.at[:, here_cols], qs.at[j, place], local_sem.at[1]
        ).start()

    for j in range(planes):

        @pl.when(helped(j))
        def _():
            for i in range(2):
                kv[j, i, :far_rows, :] = jnp.zeros((far_rows, HEAD_DIM), kv.dtype)

        @pl.when(plane == 0)
        def _():
            for i in range(2):
                kv[j, i, :reach, :] = jnp.zeros((reach, HEAD_DIM), kv.dtype)

    def share(j):
        for k in (1, 2, 0):
            remote(
                own.at[:, :, cols(j * PLANE + peers[k])],
                kv.at[j, :, mine],
                share_send.at[0],
                kv_recv.at[k, j],
                base + peers[k],
            )

    def share_q(early):
        def body(j):
            soon = helped(j) & (role * here < FEW)

            @pl.when(soon if early else jnp.logical_not(soon))
            def _():
                for k in (1, 2, 0):
                    remote(
                        q_ref.at[:, cols(j * PLANE + peers[k])],
                        qs.at[j, place],
                        share_send.at[0],
                        q_recv.at[0 if early else 1, j],
                        base + peers[k],
                    )

        return body

    def when_helped(body, truth):
        def step(j):
            @pl.when(helped(j) if truth else jnp.logical_not(helped(j)))
            def _():
                body(j)

        return step

    def descend(body):
        def step(t, carry):
            body(last - t)
            return carry

        lax.fori_loop(0, planes, step, 0)

    def forward(j, rho):
        first = BACK + rho * here
        low = rho * here < skip
        high = rho * here + here > skip
        up = more & jnp.logical_not(helps(j))

        @pl.when(up & jnp.logical_not(low))
        def _():
            remote(
                kv.at[j, :, rows(first, here)],
                kv.at[j, :, rows(jnp.maximum(rho * here - skip, 0), here)],
                halo_send.at[0],
                halo_recv.at[j],
                me + PLANE,
            )

        @pl.when(up & low & high)
        def _():
            remote(
                kv.at[j, :, rows(BACK + skip, BACK % here)],
                kv.at[j, :, rows(0, BACK % here)],
                halo_send.at[0],
                halo_recv.at[j],
                me + PLANE,
            )

        @pl.when(late & (j > plane) & low & high)
        def _():
            remote(
                kv.at[j, :, rows(first, skip % here)],
                landed_ref.at[:, rows(plane * width + rho * here, skip % here)],
                land_send.at[0],
                arrive_recv.at[0],
                j * PLANE + role,
            )

        @pl.when(late & (j > plane) & jnp.logical_not(high))
        def _():
            remote(
                kv.at[j, :, rows(first, here)],
                landed_ref.at[:, rows(plane * width + rho * here, here)],
                land_send.at[0],
                arrive_recv.at[0],
                j * PLANE + role,
            )

        @pl.when(j < plane)
        def _():
            remote(
                kv.at[j, :, rows(first, here)],
                landed_ref.at[:, rows(plane * width + rho * here, here)],
                land_send.at[0],
                arrive_recv.at[0],
                j * PLANE + role,
            )

    def start_mine(j):
        @pl.when(jnp.logical_not(hold(j)))
        def _():
            forward(j, role)

    def take(k, j):
        await_(kv.at[j, :, rows(BACK + peers[k] * here, here)], kv_recv.at[k, j])

    def start_core(truth):
        def body(j):
            later = helped(j) & (j > 0)

            @pl.when(later if truth else jnp.logical_not(later))
            def _():
                take(0, j)

                @pl.when(jnp.logical_not(hold(j)))
                def _():
                    forward(j, peers[0])

        return body

    with jax.named_scope("enter_local"):
        await_(kv.at[:, :, mine], local_sem.at[0])
    with jax.named_scope("enter_barrier"):
        pl.semaphore_wait(barrier, PLANE - 1 + planes - 1)
    with jax.named_scope("start_mine"):
        each(start_mine)
    with jax.named_scope("enter_loads"):
        await_(own, load_sem.at[0])
        await_(q_ref, load_sem.at[1])
    with jax.named_scope("share"):
        each(share_q(True))
        each(share)
        descend(share_q(False))

    with jax.named_scope("take_core"):
        each(start_core(False))

    with jax.named_scope("tables"):
        for small in smalls:
            small.wait()
        docs, valids = window_tables(
            counts_ref, tails_ref, order_ref, plane * width - BACK, BACK + width + BACK
        )
        row = lax.broadcasted_iota(jnp.int32, (BLOCK, BLOCK), 0)
        col = lax.broadcasted_iota(jnp.int32, (BLOCK, BLOCK), 1)
        hidden = jnp.full((BLOCK, BLOCK), HIDDEN, jnp.float32)

        def near(first):
            return docs[first] != docs[first - NEAR - 1]

        def shade(source, target, shown=True):
            same = (docs[source] == docs[target]) & shown
            limit = jnp.where(same, valids[source], 0)
            seen = col < limit
            if source == target:
                seen = seen & (col <= row)
            return jnp.where(seen, 0.0, HIDDEN)

        for i in range(PLANE):
            for b in range(here):
                target = BACK + i * here + b
                for w in range(BACK + here):
                    source = i * here + w
                    spot = (slice(b * BLOCK, (b + 1) * BLOCK), slice(w * BLOCK, (w + 1) * BLOCK))
                    full = hidden if source > target else shade(source, target)
                    bias[(0, i) + spot] = full
                    if source < BACK - NEAR:
                        bias[(1, i) + spot] = hidden
                    elif source < BACK and source <= target:
                        bias[(1, i) + spot] = shade(source, target, near(BACK))
                    else:
                        bias[(1, i) + spot] = full
        for g in range(FEW):
            for c in range(BACK):
                lower_bias[g * BLOCK : (g + 1) * BLOCK, c * BLOCK : (c + 1) * BLOCK] = shade(
                    BACK + skip + c, BACK + width + g
                )
        column = lax.broadcasted_iota(jnp.int32, (BLOCK, HEAD_DIM), 0)

    soon_roles = -(-FEW // here)

    def await_q(j, early):
        def pieces(count, cond):
            if count > 0:

                @pl.when(cond)
                def _():
                    await_(qs.at[j, rows(0, count * here)], q_recv.at[0 if early else 1, j])

        inside = role < soon_roles
        split = helped(j)
        if early:
            pieces(soon_roles - 1, split & inside)
            pieces(soon_roles, split & jnp.logical_not(inside))
        else:
            pieces(PLANE - 1, jnp.logical_not(split))
            pieces(PLANE - soon_roles, split & inside)
            pieces(PLANE - 1 - soon_roles, split & jnp.logical_not(inside))

    await_(qs.at[:, place], local_sem.at[1])

    def lower(j):
        await_q(j, True)
        remote(
            qs.at[j, pl.ds(0, few_rows)],
            lower_q.at[j],
            down_send.at[j],
            down_recv.at[j],
            me - PLANE,
        )

    with jax.named_scope("lower_q"):
        for h in helpable:

            @pl.when(helped(h))
            def _():
                lower(h)

    each(start_core(True))

    def await_halo(j):
        await_(kv.at[j, :, rows(0, BACK)], halo_recv.at[j])

    below = rows(jnp.maximum(plane * width - BACK, 0), BACK)

    def relay(j):
        @pl.when(late & (j > plane))
        def _():
            await_halo(j)
            remote(
                kv.at[j, :, rows(0, BACK)],
                landed_ref.at[:, below],
                land_send.at[0],
                arrive_recv.at[0],
                j * PLANE + role,
            )

    def map_places():
        pairs = counts_ref.shape[0]
        blocks = places_ref.shape[0]

        def empty(b, carry):
            places_ref[b] = 0
            return carry

        lax.fori_loop(0, blocks, empty, 0)

        def fill(i, first):
            prompt = order_ref[i]
            pair = lax.rem(prompt, pairs)
            null = prompt >= pairs
            counted = counts_ref[pair]
            end = first + jnp.where(null, 1, counted)
            slot = slot_ref[pair]

            def earlier(p, total):
                return total + jnp.where(slot_ref[p] < slot, counts_ref[p] + 1, 0)

            target = lax.fori_loop(0, pairs, earlier, jnp.where(null, counted, 0)) - first

            def mark(chunk, carry):
                for step in range(8):
                    b = chunk * 8 + step
                    inside = (first <= b) & (b < end)
                    places_ref[b] = jnp.where(inside, target + b, places_ref[b])
                return carry

            lax.fori_loop(0, blocks // 8, mark, 0)
            return end

        lax.fori_loop(0, order_ref.shape[0], fill, jnp.int32(0))

    factor = HEAD_DIM ** (-0.5) * math.log2(math.e)
    nt = (((1,), (1,)), ((), ()))
    span = (BACK + here) * BLOCK

    def soften(q, k, v, mask):
        s = lax.dot_general(q, k, nt, preferred_element_type=jnp.float32) + mask
        peak = jnp.max(s, axis=1, keepdims=True)
        w = jnp.exp2((s - peak) * factor)
        total = jnp.sum(w, axis=1, keepdims=True)
        mixed = jnp.dot(w.astype(jnp.bfloat16), v, preferred_element_type=jnp.float32)
        return mixed, peak * factor, total

    def help_out(j):
        await_(lower_q.at[j], down_recv.at[j])
        send_near = near(BACK + width)
        for first in range(0, FEW, here):
            count = min(here, FEW - first)
            lines = slice(first * BLOCK, (first + count) * BLOCK)
            window = pl.ds((BACK + skip + first) * BLOCK, (BACK - first) * BLOCK)
            mixed, peak, total = soften(
                lower_q[j, lines, :],
                kv[j, 0, window, :],
                kv[j, 1, window, :],
                lower_bias[lines, first * BLOCK :],
            )
            size = jnp.broadcast_to(peak + jnp.log2(total), (count * BLOCK, BLOCK))
            for b in range(count):
                g = first + b
                turned = size[b * BLOCK : (b + 1) * BLOCK].T
                size_out[j, g] = jnp.where(send_near, HIDDEN, turned[:8])
            mixed = (mixed / total).astype(slot_out.dtype)
            for b in range(count):
                side, line = divmod(first + b, NEAR)
                spot = pl.ds(line * BLOCK, BLOCK)
                block = kv[j, side, pl.ds((BACK + width - NEAR + line) * BLOCK, BLOCK), :]
                slot_out[j, side, spot, :] = jnp.where(
                    send_near, block, mixed[b * BLOCK : (b + 1) * BLOCK]
                )
        for g in range(FEW, 2 * NEAR):
            side, line = divmod(g, NEAR)
            slot_out[j, side, pl.ds(line * BLOCK, BLOCK), :] = kv[
                j, side, pl.ds((BACK + width - NEAR + line) * BLOCK, BLOCK), :
            ]

    def await_up(j, sem):
        words = FEW * 8 * BLOCK * 2 + 2 * NEAR * BLOCK * HEAD_DIM
        await_(kv.at[j, 0, pl.ds(0, words // HEAD_DIM)], sem.at[j])

    def send_up(j):
        remote(
            slot_out.at[j],
            kv.at[j, :, rows(BACK - NEAR, NEAR)],
            up_send.at[j],
            up_recv.at[j],
            me + PLANE,
        )
        remote(size_out.at[j], size_in.at[j], up_send.at[j], up_recv.at[j], me + PLANE)

    def release(j):
        @pl.when(hold(j))
        def _():
            forward(j, role)
            forward(j, peers[0])

    def far(t, carry):
        j = turn(t)
        with jax.named_scope("take_far"):
            for k in (1, 2):
                take(k, j)
                forward(j, peers[k])

        @pl.when(t == min(1, last))
        def _():
            each(release)

        for h in helpable:

            @pl.when(helps(h) & (j == h))
            def _():
                with jax.named_scope("help_out"):
                    help_out(h)

        for h in helpable:

            @pl.when(helps(h) & (j == h))
            def _():
                send_up(h)

        return carry

    lax.fori_loop(0, planes, far, 0)

    def climb(j):
        @pl.when((plane == 0) & (j > 0))
        def _():
            remote(
                kv.at[j, :, rows(BACK, skip)],
                landed_ref.at[:, rows(0, skip)],
                land_send.at[0],
                arrive_recv.at[0],
                j * PLANE + role,
            )

    descend(climb)

    with jax.named_scope("relay"):
        descend(relay)

    settle = pltpu.make_async_copy(
        kv.at[plane, :, rows(BACK, width)],
        landed_ref.at[:, rows(plane * width, width)],
        leave_sem.at[0],
    )
    settle.start()

    def attend(j, i, variant):
        window = pl.ds(i * tokens, span)
        return soften(
            qs[j, pl.ds(i * tokens, tokens), :],
            kv[j, 0, window, :],
            kv[j, 1, window, :],
            bias[variant, i],
        )

    def finish(j, i, mixed, total):
        real = jnp.concatenate(
            [column < valids[BACK + i * here + b] for b in range(here)], axis=0
        )
        mixed_ref[j, i] = jnp.where(real, mixed / total, 0.0).astype(mixed_ref.dtype)

    def simple(j, i):
        mixed, _, total = attend(j, i, 0)
        finish(j, i, mixed, total)

    def give(j, i):
        target = out_ref.at[:, cols(j * PLANE + role)]

        @pl.when(role == i)
        def _():
            pltpu.make_async_copy(mixed_ref.at[j, i], target, leave_sem.at[0]).start()

        @pl.when(role != i)
        def _():
            remote(mixed_ref.at[j, i], target, share_send.at[0], arrive_recv.at[0], base + i)

    top = PLANE - 1

    def own_blocks(t, carry):
        j = last - t
        with jax.named_scope("wait_q"):
            await_q(j, False)

        with jax.named_scope("top"):
            simple(j, top)

            @pl.when(t > 0)
            def _():
                give(jnp.minimum(j + 1, last), top)

        return carry

    lax.fori_loop(0, planes, own_blocks, 0)

    def reach_back(j):
        with jax.named_scope("wait_halo"):

            @pl.when(late & (j <= plane))
            def _():
                await_halo(j)

        with jax.named_scope("units"):
            for i in range(top - 1, -1, -1):
                simple(j, i)
                if i == top - 1:

                    @pl.when(j == last)
                    def _():
                        give(0, top)

                    @pl.when(j < last)
                    def _():
                        give(jnp.minimum(j + 1, last), 0)

                else:
                    give(j, i + 1)

    descend(when_helped(reach_back, False))

    settled = pltpu.make_async_copy(
        kv.at[plane, :, rows(0, BACK)], landed_ref.at[:, below], leave_sem.at[0]
    )

    @pl.when(late)
    def _():
        settled.start()

    for j in range(planes):
        first = jnp.logical_not(helped(j))

        @pl.when(first & helped(j - 1) if j else first)
        def _():
            give(j, 0)

    def merge(j):
        with jax.named_scope("wait_part"):
            await_up(j, up_recv)
        with jax.named_scope("merge"):
            for i in range(top - 1, -1, -1):
                mixed, peak, total = attend(j, i, 1)
                mixed = [mixed[b * BLOCK : (b + 1) * BLOCK] for b in range(here)]
                total = [
                    jnp.broadcast_to(total[b * BLOCK : (b + 1) * BLOCK], (BLOCK, BLOCK))
                    for b in range(here)
                ]
                for b in range(here):
                    g = i * here + b
                    if g < FEW:
                        size = jnp.broadcast_to(size_in[j, g, :1], (BLOCK, BLOCK)).T
                        mark = peak[b * BLOCK : (b + 1) * BLOCK]
                        high = jnp.maximum(mark, size)
                        mine_share = jnp.exp2(mark - high)
                        their_share = jnp.exp2(size - high)
                        side, line = divmod(g, NEAR)
                        line = (BACK - NEAR + line) * BLOCK
                        theirs = kv[j, side, line : line + BLOCK, :]
                        mixed[b] = mixed[b] * mine_share + theirs.astype(jnp.float32) * their_share
                        total[b] = total[b] * mine_share + their_share
                finish(
                    j, i, jnp.concatenate(mixed, axis=0), jnp.concatenate(total, axis=0)
                )
                if i < top - 1:
                    give(j, i + 1)
        give(j, 0)

    for h in helpable:

        @pl.when(helped(h))
        def _():
            merge(h)

    with jax.named_scope("map_places"):
        map_places()

    with jax.named_scope("drain"):
        for h in helpable:

            @pl.when(helps(h))
            def _():
                await_up(h, up_send)

            @pl.when(helped(h))
            def _():
                await_(lower_q.at[h], down_send.at[h])

        for p in range(last):

            @pl.when(plane == p)
            def _():
                count = (planes - len([j for j in helpable if j <= p and 2 * p >= planes - 2])) * BACK
                await_(landed_ref.at[:, rows(0, count)], halo_send.at[0])

        shared = 2 * here * (PLANE - 1)
        outs = here * planes // 2
        passed = (planes - 1) * width

        @pl.when(plane == 0)
        def _():
            await_(landed_ref.at[:, rows(0, (planes - 1) * skip)], land_send.at[0])
            await_(landed_ref.at[:, rows(0, width + outs)], leave_sem.at[0])

        @pl.when(late)
        def _():
            await_(landed_ref.at[:, rows(0, passed)], land_send.at[0])
            await_(landed_ref.at[:, rows(0, width + BACK + outs)], leave_sem.at[0])

        await_(kv.at[:, :, rows(0, shared)], share_send.at[0])

    with jax.named_scope("land"):
        others = outs * (PLANE - 1)

        @pl.when(late)
        def _():
            await_(landed_ref.at[:, rows(0, passed - BACK + others)], arrive_recv.at[0])

        @pl.when(plane == 0)
        def _():
            await_(kv.at[:, :, rows(0, (passed + others) // planes)], arrive_recv.at[0])


def wide_exchange(n, queries, keys, values, block_counts, last_tokens, pack_order):
    tokens, features = queries.shape
    here = tokens // BLOCK
    part = BLOCK // (n // HEADS)
    blocks = here * n
    kind = queries.dtype
    smem = pl.BlockSpec(memory_space=pltpu.SMEM)
    vmem = pl.BlockSpec(memory_space=pltpu.VMEM)
    anywhere = pl.BlockSpec(memory_space=pl.ANY)
    dma = pltpu.SemaphoreType.DMA
    return pl.pallas_call(
        functools.partial(exchange, n),
        out_shape=(
            jax.ShapeDtypeStruct((tokens, features), kind),
            jax.ShapeDtypeStruct((2, blocks * part, HEAD_DIM), kind),
        ),
        in_specs=[smem] * 3 + [anywhere] * 3,
        out_specs=(vmem, anywhere),
        scratch_shapes=[
            pltpu.VMEM((tokens, features), kind),
            pltpu.VMEM((2, tokens, features), kind),
            pltpu.VMEM((2, BACK * BLOCK, features), kind),
            pltpu.VMEM((2, 2 * BLOCK, features), kind),
            pltpu.VMEM((tokens, (BACK + here) * BLOCK), jnp.float32),
            dma((CHUNKS * 18,)),
            dma((BACK + 2, CHUNKS)),
            dma((2,)),
            dma((here,)),
            dma((3,)),
        ],
        compiler_params=pltpu.CompilerParams(
            collective_id=0, has_side_effects=True, vmem_limit_bytes=60 * 1024 * 1024
        ),
    )(block_counts, last_tokens, pack_order, queries, keys, values)


def local(n, queries, keys, values, block_counts, last_tokens, pack_order, decode_slot):
    tokens, features = queries.shape
    here = tokens // BLOCK
    splits = n // HEADS
    part = BLOCK // splits
    blocks = here * n
    kind = queries.dtype
    smem = pl.BlockSpec(memory_space=pltpu.SMEM)
    anywhere = pl.BlockSpec(memory_space=pl.ANY)
    dma = pltpu.SemaphoreType.DMA
    planes = n // PLANE
    few = FEW * BLOCK
    last = planes - 1
    cache = jax.ShapeDtypeStruct((1, blocks, part, HEAD_DIM), kind)
    if splits == 1 and here == 2 and planes > 1:
        attended, landed, places = pl.pallas_call(
            functools.partial(handoff, n),
            out_shape=(
                pltpu.VMEM((tokens, features), kind),
                pltpu.VMEM((2, blocks * part, HEAD_DIM), kind),
                pltpu.SMEM((blocks,), jnp.int32),
            ),
            in_specs=[anywhere] * 7,
            out_specs=(anywhere, anywhere, smem),
            scratch_shapes=[
                pltpu.SMEM(block_counts.shape, jnp.int32),
                pltpu.SMEM(last_tokens.shape, jnp.int32),
                pltpu.SMEM(pack_order.shape, jnp.int32),
                pltpu.SMEM(decode_slot.shape, jnp.int32),
                pltpu.VMEM((tokens, features), kind),
                pltpu.VMEM((2, tokens, features), kind),
                pltpu.VMEM((planes, 2, (BACK + PLANE * here) * BLOCK, HEAD_DIM), kind),
                pltpu.VMEM((planes, PLANE * tokens, HEAD_DIM), kind),
                pltpu.VMEM((planes, PLANE, tokens, HEAD_DIM), kind),
                pltpu.VMEM((2, PLANE, tokens, (BACK + here) * BLOCK), jnp.float32),
                pltpu.VMEM((planes, few, HEAD_DIM), kind),
                pltpu.VMEM((few, BACK * BLOCK), jnp.float32),
                pltpu.VMEM((planes, 2, NEAR * BLOCK, HEAD_DIM), kind),
                pltpu.VMEM((planes, FEW, 8, BLOCK), jnp.float32),
                pltpu.VMEM((planes, FEW, 8, BLOCK), jnp.float32),
                dma((6,)),
                dma((2,)),
                dma((1,)),
                dma((1,)),
                dma((PLANE - 1, planes)),
                dma((2, planes)),
                dma((1,)),
                dma((planes,)),
                dma((1,)),
                dma((1,)),
                dma((last // 2 + 1,)),
                dma((last // 2 + 1,)),
                dma((last // 2 + 1,)),
                dma((last // 2 + 1,)),
            ],
            compiler_params=pltpu.CompilerParams(
                collective_id=0, has_side_effects=True, vmem_limit_bytes=60 * 1024 * 1024
            ),
        )(block_counts, last_tokens, pack_order, decode_slot, queries, keys, values)
        return pl.pallas_call(
            publish,
            out_shape=(jax.ShapeDtypeStruct((tokens, features), kind), cache, cache),
            in_specs=[smem] + [anywhere] * 2,
            out_specs=(anywhere,) * 3,
            scratch_shapes=[dma((3,))],
        )(
            pltpu.with_memory_space_constraint(places, pltpu.SMEM),
            pltpu.with_memory_space_constraint(landed, pltpu.VMEM),
            pltpu.with_memory_space_constraint(attended, pltpu.VMEM),
        )
    attended, landed = wide_exchange(
        n, queries, keys, values, block_counts, last_tokens, pack_order
    )
    cache_keys, cache_values = pl.pallas_call(
        reorder,
        out_shape=(cache, cache),
        in_specs=[smem] * 3 + [anywhere],
        out_specs=(anywhere, anywhere),
        scratch_shapes=[
            pltpu.VMEM((2, blocks, part, HEAD_DIM), kind),
            pltpu.SMEM(block_counts.shape, jnp.int32),
            pltpu.SMEM(block_counts.shape, jnp.int32),
            dma((2,)),
            dma((2,)),
        ],
    )(block_counts, pack_order, decode_slot, landed)
    return attended, cache_keys, cache_values


def solution(mesh):
    rows = P(("groups", "seq"), None)
    small = P("groups")
    cache = P(("groups", "seq"), None, None, None)
    return jax.shard_map(
        functools.partial(local, mesh.shape["seq"]),
        mesh=mesh,
        in_specs=(rows, rows, rows, small, small, small, small),
        out_specs=(rows, cache, cache),
        check_vma=False,
    )
```

```python
import functools
import math

import jax
import jax.numpy as jnp
from jax import lax
from jax.experimental import pallas as pl
from jax.experimental.pallas import tpu as pltpu
from jax.sharding import PartitionSpec as P

HEADS = 16
HEAD_DIM = 128
BLOCK = 128
MAXB = 6
BACK = MAXB - 1
HIDDEN = -1e30
PLANE = 4
CHUNKS = 4
RELAY = BACK
ROUND = 2
NEAR = 2
FEW = MAXB - NEAR - 1


def window_tables(counts_ref, tails_ref, order_ref, first, width):
    pairs = counts_ref.shape[0]
    prompts = order_ref.shape[0]

    def place(i, carry):
        start, docs, valids = carry
        prompt = order_ref[i]
        counted = counts_ref[lax.rem(prompt, pairs)]
        size = jnp.where(prompt < pairs, counted, 1)
        tail = tails_ref[prompt]
        end = start + size
        new_docs, new_valids = [], []
        for w in range(width):
            b = first + w
            inside = (start <= b) & (b < end)
            new_docs.append(jnp.where(inside, i, docs[w]))
            new_valids.append(
                jnp.where(inside, jnp.where(b + 1 == end, tail, BLOCK), valids[w])
            )
        return end, tuple(new_docs), tuple(new_valids)

    none = jnp.int32(-1)
    zero = jnp.int32(0)
    _, docs, valids = lax.fori_loop(
        0, prompts, place, (zero, (none,) * width, (zero,) * width)
    )
    return docs, valids


def exchange(
    n,
    counts_ref,
    tails_ref,
    order_ref,
    q_hbm,
    k_hbm,
    v_hbm,
    out_ref,
    landed_ref,
    q_ref,
    own,
    halo,
    relay,
    bias,
    halo_send,
    halo_recv,
    cache_sem,
    own_sem,
    load_sem,
):
    me = lax.axis_index("seq")
    role = lax.rem(me, PLANE)
    plane = me // PLANE
    planes = n // PLANE
    tokens, features = q_ref.shape
    here = tokens // BLOCK
    splits = n // HEADS
    part = BLOCK // splits
    wide = features // CHUNKS

    loads = [
        pltpu.make_async_copy(src, dst, load_sem.at[i])
        for i, (src, dst) in enumerate(
            ((k_hbm, own.at[0]), (v_hbm, own.at[1]), (q_hbm, q_ref))
        )
    ]
    for copy in loads:
        copy.start()

    barrier = pltpu.get_barrier_semaphore()

    def greet(r, carry):
        pl.semaphore_signal(
            barrier,
            inc=1,
            device_id={"seq": lax.rem(me + r, n)},
            device_id_type=pl.DeviceIdType.MESH,
        )
        return carry

    lax.fori_loop(1, n, greet, 0)
    loads[0].wait()
    loads[1].wait()
    pl.semaphore_wait(barrier, n - 1)

    pending = []

    def spot(block, c):
        return (
            slice(None),
            pl.ds(block * BLOCK, BLOCK),
            pl.ds(c * wide, wide),
        )

    def mine(block):
        return lambda c: own.at[spot(block, c)]

    def held(slot):
        if slot >= RELAY:
            return lambda c: relay.at[spot(slot - RELAY, c)]
        return lambda c: halo.at[spot(slot, c)]

    def start(cond, c, moves):
        copies = []
        for src, target, slot in moves:
            copy = pltpu.make_async_remote_copy(
                src_ref=src(c),
                dst_ref=held(slot)(c),
                send_sem=halo_send.at[len(pending)],
                recv_sem=halo_recv.at[slot, c],
                device_id={"seq": lax.rem(target + n, n)},
                device_id_type=pl.DeviceIdType.MESH,
            )
            pending.append((cond, copy))
            copies.append(copy)

        @pl.when(cond)
        def _():
            for copy in copies:
                copy.start()

    def await_slots(cond, c, slots):
        @pl.when(cond)
        def _():
            for slot in slots:
                ref = held(slot)(c)
                pltpu.make_async_copy(ref, ref, halo_recv.at[slot, c]).wait()

    more = plane < planes - 1
    late = plane > 0
    for c in range(CHUNKS):
        start((role == 3) & more, c, [(mine(0), me + 3, RELAY), (mine(1), me + 3, 0)])
        if c < ROUND:
            moves = [(mine(1), me - 2, RELAY + 1), (mine(0), me - 2, RELAY)]
        else:
            moves = [(mine(1), me + 2, 2), (mine(0), me + 2, 1)]
        start((role == 2) & more, c, moves)
        start((role == 1) & more, c, [(mine(1), me + 3, 0)])
        start(role == 1, c, [(mine(0), me + 1, 3), (mine(1), me + 1, 4)])
        start(role == 0, c, [(mine(1), me + 2, 2), (mine(0), me + 2, 1)])
        start(
            (role == 0) | (role == 2),
            c,
            [(mine(0), me + 1, 3), (mine(1), me + 1, 4)],
        )

    def piece(owner, block):
        head = owner // splits
        cols = pl.ds(pl.multiple_of(head * HEAD_DIM, HEAD_DIM), HEAD_DIM)
        if splits == 1:
            return own.at[:, :, cols]
        offset = pl.multiple_of(block * BLOCK + lax.rem(owner, splits) * part, part)
        return own.at[:, pl.ds(offset, part), cols]

    def place(block):
        if splits == 1:
            return landed_ref.at[:, pl.ds(pl.multiple_of(me * tokens, tokens), tokens)]
        return landed_ref.at[
            :, pl.ds(pl.multiple_of((me * here + block) * part, part), part)
        ]

    pieces = 1 if splits == 1 else here

    def give(s, carry):
        sign = 1 - 2 * lax.rem(s, 2)
        target = lax.rem(me + n // 2 + sign * ((s + 1) // 2), n)
        for block in range(pieces):
            pltpu.make_async_remote_copy(
                src_ref=piece(target, block),
                dst_ref=place(block),
                send_sem=cache_sem.at[0],
                recv_sem=cache_sem.at[1],
                device_id={"seq": target},
                device_id_type=pl.DeviceIdType.MESH,
            ).start()
        return carry

    cuts = [(n - 1) * i // CHUNKS for i in range(CHUNKS + 1)]

    docs, valids = window_tables(
        counts_ref, tails_ref, order_ref, me * here - BACK, BACK + here
    )
    row = lax.broadcasted_iota(jnp.int32, (BLOCK, BLOCK), 0)
    col = lax.broadcasted_iota(jnp.int32, (BLOCK, BLOCK), 1)
    for b in range(here):
        for w in range(BACK + here):
            if w > BACK + b:
                shade = jnp.full((BLOCK, BLOCK), HIDDEN, jnp.float32)
            else:
                limit = jnp.where(docs[w] == docs[BACK + b], valids[w], 0)
                seen = col < limit
                if w == BACK + b:
                    seen = seen & (col <= row)
                shade = jnp.where(seen, 0.0, HIDDEN)
            bias[b * BLOCK : (b + 1) * BLOCK, w * BLOCK : (w + 1) * BLOCK] = shade
    column = lax.broadcasted_iota(jnp.int32, (BLOCK, HEAD_DIM), 0)
    real = jnp.concatenate(
        [column < valids[BACK + b] for b in range(here)], axis=0
    )

    empty = jnp.zeros((BLOCK, features), halo.dtype)
    for slot, reach in ((0, 3), (1, 2), (2, 2), (3, 1), (4, 1)):

        @pl.when(me < reach)
        def _():
            for kv in range(2):
                halo[kv, slot * BLOCK : (slot + 1) * BLOCK, :] = empty

    loads[2].wait()

    factor = HEAD_DIM ** (-0.5) * math.log2(math.e)
    prior = BACK * BLOCK
    nt = (((1,), (1,)), ((), ()))

    def one_head(h, carry):
        cols = pl.ds(pl.multiple_of(h * HEAD_DIM, HEAD_DIM), HEAD_DIM)
        q = q_ref[:, cols]
        s1 = lax.dot_general(q, halo[0, :, cols], nt, preferred_element_type=jnp.float32)
        s2 = lax.dot_general(q, own[0, :, cols], nt, preferred_element_type=jnp.float32)
        s1 = s1 + bias[:, :prior]
        s2 = s2 + bias[:, prior:]
        peak = jnp.maximum(
            jnp.max(s1, axis=1, keepdims=True), jnp.max(s2, axis=1, keepdims=True)
        )
        w1 = jnp.exp2((s1 - peak) * factor)
        w2 = jnp.exp2((s2 - peak) * factor)
        total = jnp.sum(w1, axis=1, keepdims=True) + jnp.sum(w2, axis=1, keepdims=True)
        mixed = jnp.dot(
            w1.astype(jnp.bfloat16), halo[1, :, cols], preferred_element_type=jnp.float32
        ) + jnp.dot(
            w2.astype(jnp.bfloat16), own[1, :, cols], preferred_element_type=jnp.float32
        )
        out_ref[:, cols] = jnp.where(real, mixed / total, 0.0).astype(out_ref.dtype)
        return carry

    for c in range(CHUNKS):
        lax.fori_loop(cuts[c], cuts[c + 1], give, 0)
        if c < ROUND:
            await_slots((role == 0) & more, c, [RELAY, RELAY + 1])
            start(
                (role == 0) & more,
                c,
                [(held(RELAY + 1), me + PLANE, 2), (held(RELAY), me + PLANE, 1)],
            )
        await_slots((role == 2) & late, c, [RELAY, 0])
        start(
            (role == 2) & late, c, [(held(RELAY), me - 2 + n, 3), (held(0), me - 2 + n, 4)]
        )
        await_slots((role == 0) & late, c, [2, 3, 4])
        await_slots(role == 2, c, [2, 3, 4])
        start(
            (role == 2) | ((role == 0) & late),
            c,
            [(held(2), me + 1, 0), (held(3), me + 1, 1), (held(4), me + 1, 2)],
        )
        await_slots((role == 0) & late, c, [0, 1])
        await_slots(role == 1, c, [3, 4])
        await_slots((role == 1) & late, c, [0, 1, 2])
        await_slots(role == 2, c, [1])
        await_slots(role == 3, c, [0, 1, 2, 3, 4])
        each = HEADS // CHUNKS
        lax.fori_loop(c * each, (c + 1) * each, one_head, 0)

    copies = [
        pltpu.make_async_copy(piece(me, block), place(block), own_sem.at[block])
        for block in range(pieces)
    ]
    for copy in copies:
        copy.start()

    for cond, copy in pending:

        @pl.when(cond)
        def _():
            copy.wait_send()

    for copy in copies:
        copy.wait()
    others = landed_ref.shape[1] // n * (n - 1)
    ref = landed_ref.at[:, pl.ds(0, others)]
    pltpu.make_async_copy(ref, ref, cache_sem.at[0]).wait()
    pltpu.make_async_copy(ref, ref, cache_sem.at[1]).wait()


def decode_places(counts_ref, order_ref, slot_ref, who, base, put):
    pairs = counts_ref.shape[0]
    prompts = order_ref.shape[0]

    def invert(p, carry):
        who[slot_ref[p]] = p
        return carry

    lax.fori_loop(0, pairs, invert, 0)

    def lay(s, first):
        p = who[s]
        base[p] = first
        return first + counts_ref[p] + 1

    lax.fori_loop(0, pairs, lay, jnp.int32(0))

    def fetch(i, first):
        prompt = order_ref[i]
        pair = lax.rem(prompt, pairs)
        null = prompt >= pairs
        counted = counts_ref[pair]
        size = jnp.where(null, 1, counted)
        target = base[pair] + jnp.where(null, counted, 0)

        def one(w, carry):
            put(first + w, target + w)
            return carry

        lax.fori_loop(0, size, one, 0)
        return first + size

    lax.fori_loop(0, prompts, fetch, jnp.int32(0))


def reorder(
    counts_ref,
    order_ref,
    slot_ref,
    landed_ref,
    keys_ref,
    values_ref,
    staged,
    who,
    base,
    in_sem,
    out_sem,
):
    part = staged.shape[2]

    def put(source, target):
        for kv in range(2):
            pltpu.make_async_copy(
                landed_ref.at[kv, pl.ds(source * part, part)],
                staged.at[kv, target],
                in_sem.at[kv],
            ).start()

    decode_places(counts_ref, order_ref, slot_ref, who, base, put)
    outs = []
    for kv, ref in enumerate((keys_ref, values_ref)):
        pltpu.make_async_copy(staged.at[kv], staged.at[kv], in_sem.at[kv]).wait()
        copy = pltpu.make_async_copy(staged.at[kv], ref.at[0], out_sem.at[kv])
        copy.start()
        outs.append(copy)
    for copy in outs:
        copy.wait()


def publish(places_ref, landed_ref, mixed_ref, attended_ref, keys_ref, values_ref, out_sem):
    leave = pltpu.make_async_copy(mixed_ref, attended_ref, out_sem.at[2])
    leave.start()
    refs = (keys_ref, values_ref)
    part = keys_ref.shape[2]

    for b in range(places_ref.shape[0]):
        place = places_ref[b]
        for kv, ref in enumerate(refs):
            pltpu.make_async_copy(
                landed_ref.at[kv, b * part : (b + 1) * part], ref.at[0, place], out_sem.at[kv]
            ).start()
    leave.wait()
    for kv, ref in enumerate(refs):
        pltpu.make_async_copy(ref.at[0], ref.at[0], out_sem.at[kv]).wait()


def handoff(
    n,
    counts_hbm,
    tails_hbm,
    order_hbm,
    slot_hbm,
    q_hbm,
    k_hbm,
    v_hbm,
    out_ref,
    landed_ref,
    places_ref,
    counts_ref,
    tails_ref,
    order_ref,
    slot_ref,
    q_ref,
    own,
    kv,
    qs,
    mixed_ref,
    bias,
    lower_q,
    lower_bias,
    slot_out,
    size_out,
    size_in,
    load_sem,
    local_sem,
    leave_sem,
    share_send,
    kv_recv,
    q_recv,
    halo_send,
    halo_recv,
    land_send,
    arrive_recv,
    down_send,
    down_recv,
    up_send,
    up_recv,
):
    me = lax.axis_index("seq")
    role = lax.rem(me, PLANE)
    plane = me // PLANE
    planes = n // PLANE
    tokens, features = q_ref.shape
    here = tokens // BLOCK
    width = PLANE * here
    skip = width - BACK
    reach = BACK * BLOCK
    few_rows = FEW * BLOCK
    far_rows = (BACK - NEAR) * BLOCK
    peers = (role + 1 - 2 * lax.rem(role, 2), lax.rem(role + 2, PLANE), PLANE - 1 - role)
    more = plane < planes - 1
    late = plane > 0
    base = plane * PLANE
    last = planes - 1
    orders = []
    for p in range(planes):
        above = list(range(last, p, -1))
        helping = [j for j in range(p + 1) if 2 * j < planes and 2 * p >= planes - 2]
        rest = [j for j in range(p, -1, -1) if j not in helping]
        if p == last:
            above, helping, rest = [last - 1], list(range(last - 1)), [last]
        orders.append(above + helping + rest)
    def one_if(i, value):
        return (i + planes - value) // planes - (i + planes - value - 1) // planes

    picks = [
        sum(orders[p][t] * one_if(plane, p) for p in range(planes)) for t in range(planes)
    ]

    def turn(t):
        return sum(picks[other] * one_if(t, other) for other in range(planes))

    def hold(j):
        return ((plane == last) & (j < plane - 1)) | ((plane == 0) & (j < planes // 2))

    def defer(j):
        return (plane == last) & (j > 0) & (j < plane - 1)

    def back(j, p):
        return (j <= p) & (2 * j < planes) & (2 * p >= planes - 2)

    helpable = [j for j in range(last) if 2 * j < planes]

    def helps(j):
        return more & back(j, plane)

    def helped(j):
        return late & back(j, plane - 1)

    def each(body):
        def step(t, carry):
            body(turn(t))
            return carry

        lax.fori_loop(0, planes, step, 0)

    def rows(first, count):
        return pl.ds(pl.multiple_of(first * BLOCK, BLOCK), count * BLOCK)

    def cols(head):
        return pl.ds(pl.multiple_of(head * HEAD_DIM, HEAD_DIM), HEAD_DIM)

    def remote(src, dst, send, recv, target):
        pltpu.make_async_remote_copy(
            src_ref=src,
            dst_ref=dst,
            send_sem=send,
            recv_sem=recv,
            device_id={"seq": target},
            device_id_type=pl.DeviceIdType.MESH,
        ).start()

    def await_(ref, sem):
        pltpu.make_async_copy(ref, ref, sem).wait()

    mine = rows(BACK + role * here, here)
    place = rows(role * here, here)

    loads = [
        pltpu.make_async_copy(src, dst, load_sem.at[i])
        for src, dst, i in ((k_hbm, own.at[0], 0), (v_hbm, own.at[1], 0), (q_hbm, q_ref, 1))
    ]
    barrier = pltpu.get_barrier_semaphore()
    for peer in peers:
        pl.semaphore_signal(
            barrier,
            inc=1,
            device_id={"seq": base + peer},
            device_id_type=pl.DeviceIdType.MESH,
        )
    for step in range(1, planes):
        pl.semaphore_signal(
            barrier,
            inc=1,
            device_id={"seq": lax.rem(me + step * PLANE, n)},
            device_id_type=pl.DeviceIdType.MESH,
        )
    for j in range(planes):
        here_cols = cols(j * PLANE + role)
        for i, src in enumerate((k_hbm, v_hbm)):
            pltpu.make_async_copy(
                src.at[:, here_cols], kv.at[j, i, mine], local_sem.at[0]
            ).start()
    for load in loads:
        load.start()
    smalls = [
        pltpu.make_async_copy(src, dst, load_sem.at[2 + i])
        for i, (src, dst) in enumerate(
            (
                (counts_hbm, counts_ref),
                (tails_hbm, tails_ref),
                (order_hbm, order_ref),
                (slot_hbm, slot_ref),
            )
        )
    ]
    for small in smalls:
        small.start()
    for j in range(planes):
        here_cols = cols(j * PLANE + role)
        pltpu.make_async_copy(
            q_hbm.at[:, here_cols], qs.at[j, place], local_sem.at[1]
        ).start()

    for j in range(planes):

        @pl.when(helped(j))
        def _():
            for i in range(2):
                kv[j, i, :far_rows, :] = jnp.zeros((far_rows, HEAD_DIM), kv.dtype)

        @pl.when(plane == 0)
        def _():
            for i in range(2):
                kv[j, i, :reach, :] = jnp.zeros((reach, HEAD_DIM), kv.dtype)

    def share(j):
        for k in (1, 2, 0):
            remote(
                own.at[:, :, cols(j * PLANE + peers[k])],
                kv.at[j, :, mine],
                share_send.at[0],
                kv_recv.at[k, j],
                base + peers[k],
            )

    def share_q(early):
        def body(j):
            soon = helped(j) & (role * here < FEW)

            @pl.when(soon if early else jnp.logical_not(soon))
            def _():
                for k in (1, 2, 0):
                    remote(
                        q_ref.at[:, cols(j * PLANE + peers[k])],
                        qs.at[j, place],
                        share_send.at[0],
                        q_recv.at[0 if early else 1, j],
                        base + peers[k],
                    )

        return body

    def when_helped(body, truth):
        def step(j):
            @pl.when(helped(j) if truth else jnp.logical_not(helped(j)))
            def _():
                body(j)

        return step

    def descend(body):
        def step(t, carry):
            body(last - t)
            return carry

        lax.fori_loop(0, planes, step, 0)

    def forward(j, rho):
        first = BACK + rho * here
        low = rho * here < skip
        high = rho * here + here > skip
        up = more & jnp.logical_not(helps(j))

        @pl.when(up & jnp.logical_not(low))
        def _():
            remote(
                kv.at[j, :, rows(first, here)],
                kv.at[j, :, rows(jnp.maximum(rho * here - skip, 0), here)],
                halo_send.at[0],
                halo_recv.at[j],
                me + PLANE,
            )

        @pl.when(up & low & high)
        def _():
            remote(
                kv.at[j, :, rows(BACK + skip, BACK % here)],
                kv.at[j, :, rows(0, BACK % here)],
                halo_send.at[0],
                halo_recv.at[j],
                me + PLANE,
            )

        @pl.when(late & (j > plane) & low & high)
        def _():
            remote(
                kv.at[j, :, rows(first, skip % here)],
                landed_ref.at[:, rows(plane * width + rho * here, skip % here)],
                land_send.at[0],
                arrive_recv.at[0],
                j * PLANE + role,
            )

        @pl.when(late & (j > plane) & jnp.logical_not(high))
        def _():
            remote(
                kv.at[j, :, rows(first, here)],
                landed_ref.at[:, rows(plane * width + rho * here, here)],
                land_send.at[0],
                arrive_recv.at[0],
                j * PLANE + role,
            )

        @pl.when(j < plane)
        def _():
            remote(
                kv.at[j, :, rows(first, here)],
                landed_ref.at[:, rows(plane * width + rho * here, here)],
                land_send.at[0],
                arrive_recv.at[0],
                j * PLANE + role,
            )

    def start_mine(j):
        @pl.when(jnp.logical_not(hold(j)))
        def _():
            forward(j, role)

    def take(k, j):
        await_(kv.at[j, :, rows(BACK + peers[k] * here, here)], kv_recv.at[k, j])

    def start_core(truth):
        def body(j):
            later = helped(j) & (j > 0)

            @pl.when(later if truth else jnp.logical_not(later))
            def _():
                take(0, j)

                @pl.when(jnp.logical_not(hold(j)))
                def _():
                    forward(j, peers[0])

        return body

    with jax.named_scope("enter_local"):
        await_(kv.at[:, :, mine], local_sem.at[0])
    with jax.named_scope("enter_barrier"):
        pl.semaphore_wait(barrier, PLANE - 1 + planes - 1)
    with jax.named_scope("start_mine"):
        each(start_mine)
    with jax.named_scope("enter_loads"):
        await_(own, load_sem.at[0])
        await_(q_ref, load_sem.at[1])
    with jax.named_scope("share"):
        each(share_q(True))
        each(share)
        descend(share_q(False))

    with jax.named_scope("take_core"):
        each(start_core(False))

    with jax.named_scope("tables"):
        for small in smalls:
            small.wait()
        docs, valids = window_tables(
            counts_ref, tails_ref, order_ref, plane * width - BACK, BACK + width + BACK
        )
        row = lax.broadcasted_iota(jnp.int32, (BLOCK, BLOCK), 0)
        col = lax.broadcasted_iota(jnp.int32, (BLOCK, BLOCK), 1)
        hidden = jnp.full((BLOCK, BLOCK), HIDDEN, jnp.float32)

        def near(first):
            return docs[first] != docs[first - NEAR - 1]

        def shade(source, target, shown=True):
            same = (docs[source] == docs[target]) & shown
            limit = jnp.where(same, valids[source], 0)
            seen = col < limit
            if source == target:
                seen = seen & (col <= row)
            return jnp.where(seen, 0.0, HIDDEN)

        for i in range(PLANE):
            for b in range(here):
                target = BACK + i * here + b
                for w in range(BACK + here):
                    source = i * here + w
                    spot = (slice(b * BLOCK, (b + 1) * BLOCK), slice(w * BLOCK, (w + 1) * BLOCK))
                    full = hidden if source > target else shade(source, target)
                    bias[(0, i) + spot] = full
                    if source < BACK - NEAR:
                        bias[(1, i) + spot] = hidden
                    elif source < BACK and source <= target:
                        bias[(1, i) + spot] = shade(source, target, near(BACK))
                    else:
                        bias[(1, i) + spot] = full
        for g in range(FEW):
            for c in range(BACK):
                lower_bias[g * BLOCK : (g + 1) * BLOCK, c * BLOCK : (c + 1) * BLOCK] = shade(
                    BACK + skip + c, BACK + width + g
                )
        column = lax.broadcasted_iota(jnp.int32, (BLOCK, HEAD_DIM), 0)

    soon_roles = -(-FEW // here)

    def await_q(j, early):
        def pieces(count, cond):
            if count > 0:

                @pl.when(cond)
                def _():
                    await_(qs.at[j, rows(0, count * here)], q_recv.at[0 if early else 1, j])

        inside = role < soon_roles
        split = helped(j)
        if early:
            pieces(soon_roles - 1, split & inside)
            pieces(soon_roles, split & jnp.logical_not(inside))
        else:
            pieces(PLANE - 1, jnp.logical_not(split))
            pieces(PLANE - soon_roles, split & inside)
            pieces(PLANE - 1 - soon_roles, split & jnp.logical_not(inside))

    await_(qs.at[:, place], local_sem.at[1])

    def lower(j):
        await_q(j, True)
        remote(
            qs.at[j, pl.ds(0, few_rows)],
            lower_q.at[j],
            down_send.at[j],
            down_recv.at[j],
            me - PLANE,
        )

    with jax.named_scope("lower_q"):
        for h in helpable:

            @pl.when(helped(h))
            def _():
                lower(h)

    each(start_core(True))

    def await_halo(j):
        await_(kv.at[j, :, rows(0, BACK)], halo_recv.at[j])

    below = rows(jnp.maximum(plane * width - BACK, 0), BACK)

    def relay(j):
        @pl.when(late & (j > plane))
        def _():
            await_halo(j)
            remote(
                kv.at[j, :, rows(0, BACK)],
                landed_ref.at[:, below],
                land_send.at[0],
                arrive_recv.at[0],
                j * PLANE + role,
            )

    def map_places():
        pairs = counts_ref.shape[0]
        blocks = places_ref.shape[0]

        def empty(b, carry):
            places_ref[b] = 0
            return carry

        lax.fori_loop(0, blocks, empty, 0)

        def fill(i, first):
            prompt = order_ref[i]
            pair = lax.rem(prompt, pairs)
            null = prompt >= pairs
            counted = counts_ref[pair]
            end = first + jnp.where(null, 1, counted)
            slot = slot_ref[pair]

            def earlier(p, total):
                return total + jnp.where(slot_ref[p] < slot, counts_ref[p] + 1, 0)

            target = lax.fori_loop(0, pairs, earlier, jnp.where(null, counted, 0)) - first

            def mark(chunk, carry):
                for step in range(8):
                    b = chunk * 8 + step
                    inside = (first <= b) & (b < end)
                    places_ref[b] = jnp.where(inside, target + b, places_ref[b])
                return carry

            lax.fori_loop(0, blocks // 8, mark, 0)
            return end

        lax.fori_loop(0, order_ref.shape[0], fill, jnp.int32(0))

    factor = HEAD_DIM ** (-0.5) * math.log2(math.e)
    nt = (((1,), (1,)), ((), ()))
    span = (BACK + here) * BLOCK

    def soften(q, k, v, mask):
        s = lax.dot_general(q, k, nt, preferred_element_type=jnp.float32) + mask
        peak = jnp.max(s, axis=1, keepdims=True)
        w = jnp.exp2((s - peak) * factor)
        total = jnp.sum(w, axis=1, keepdims=True)
        mixed = jnp.dot(w.astype(jnp.bfloat16), v, preferred_element_type=jnp.float32)
        return mixed, peak * factor, total

    def help_out(j):
        await_(lower_q.at[j], down_recv.at[j])
        send_near = near(BACK + width)
        for first in range(0, FEW, here):
            count = min(here, FEW - first)
            lines = slice(first * BLOCK, (first + count) * BLOCK)
            window = pl.ds((BACK + skip + first) * BLOCK, (BACK - first) * BLOCK)
            mixed, peak, total = soften(
                lower_q[j, lines, :],
                kv[j, 0, window, :],
                kv[j, 1, window, :],
                lower_bias[lines, first * BLOCK :],
            )
            size = jnp.broadcast_to(peak + jnp.log2(total), (count * BLOCK, BLOCK))
            for b in range(count):
                g = first + b
                turned = size[b * BLOCK : (b + 1) * BLOCK].T
                size_out[j, g] = jnp.where(send_near, HIDDEN, turned[:8])
            mixed = (mixed / total).astype(slot_out.dtype)
            for b in range(count):
                side, line = divmod(first + b, NEAR)
                spot = pl.ds(line * BLOCK, BLOCK)
                block = kv[j, side, pl.ds((BACK + width - NEAR + line) * BLOCK, BLOCK), :]
                slot_out[j, side, spot, :] = jnp.where(
                    send_near, block, mixed[b * BLOCK : (b + 1) * BLOCK]
                )
        for g in range(FEW, 2 * NEAR):
            side, line = divmod(g, NEAR)
            slot_out[j, side, pl.ds(line * BLOCK, BLOCK), :] = kv[
                j, side, pl.ds((BACK + width - NEAR + line) * BLOCK, BLOCK), :
            ]

    def await_up(j, sem):
        words = FEW * 8 * BLOCK * 2 + 2 * NEAR * BLOCK * HEAD_DIM
        await_(kv.at[j, 0, pl.ds(0, words // HEAD_DIM)], sem.at[j])

    def send_up(j):
        remote(
            slot_out.at[j],
            kv.at[j, :, rows(BACK - NEAR, NEAR)],
            up_send.at[j],
            up_recv.at[j],
            me + PLANE,
        )
        remote(size_out.at[j], size_in.at[j], up_send.at[j], up_recv.at[j], me + PLANE)

    def release(j):
        @pl.when(hold(j) & jnp.logical_not(defer(j)))
        def _():
            forward(j, role)
            forward(j, peers[0])

    def far(t, carry):
        j = turn(t)
        with jax.named_scope("take_far"):
            for k in (1, 2):
                take(k, j)

                @pl.when(jnp.logical_not(defer(j)))
                def _():
                    forward(j, peers[k])

        @pl.when(t == min(1, last))
        def _():
            each(release)

        for h in helpable:

            @pl.when(helps(h) & (j == h))
            def _():
                with jax.named_scope("help_out"):
                    help_out(h)

        for h in helpable:

            @pl.when(helps(h) & (j == h))
            def _():
                send_up(h)

        return carry

    lax.fori_loop(0, planes, far, 0)

    def climb(j):
        @pl.when((plane == 0) & (j > 0))
        def _():
            remote(
                kv.at[j, :, rows(BACK, skip)],
                landed_ref.at[:, rows(0, skip)],
                land_send.at[0],
                arrive_recv.at[0],
                j * PLANE + role,
            )

    descend(climb)

    with jax.named_scope("relay"):
        descend(relay)

    settle = pltpu.make_async_copy(
        kv.at[plane, :, rows(BACK, width)],
        landed_ref.at[:, rows(plane * width, width)],
        leave_sem.at[0],
    )
    settle.start()

    def attend(j, i, variant):
        window = pl.ds(i * tokens, span)
        return soften(
            qs[j, pl.ds(i * tokens, tokens), :],
            kv[j, 0, window, :],
            kv[j, 1, window, :],
            bias[variant, i],
        )

    def finish(j, i, mixed, total):
        real = jnp.concatenate(
            [column < valids[BACK + i * here + b] for b in range(here)], axis=0
        )
        mixed_ref[j, i] = jnp.where(real, mixed / total, 0.0).astype(mixed_ref.dtype)

    def simple(j, i):
        mixed, _, total = attend(j, i, 0)
        finish(j, i, mixed, total)

    def give(j, i):
        target = out_ref.at[:, cols(j * PLANE + role)]

        @pl.when(role == i)
        def _():
            pltpu.make_async_copy(mixed_ref.at[j, i], target, leave_sem.at[0]).start()

        @pl.when(role != i)
        def _():
            remote(mixed_ref.at[j, i], target, share_send.at[0], arrive_recv.at[0], base + i)

    top = PLANE - 1

    def lump(j):
        @pl.when(defer(j))
        def _():
            remote(
                kv.at[j, :, rows(BACK, width)],
                landed_ref.at[:, rows(plane * width, width)],
                land_send.at[0],
                arrive_recv.at[0],
                j * PLANE + role,
            )

    def reach_back(j, waiting):
        with jax.named_scope("wait_halo"):

            @pl.when(late & (j <= plane))
            def _():
                await_halo(j)

        with jax.named_scope("units"):
            for i in range(top - 1, -1, -1):
                simple(j, i)
                if i == top - 1:
                    give(*waiting)
                else:
                    give(j, i + 1)

    def one_head(t, carry):
        j = last - t
        with jax.named_scope("wait_q"):
            await_q(j, False)
        with jax.named_scope("top"):
            simple(j, top)

            @pl.when(t == min(1, last))
            def _():
                descend(lump)

        before = jnp.minimum(j + 1, last)
        earlier = jnp.minimum(j + 2, last)
        full = jnp.logical_not(helped(earlier))

        @pl.when((t > 1) & full)
        def _():
            give(earlier, 0)

        @pl.when((t == 1) | ((t > 1) & jnp.logical_not(full)))
        def _():
            give(before, top)

        @pl.when((t > 0) & jnp.logical_not(helped(before)))
        def _():
            reach_back(before, (j, top))

        return carry

    lax.fori_loop(0, planes, one_head, 0)
    whole = jnp.logical_not(helped(0))

    @pl.when(whole)
    def _():
        reach_back(0, (1, 0))

    settled = pltpu.make_async_copy(
        kv.at[plane, :, rows(0, BACK)], landed_ref.at[:, below], leave_sem.at[0]
    )

    @pl.when(late)
    def _():
        settled.start()

    @pl.when(whole)
    def _():
        give(0, 0)

    @pl.when(helped(0) & jnp.logical_not(helped(1)))
    def _():
        give(1, 0)

    @pl.when(helped(0) & helped(1))
    def _():
        give(0, top)

    def merge(j):
        with jax.named_scope("wait_part"):
            await_up(j, up_recv)
        with jax.named_scope("merge"):
            for i in range(top - 1, -1, -1):
                mixed, peak, total = attend(j, i, 1)
                mixed = [mixed[b * BLOCK : (b + 1) * BLOCK] for b in range(here)]
                total = [
                    jnp.broadcast_to(total[b * BLOCK : (b + 1) * BLOCK], (BLOCK, BLOCK))
                    for b in range(here)
                ]
                for b in range(here):
                    g = i * here + b
                    if g < FEW:
                        size = jnp.broadcast_to(size_in[j, g, :1], (BLOCK, BLOCK)).T
                        mark = peak[b * BLOCK : (b + 1) * BLOCK]
                        high = jnp.maximum(mark, size)
                        mine_share = jnp.exp2(mark - high)
                        their_share = jnp.exp2(size - high)
                        side, line = divmod(g, NEAR)
                        line = (BACK - NEAR + line) * BLOCK
                        theirs = kv[j, side, line : line + BLOCK, :]
                        mixed[b] = mixed[b] * mine_share + theirs.astype(jnp.float32) * their_share
                        total[b] = total[b] * mine_share + their_share
                finish(
                    j, i, jnp.concatenate(mixed, axis=0), jnp.concatenate(total, axis=0)
                )
                if i < top - 1:
                    give(j, i + 1)
        give(j, 0)

    for h in helpable:

        @pl.when(helped(h))
        def _():
            merge(h)

    with jax.named_scope("map_places"):
        map_places()

    with jax.named_scope("drain"):
        for h in helpable:

            @pl.when(helps(h))
            def _():
                await_up(h, up_send)

            @pl.when(helped(h))
            def _():
                await_(lower_q.at[h], down_send.at[h])

        for p in range(last):

            @pl.when(plane == p)
            def _():
                count = (planes - len([j for j in helpable if j <= p and 2 * p >= planes - 2])) * BACK
                await_(landed_ref.at[:, rows(0, count)], halo_send.at[0])

        shared = 2 * here * (PLANE - 1)
        outs = here * planes // 2
        passed = (planes - 1) * width

        @pl.when(plane == 0)
        def _():
            await_(landed_ref.at[:, rows(0, (planes - 1) * skip)], land_send.at[0])
            await_(landed_ref.at[:, rows(0, width + outs)], leave_sem.at[0])

        @pl.when(late)
        def _():
            await_(landed_ref.at[:, rows(0, passed)], land_send.at[0])
            await_(landed_ref.at[:, rows(0, width + BACK + outs)], leave_sem.at[0])

        await_(kv.at[:, :, rows(0, shared)], share_send.at[0])

    with jax.named_scope("land"):
        others = outs * (PLANE - 1)

        @pl.when(late)
        def _():
            await_(landed_ref.at[:, rows(0, passed - BACK + others)], arrive_recv.at[0])

        @pl.when(plane == 0)
        def _():
            await_(kv.at[:, :, rows(0, (passed + others) // planes)], arrive_recv.at[0])


def wide_exchange(n, queries, keys, values, block_counts, last_tokens, pack_order):
    tokens, features = queries.shape
    here = tokens // BLOCK
    part = BLOCK // (n // HEADS)
    blocks = here * n
    kind = queries.dtype
    smem = pl.BlockSpec(memory_space=pltpu.SMEM)
    vmem = pl.BlockSpec(memory_space=pltpu.VMEM)
    anywhere = pl.BlockSpec(memory_space=pl.ANY)
    dma = pltpu.SemaphoreType.DMA
    return pl.pallas_call(
        functools.partial(exchange, n),
        out_shape=(
            jax.ShapeDtypeStruct((tokens, features), kind),
            jax.ShapeDtypeStruct((2, blocks * part, HEAD_DIM), kind),
        ),
        in_specs=[smem] * 3 + [anywhere] * 3,
        out_specs=(vmem, anywhere),
        scratch_shapes=[
            pltpu.VMEM((tokens, features), kind),
            pltpu.VMEM((2, tokens, features), kind),
            pltpu.VMEM((2, BACK * BLOCK, features), kind),
            pltpu.VMEM((2, 2 * BLOCK, features), kind),
            pltpu.VMEM((tokens, (BACK + here) * BLOCK), jnp.float32),
            dma((CHUNKS * 18,)),
            dma((BACK + 2, CHUNKS)),
            dma((2,)),
            dma((here,)),
            dma((3,)),
        ],
        compiler_params=pltpu.CompilerParams(
            collective_id=0, has_side_effects=True, vmem_limit_bytes=60 * 1024 * 1024
        ),
    )(block_counts, last_tokens, pack_order, queries, keys, values)


def local(n, queries, keys, values, block_counts, last_tokens, pack_order, decode_slot):
    tokens, features = queries.shape
    here = tokens // BLOCK
    splits = n // HEADS
    part = BLOCK // splits
    blocks = here * n
    kind = queries.dtype
    smem = pl.BlockSpec(memory_space=pltpu.SMEM)
    anywhere = pl.BlockSpec(memory_space=pl.ANY)
    dma = pltpu.SemaphoreType.DMA
    planes = n // PLANE
    few = FEW * BLOCK
    last = planes - 1
    cache = jax.ShapeDtypeStruct((1, blocks, part, HEAD_DIM), kind)
    if splits == 1 and here == 2 and planes > 1:
        attended, landed, places = pl.pallas_call(
            functools.partial(handoff, n),
            out_shape=(
                pltpu.VMEM((tokens, features), kind),
                pltpu.VMEM((2, blocks * part, HEAD_DIM), kind),
                pltpu.SMEM((blocks,), jnp.int32),
            ),
            in_specs=[anywhere] * 7,
            out_specs=(anywhere, anywhere, smem),
            scratch_shapes=[
                pltpu.SMEM(block_counts.shape, jnp.int32),
                pltpu.SMEM(last_tokens.shape, jnp.int32),
                pltpu.SMEM(pack_order.shape, jnp.int32),
                pltpu.SMEM(decode_slot.shape, jnp.int32),
                pltpu.VMEM((tokens, features), kind),
                pltpu.VMEM((2, tokens, features), kind),
                pltpu.VMEM((planes, 2, (BACK + PLANE * here) * BLOCK, HEAD_DIM), kind),
                pltpu.VMEM((planes, PLANE * tokens, HEAD_DIM), kind),
                pltpu.VMEM((planes, PLANE, tokens, HEAD_DIM), kind),
                pltpu.VMEM((2, PLANE, tokens, (BACK + here) * BLOCK), jnp.float32),
                pltpu.VMEM((planes, few, HEAD_DIM), kind),
                pltpu.VMEM((few, BACK * BLOCK), jnp.float32),
                pltpu.VMEM((planes, 2, NEAR * BLOCK, HEAD_DIM), kind),
                pltpu.VMEM((planes, FEW, 8, BLOCK), jnp.float32),
                pltpu.VMEM((planes, FEW, 8, BLOCK), jnp.float32),
                dma((6,)),
                dma((2,)),
                dma((1,)),
                dma((1,)),
                dma((PLANE - 1, planes)),
                dma((2, planes)),
                dma((1,)),
                dma((planes,)),
                dma((1,)),
                dma((1,)),
                dma((last // 2 + 1,)),
                dma((last // 2 + 1,)),
                dma((last // 2 + 1,)),
                dma((last // 2 + 1,)),
            ],
            compiler_params=pltpu.CompilerParams(
                collective_id=0, has_side_effects=True, vmem_limit_bytes=60 * 1024 * 1024
            ),
        )(block_counts, last_tokens, pack_order, decode_slot, queries, keys, values)
        return pl.pallas_call(
            publish,
            out_shape=(jax.ShapeDtypeStruct((tokens, features), kind), cache, cache),
            in_specs=[smem] + [anywhere] * 2,
            out_specs=(anywhere,) * 3,
            scratch_shapes=[dma((3,))],
        )(
            pltpu.with_memory_space_constraint(places, pltpu.SMEM),
            pltpu.with_memory_space_constraint(landed, pltpu.VMEM),
            pltpu.with_memory_space_constraint(attended, pltpu.VMEM),
        )
    attended, landed = wide_exchange(
        n, queries, keys, values, block_counts, last_tokens, pack_order
    )
    cache_keys, cache_values = pl.pallas_call(
        reorder,
        out_shape=(cache, cache),
        in_specs=[smem] * 3 + [anywhere],
        out_specs=(anywhere, anywhere),
        scratch_shapes=[
            pltpu.VMEM((2, blocks, part, HEAD_DIM), kind),
            pltpu.SMEM(block_counts.shape, jnp.int32),
            pltpu.SMEM(block_counts.shape, jnp.int32),
            dma((2,)),
            dma((2,)),
        ],
    )(block_counts, pack_order, decode_slot, landed)
    return attended, cache_keys, cache_values


def solution(mesh):
    rows = P(("groups", "seq"), None)
    small = P("groups")
    cache = P(("groups", "seq"), None, None, None)
    return jax.shard_map(
        functools.partial(local, mesh.shape["seq"]),
        mesh=mesh,
        in_specs=(rows, rows, rows, small, small, small, small),
        out_specs=(rows, cache, cache),
        check_vma=False,
    )
```

```python
import functools
import math

import jax
import jax.numpy as jnp
from jax import lax
from jax.experimental import pallas as pl
from jax.experimental.pallas import tpu as pltpu
from jax.sharding import PartitionSpec as P

HEADS = 16
HEAD_DIM = 128
BLOCK = 128
MAXB = 6
BACK = MAXB - 1
HIDDEN = -1e30
PLANE = 4
CHUNKS = 4
RELAY = BACK
ROUND = 2
NEAR = 2
FEW = MAXB - NEAR - 1


def window_tables(counts_ref, tails_ref, order_ref, first, width):
    pairs = counts_ref.shape[0]
    prompts = order_ref.shape[0]

    def place(i, carry):
        start, docs, valids = carry
        prompt = order_ref[i]
        counted = counts_ref[lax.rem(prompt, pairs)]
        size = jnp.where(prompt < pairs, counted, 1)
        tail = tails_ref[prompt]
        end = start + size
        new_docs, new_valids = [], []
        for w in range(width):
            b = first + w
            inside = (start <= b) & (b < end)
            new_docs.append(jnp.where(inside, i, docs[w]))
            new_valids.append(
                jnp.where(inside, jnp.where(b + 1 == end, tail, BLOCK), valids[w])
            )
        return end, tuple(new_docs), tuple(new_valids)

    none = jnp.int32(-1)
    zero = jnp.int32(0)
    _, docs, valids = lax.fori_loop(
        0, prompts, place, (zero, (none,) * width, (zero,) * width)
    )
    return docs, valids


def exchange(
    n,
    counts_ref,
    tails_ref,
    order_ref,
    q_hbm,
    k_hbm,
    v_hbm,
    out_ref,
    landed_ref,
    q_ref,
    own,
    halo,
    relay,
    bias,
    halo_send,
    halo_recv,
    cache_sem,
    own_sem,
    load_sem,
):
    me = lax.axis_index("seq")
    role = lax.rem(me, PLANE)
    plane = me // PLANE
    planes = n // PLANE
    tokens, features = q_ref.shape
    here = tokens // BLOCK
    splits = n // HEADS
    part = BLOCK // splits
    wide = features // CHUNKS

    loads = [
        pltpu.make_async_copy(src, dst, load_sem.at[i])
        for i, (src, dst) in enumerate(
            ((k_hbm, own.at[0]), (v_hbm, own.at[1]), (q_hbm, q_ref))
        )
    ]
    for copy in loads:
        copy.start()

    barrier = pltpu.get_barrier_semaphore()

    def greet(r, carry):
        pl.semaphore_signal(
            barrier,
            inc=1,
            device_id={"seq": lax.rem(me + r, n)},
            device_id_type=pl.DeviceIdType.MESH,
        )
        return carry

    lax.fori_loop(1, n, greet, 0)
    loads[0].wait()
    loads[1].wait()
    pl.semaphore_wait(barrier, n - 1)

    pending = []

    def spot(block, c):
        return (
            slice(None),
            pl.ds(block * BLOCK, BLOCK),
            pl.ds(c * wide, wide),
        )

    def mine(block):
        return lambda c: own.at[spot(block, c)]

    def held(slot):
        if slot >= RELAY:
            return lambda c: relay.at[spot(slot - RELAY, c)]
        return lambda c: halo.at[spot(slot, c)]

    def start(cond, c, moves):
        copies = []
        for src, target, slot in moves:
            copy = pltpu.make_async_remote_copy(
                src_ref=src(c),
                dst_ref=held(slot)(c),
                send_sem=halo_send.at[len(pending)],
                recv_sem=halo_recv.at[slot, c],
                device_id={"seq": lax.rem(target + n, n)},
                device_id_type=pl.DeviceIdType.MESH,
            )
            pending.append((cond, copy))
            copies.append(copy)

        @pl.when(cond)
        def _():
            for copy in copies:
                copy.start()

    def await_slots(cond, c, slots):
        @pl.when(cond)
        def _():
            for slot in slots:
                ref = held(slot)(c)
                pltpu.make_async_copy(ref, ref, halo_recv.at[slot, c]).wait()

    more = plane < planes - 1
    late = plane > 0
    for c in range(CHUNKS):
        start((role == 3) & more, c, [(mine(0), me + 3, RELAY), (mine(1), me + 3, 0)])
        if c < ROUND:
            moves = [(mine(1), me - 2, RELAY + 1), (mine(0), me - 2, RELAY)]
        else:
            moves = [(mine(1), me + 2, 2), (mine(0), me + 2, 1)]
        start((role == 2) & more, c, moves)
        start((role == 1) & more, c, [(mine(1), me + 3, 0)])
        start(role == 1, c, [(mine(0), me + 1, 3), (mine(1), me + 1, 4)])
        start(role == 0, c, [(mine(1), me + 2, 2), (mine(0), me + 2, 1)])
        start(
            (role == 0) | (role == 2),
            c,
            [(mine(0), me + 1, 3), (mine(1), me + 1, 4)],
        )

    def piece(owner, block):
        head = owner // splits
        cols = pl.ds(pl.multiple_of(head * HEAD_DIM, HEAD_DIM), HEAD_DIM)
        if splits == 1:
            return own.at[:, :, cols]
        offset = pl.multiple_of(block * BLOCK + lax.rem(owner, splits) * part, part)
        return own.at[:, pl.ds(offset, part), cols]

    def place(block):
        if splits == 1:
            return landed_ref.at[:, pl.ds(pl.multiple_of(me * tokens, tokens), tokens)]
        return landed_ref.at[
            :, pl.ds(pl.multiple_of((me * here + block) * part, part), part)
        ]

    pieces = 1 if splits == 1 else here

    def give(s, carry):
        sign = 1 - 2 * lax.rem(s, 2)
        target = lax.rem(me + n // 2 + sign * ((s + 1) // 2), n)
        for block in range(pieces):
            pltpu.make_async_remote_copy(
                src_ref=piece(target, block),
                dst_ref=place(block),
                send_sem=cache_sem.at[0],
                recv_sem=cache_sem.at[1],
                device_id={"seq": target},
                device_id_type=pl.DeviceIdType.MESH,
            ).start()
        return carry

    cuts = [(n - 1) * i // CHUNKS for i in range(CHUNKS + 1)]

    docs, valids = window_tables(
        counts_ref, tails_ref, order_ref, me * here - BACK, BACK + here
    )
    row = lax.broadcasted_iota(jnp.int32, (BLOCK, BLOCK), 0)
    col = lax.broadcasted_iota(jnp.int32, (BLOCK, BLOCK), 1)
    for b in range(here):
        for w in range(BACK + here):
            if w > BACK + b:
                shade = jnp.full((BLOCK, BLOCK), HIDDEN, jnp.float32)
            else:
                limit = jnp.where(docs[w] == docs[BACK + b], valids[w], 0)
                seen = col < limit
                if w == BACK + b:
                    seen = seen & (col <= row)
                shade = jnp.where(seen, 0.0, HIDDEN)
            bias[b * BLOCK : (b + 1) * BLOCK, w * BLOCK : (w + 1) * BLOCK] = shade
    column = lax.broadcasted_iota(jnp.int32, (BLOCK, HEAD_DIM), 0)
    real = jnp.concatenate(
        [column < valids[BACK + b] for b in range(here)], axis=0
    )

    empty = jnp.zeros((BLOCK, features), halo.dtype)
    for slot, reach in ((0, 3), (1, 2), (2, 2), (3, 1), (4, 1)):

        @pl.when(me < reach)
        def _():
            for kv in range(2):
                halo[kv, slot * BLOCK : (slot + 1) * BLOCK, :] = empty

    loads[2].wait()

    factor = HEAD_DIM ** (-0.5) * math.log2(math.e)
    prior = BACK * BLOCK
    nt = (((1,), (1,)), ((), ()))

    def one_head(h, carry):
        cols = pl.ds(pl.multiple_of(h * HEAD_DIM, HEAD_DIM), HEAD_DIM)
        q = q_ref[:, cols]
        s1 = lax.dot_general(q, halo[0, :, cols], nt, preferred_element_type=jnp.float32)
        s2 = lax.dot_general(q, own[0, :, cols], nt, preferred_element_type=jnp.float32)
        s1 = s1 + bias[:, :prior]
        s2 = s2 + bias[:, prior:]
        peak = jnp.maximum(
            jnp.max(s1, axis=1, keepdims=True), jnp.max(s2, axis=1, keepdims=True)
        )
        w1 = jnp.exp2((s1 - peak) * factor)
        w2 = jnp.exp2((s2 - peak) * factor)
        total = jnp.sum(w1, axis=1, keepdims=True) + jnp.sum(w2, axis=1, keepdims=True)
        mixed = jnp.dot(
            w1.astype(jnp.bfloat16), halo[1, :, cols], preferred_element_type=jnp.float32
        ) + jnp.dot(
            w2.astype(jnp.bfloat16), own[1, :, cols], preferred_element_type=jnp.float32
        )
        out_ref[:, cols] = jnp.where(real, mixed / total, 0.0).astype(out_ref.dtype)
        return carry

    for c in range(CHUNKS):
        lax.fori_loop(cuts[c], cuts[c + 1], give, 0)
        if c < ROUND:
            await_slots((role == 0) & more, c, [RELAY, RELAY + 1])
            start(
                (role == 0) & more,
                c,
                [(held(RELAY + 1), me + PLANE, 2), (held(RELAY), me + PLANE, 1)],
            )
        await_slots((role == 2) & late, c, [RELAY, 0])
        start(
            (role == 2) & late, c, [(held(RELAY), me - 2 + n, 3), (held(0), me - 2 + n, 4)]
        )
        await_slots((role == 0) & late, c, [2, 3, 4])
        await_slots(role == 2, c, [2, 3, 4])
        start(
            (role == 2) | ((role == 0) & late),
            c,
            [(held(2), me + 1, 0), (held(3), me + 1, 1), (held(4), me + 1, 2)],
        )
        await_slots((role == 0) & late, c, [0, 1])
        await_slots(role == 1, c, [3, 4])
        await_slots((role == 1) & late, c, [0, 1, 2])
        await_slots(role == 2, c, [1])
        await_slots(role == 3, c, [0, 1, 2, 3, 4])
        each = HEADS // CHUNKS
        lax.fori_loop(c * each, (c + 1) * each, one_head, 0)

    copies = [
        pltpu.make_async_copy(piece(me, block), place(block), own_sem.at[block])
        for block in range(pieces)
    ]
    for copy in copies:
        copy.start()

    for cond, copy in pending:

        @pl.when(cond)
        def _():
            copy.wait_send()

    for copy in copies:
        copy.wait()
    others = landed_ref.shape[1] // n * (n - 1)
    ref = landed_ref.at[:, pl.ds(0, others)]
    pltpu.make_async_copy(ref, ref, cache_sem.at[0]).wait()
    pltpu.make_async_copy(ref, ref, cache_sem.at[1]).wait()


def decode_places(counts_ref, order_ref, slot_ref, who, base, put):
    pairs = counts_ref.shape[0]
    prompts = order_ref.shape[0]

    def invert(p, carry):
        who[slot_ref[p]] = p
        return carry

    lax.fori_loop(0, pairs, invert, 0)

    def lay(s, first):
        p = who[s]
        base[p] = first
        return first + counts_ref[p] + 1

    lax.fori_loop(0, pairs, lay, jnp.int32(0))

    def fetch(i, first):
        prompt = order_ref[i]
        pair = lax.rem(prompt, pairs)
        null = prompt >= pairs
        counted = counts_ref[pair]
        size = jnp.where(null, 1, counted)
        target = base[pair] + jnp.where(null, counted, 0)

        def one(w, carry):
            put(first + w, target + w)
            return carry

        lax.fori_loop(0, size, one, 0)
        return first + size

    lax.fori_loop(0, prompts, fetch, jnp.int32(0))


def reorder(
    counts_ref,
    order_ref,
    slot_ref,
    landed_ref,
    keys_ref,
    values_ref,
    staged,
    who,
    base,
    in_sem,
    out_sem,
):
    part = staged.shape[2]

    def put(source, target):
        for kv in range(2):
            pltpu.make_async_copy(
                landed_ref.at[kv, pl.ds(source * part, part)],
                staged.at[kv, target],
                in_sem.at[kv],
            ).start()

    decode_places(counts_ref, order_ref, slot_ref, who, base, put)
    outs = []
    for kv, ref in enumerate((keys_ref, values_ref)):
        pltpu.make_async_copy(staged.at[kv], staged.at[kv], in_sem.at[kv]).wait()
        copy = pltpu.make_async_copy(staged.at[kv], ref.at[0], out_sem.at[kv])
        copy.start()
        outs.append(copy)
    for copy in outs:
        copy.wait()


def publish(places_ref, landed_ref, mixed_ref, attended_ref, keys_ref, values_ref, out_sem):
    leave = pltpu.make_async_copy(mixed_ref, attended_ref, out_sem.at[2])
    leave.start()
    refs = (keys_ref, values_ref)
    part = keys_ref.shape[2]

    for b in range(places_ref.shape[0]):
        place = places_ref[b]
        for kv, ref in enumerate(refs):
            pltpu.make_async_copy(
                landed_ref.at[kv, b * part : (b + 1) * part], ref.at[0, place], out_sem.at[kv]
            ).start()
    leave.wait()
    for kv, ref in enumerate(refs):
        pltpu.make_async_copy(ref.at[0], ref.at[0], out_sem.at[kv]).wait()


def handoff(
    n,
    counts_hbm,
    tails_hbm,
    order_hbm,
    slot_hbm,
    q_hbm,
    k_hbm,
    v_hbm,
    out_ref,
    landed_ref,
    places_ref,
    counts_ref,
    tails_ref,
    order_ref,
    slot_ref,
    q_ref,
    own,
    kv,
    qs,
    mixed_ref,
    bias,
    lower_q,
    lower_bias,
    slot_out,
    size_out,
    size_in,
    load_sem,
    local_sem,
    leave_sem,
    share_send,
    kv_recv,
    q_recv,
    halo_send,
    halo_recv,
    land_send,
    arrive_recv,
    down_send,
    down_recv,
    up_send,
    up_recv,
):
    me = lax.axis_index("seq")
    role = lax.rem(me, PLANE)
    plane = me // PLANE
    planes = n // PLANE
    tokens, features = q_ref.shape
    here = tokens // BLOCK
    width = PLANE * here
    skip = width - BACK
    reach = BACK * BLOCK
    few_rows = FEW * BLOCK
    far_rows = (BACK - NEAR) * BLOCK
    peers = (role + 1 - 2 * lax.rem(role, 2), lax.rem(role + 2, PLANE), PLANE - 1 - role)
    more = plane < planes - 1
    late = plane > 0
    base = plane * PLANE
    last = planes - 1
    orders = []
    for p in range(planes):
        above = list(range(last, p, -1))
        helping = [j for j in range(p + 1) if 2 * j < planes and 2 * p >= planes - 2]
        rest = [j for j in range(p, -1, -1) if j not in helping]
        if p == last:
            above, helping, rest = [last - 1], list(range(last - 1)), [last]
        orders.append(above + helping + rest)
    def one_if(i, value):
        return (i + planes - value) // planes - (i + planes - value - 1) // planes

    picks = [
        sum(orders[p][t] * one_if(plane, p) for p in range(planes)) for t in range(planes)
    ]

    def turn(t):
        return sum(picks[other] * one_if(t, other) for other in range(planes))

    def hold(j):
        return ((plane == last) & (j < plane - 1)) | ((plane == 0) & (j < planes // 2))

    def defer(j):
        return (plane == last) & (j > 0) & (j < plane - 1)

    def back(j, p):
        return (j <= p) & (2 * j < planes) & (2 * p >= planes - 2)

    helpable = [j for j in range(last) if 2 * j < planes]

    def helps(j):
        return more & back(j, plane)

    def helped(j):
        return late & back(j, plane - 1)

    def each(body):
        def step(t, carry):
            body(turn(t))
            return carry

        lax.fori_loop(0, planes, step, 0)

    def rows(first, count):
        return pl.ds(pl.multiple_of(first * BLOCK, BLOCK), count * BLOCK)

    def cols(head):
        return pl.ds(pl.multiple_of(head * HEAD_DIM, HEAD_DIM), HEAD_DIM)

    def remote(src, dst, send, recv, target):
        pltpu.make_async_remote_copy(
            src_ref=src,
            dst_ref=dst,
            send_sem=send,
            recv_sem=recv,
            device_id={"seq": target},
            device_id_type=pl.DeviceIdType.MESH,
        ).start()

    def await_(ref, sem):
        pltpu.make_async_copy(ref, ref, sem).wait()

    mine = rows(BACK + role * here, here)
    place = rows(role * here, here)

    loads = [
        pltpu.make_async_copy(src, dst, load_sem.at[i])
        for src, dst, i in ((k_hbm, own.at[0], 0), (v_hbm, own.at[1], 0), (q_hbm, q_ref, 1))
    ]
    barrier = pltpu.get_barrier_semaphore()
    for peer in peers:
        pl.semaphore_signal(
            barrier,
            inc=1,
            device_id={"seq": base + peer},
            device_id_type=pl.DeviceIdType.MESH,
        )
    for step in range(1, planes):
        pl.semaphore_signal(
            barrier,
            inc=1,
            device_id={"seq": lax.rem(me + step * PLANE, n)},
            device_id_type=pl.DeviceIdType.MESH,
        )
    for j in range(planes):
        here_cols = cols(j * PLANE + role)
        for i, src in enumerate((k_hbm, v_hbm)):
            pltpu.make_async_copy(
                src.at[:, here_cols], kv.at[j, i, mine], local_sem.at[0]
            ).start()
    for load in loads:
        load.start()
    smalls = [
        pltpu.make_async_copy(src, dst, load_sem.at[2 + i])
        for i, (src, dst) in enumerate(
            (
                (counts_hbm, counts_ref),
                (tails_hbm, tails_ref),
                (order_hbm, order_ref),
                (slot_hbm, slot_ref),
            )
        )
    ]
    for small in smalls:
        small.start()
    for j in range(planes):
        here_cols = cols(j * PLANE + role)
        pltpu.make_async_copy(
            q_hbm.at[:, here_cols], qs.at[j, place], local_sem.at[1]
        ).start()

    for j in range(planes):

        @pl.when(helped(j))
        def _():
            for i in range(2):
                kv[j, i, :far_rows, :] = jnp.zeros((far_rows, HEAD_DIM), kv.dtype)

        @pl.when(plane == 0)
        def _():
            for i in range(2):
                kv[j, i, :reach, :] = jnp.zeros((reach, HEAD_DIM), kv.dtype)

    def share(j):
        for k in (1, 2, 0):
            remote(
                own.at[:, :, cols(j * PLANE + peers[k])],
                kv.at[j, :, mine],
                share_send.at[0],
                kv_recv.at[k, j],
                base + peers[k],
            )

    def share_q(early):
        def body(j):
            soon = helped(j) & (role * here < FEW)

            @pl.when(soon if early else jnp.logical_not(soon))
            def _():
                for k in (1, 2, 0):
                    remote(
                        q_ref.at[:, cols(j * PLANE + peers[k])],
                        qs.at[j, place],
                        share_send.at[0],
                        q_recv.at[0 if early else 1, j],
                        base + peers[k],
                    )

        return body

    def when_helped(body, truth):
        def step(j):
            @pl.when(helped(j) if truth else jnp.logical_not(helped(j)))
            def _():
                body(j)

        return step

    def descend(body):
        def step(t, carry):
            body(last - t)
            return carry

        lax.fori_loop(0, planes, step, 0)

    def forward(j, rho):
        first = BACK + rho * here
        low = rho * here < skip
        high = rho * here + here > skip
        up = more & jnp.logical_not(helps(j))

        @pl.when(up & jnp.logical_not(low))
        def _():
            remote(
                kv.at[j, :, rows(first, here)],
                kv.at[j, :, rows(jnp.maximum(rho * here - skip, 0), here)],
                halo_send.at[0],
                halo_recv.at[j],
                me + PLANE,
            )

        @pl.when(up & low & high)
        def _():
            remote(
                kv.at[j, :, rows(BACK + skip, BACK % here)],
                kv.at[j, :, rows(0, BACK % here)],
                halo_send.at[0],
                halo_recv.at[j],
                me + PLANE,
            )

        @pl.when(late & (j > plane) & low & high)
        def _():
            remote(
                kv.at[j, :, rows(first, skip % here)],
                landed_ref.at[:, rows(plane * width + rho * here, skip % here)],
                land_send.at[0],
                arrive_recv.at[0],
                j * PLANE + role,
            )

        @pl.when(late & (j > plane) & jnp.logical_not(high))
        def _():
            remote(
                kv.at[j, :, rows(first, here)],
                landed_ref.at[:, rows(plane * width + rho * here, here)],
                land_send.at[0],
                arrive_recv.at[0],
                j * PLANE + role,
            )

        @pl.when(j < plane)
        def _():
            remote(
                kv.at[j, :, rows(first, here)],
                landed_ref.at[:, rows(plane * width + rho * here, here)],
                land_send.at[0],
                arrive_recv.at[0],
                j * PLANE + role,
            )

    def start_mine(j):
        @pl.when(jnp.logical_not(hold(j)))
        def _():
            forward(j, role)

    def take(k, j):
        await_(kv.at[j, :, rows(BACK + peers[k] * here, here)], kv_recv.at[k, j])

    def start_core(truth):
        def body(j):
            later = helped(j) & (j > 0)

            @pl.when(later if truth else jnp.logical_not(later))
            def _():
                take(0, j)

                @pl.when(jnp.logical_not(hold(j)))
                def _():
                    forward(j, peers[0])

        return body

    with jax.named_scope("enter_local"):
        await_(kv.at[:, :, mine], local_sem.at[0])
    with jax.named_scope("enter_barrier"):
        pl.semaphore_wait(barrier, PLANE - 1 + planes - 1)
    with jax.named_scope("start_mine"):
        each(start_mine)
    with jax.named_scope("enter_loads"):
        await_(own, load_sem.at[0])
        await_(q_ref, load_sem.at[1])
    with jax.named_scope("share"):
        each(share_q(True))
        each(share)
        descend(share_q(False))

    with jax.named_scope("take_core"):
        each(start_core(False))

    with jax.named_scope("tables"):
        for small in smalls:
            small.wait()
        docs, valids = window_tables(
            counts_ref, tails_ref, order_ref, plane * width - BACK, BACK + width + BACK
        )
        row = lax.broadcasted_iota(jnp.int32, (BLOCK, BLOCK), 0)
        col = lax.broadcasted_iota(jnp.int32, (BLOCK, BLOCK), 1)
        hidden = jnp.full((BLOCK, BLOCK), HIDDEN, jnp.float32)

        def near(first):
            return docs[first] != docs[first - NEAR - 1]

        def shade(source, target, shown=True):
            same = (docs[source] == docs[target]) & shown
            limit = jnp.where(same, valids[source], 0)
            seen = col < limit
            if source == target:
                seen = seen & (col <= row)
            return jnp.where(seen, 0.0, HIDDEN)

        for i in range(PLANE):
            for b in range(here):
                target = BACK + i * here + b
                for w in range(BACK + here):
                    source = i * here + w
                    spot = (slice(b * BLOCK, (b + 1) * BLOCK), slice(w * BLOCK, (w + 1) * BLOCK))
                    full = hidden if source > target else shade(source, target)
                    bias[(0, i) + spot] = full
                    if source < BACK - NEAR:
                        bias[(1, i) + spot] = hidden
                    elif source < BACK and source <= target:
                        bias[(1, i) + spot] = shade(source, target, near(BACK))
                    else:
                        bias[(1, i) + spot] = full
        for g in range(FEW):
            for c in range(BACK):
                lower_bias[g * BLOCK : (g + 1) * BLOCK, c * BLOCK : (c + 1) * BLOCK] = shade(
                    BACK + skip + c, BACK + width + g
                )
        column = lax.broadcasted_iota(jnp.int32, (BLOCK, HEAD_DIM), 0)

    soon_roles = -(-FEW // here)

    def await_q(j, early):
        def pieces(count, cond):
            if count > 0:

                @pl.when(cond)
                def _():
                    await_(qs.at[j, rows(0, count * here)], q_recv.at[0 if early else 1, j])

        inside = role < soon_roles
        split = helped(j)
        if early:
            pieces(soon_roles - 1, split & inside)
            pieces(soon_roles, split & jnp.logical_not(inside))
        else:
            pieces(PLANE - 1, jnp.logical_not(split))
            pieces(PLANE - soon_roles, split & inside)
            pieces(PLANE - 1 - soon_roles, split & jnp.logical_not(inside))

    await_(qs.at[:, place], local_sem.at[1])

    def lower(j):
        await_q(j, True)
        remote(
            qs.at[j, pl.ds(0, few_rows)],
            lower_q.at[j],
            down_send.at[j],
            down_recv.at[j],
            me - PLANE,
        )

    with jax.named_scope("lower_q"):
        for h in helpable:

            @pl.when(helped(h))
            def _():
                lower(h)

    each(start_core(True))

    def await_halo(j):
        await_(kv.at[j, :, rows(0, BACK)], halo_recv.at[j])

    below = rows(jnp.maximum(plane * width - BACK, 0), BACK)

    def relay(j):
        @pl.when(late & (j > plane))
        def _():
            await_halo(j)
            remote(
                kv.at[j, :, rows(0, BACK)],
                landed_ref.at[:, below],
                land_send.at[0],
                arrive_recv.at[0],
                j * PLANE + role,
            )

    def map_places():
        pairs = counts_ref.shape[0]
        blocks = places_ref.shape[0]

        def fill(i, first):
            prompt = order_ref[i]
            pair = lax.rem(prompt, pairs)
            null = prompt >= pairs
            counted = counts_ref[pair]
            end = first + jnp.where(null, 1, counted)
            slot = slot_ref[pair]

            def earlier(p, total):
                return total + jnp.where(slot_ref[p] < slot, counts_ref[p] + 1, 0)

            target = lax.fori_loop(0, pairs, earlier, jnp.where(null, counted, 0)) - first

            def mark(chunk, carry):
                for step in range(8):
                    b = chunk * 8 + step
                    inside = (first <= b) & (b < end)
                    places_ref[b] = jnp.where(inside, target + b, places_ref[b])
                return carry

            lax.fori_loop(0, blocks // 8, mark, 0)
            return end

        lax.fori_loop(0, order_ref.shape[0], fill, jnp.int32(0))

    factor = HEAD_DIM ** (-0.5) * math.log2(math.e)
    nt = (((1,), (1,)), ((), ()))
    span = (BACK + here) * BLOCK

    def soften(q, k, v, mask):
        s = lax.dot_general(q, k, nt, preferred_element_type=jnp.float32) + mask
        peak = jnp.max(s, axis=1, keepdims=True)
        w = jnp.exp2((s - peak) * factor)
        total = jnp.sum(w, axis=1, keepdims=True)
        mixed = jnp.dot(w.astype(jnp.bfloat16), v, preferred_element_type=jnp.float32)
        return mixed, peak * factor, total

    def help_out(j):
        await_(lower_q.at[j], down_recv.at[j])
        send_near = near(BACK + width)
        for first in range(0, FEW, here):
            count = min(here, FEW - first)
            lines = slice(first * BLOCK, (first + count) * BLOCK)
            window = pl.ds((BACK + skip + first) * BLOCK, (BACK - first) * BLOCK)
            mixed, peak, total = soften(
                lower_q[j, lines, :],
                kv[j, 0, window, :],
                kv[j, 1, window, :],
                lower_bias[lines, first * BLOCK :],
            )
            size = jnp.broadcast_to(peak + jnp.log2(total), (count * BLOCK, BLOCK))
            for b in range(count):
                g = first + b
                turned = size[b * BLOCK : (b + 1) * BLOCK].T
                size_out[j, g] = jnp.where(send_near, HIDDEN, turned[:8])
            mixed = (mixed / total).astype(slot_out.dtype)
            for b in range(count):
                side, line = divmod(first + b, NEAR)
                spot = pl.ds(line * BLOCK, BLOCK)
                block = kv[j, side, pl.ds((BACK + width - NEAR + line) * BLOCK, BLOCK), :]
                slot_out[j, side, spot, :] = jnp.where(
                    send_near, block, mixed[b * BLOCK : (b + 1) * BLOCK]
                )
        for g in range(FEW, 2 * NEAR):
            side, line = divmod(g, NEAR)
            slot_out[j, side, pl.ds(line * BLOCK, BLOCK), :] = kv[
                j, side, pl.ds((BACK + width - NEAR + line) * BLOCK, BLOCK), :
            ]

    def await_up(j, sem):
        words = FEW * 8 * BLOCK * 2 + 2 * NEAR * BLOCK * HEAD_DIM
        await_(kv.at[j, 0, pl.ds(0, words // HEAD_DIM)], sem.at[j])

    def send_up(j):
        remote(
            slot_out.at[j],
            kv.at[j, :, rows(BACK - NEAR, NEAR)],
            up_send.at[j],
            up_recv.at[j],
            me + PLANE,
        )
        remote(size_out.at[j], size_in.at[j], up_send.at[j], up_recv.at[j], me + PLANE)

    def release(j):
        @pl.when(hold(j) & jnp.logical_not(defer(j)))
        def _():
            forward(j, role)
            forward(j, peers[0])

    def empty_places():
        def empty(b, carry):
            places_ref[b] = 0
            return carry

        lax.fori_loop(0, places_ref.shape[0], empty, 0)

    empty_places()

    def far(t, carry):
        j = turn(t)
        with jax.named_scope("take_far"):
            for k in (1, 2):
                take(k, j)

                @pl.when(jnp.logical_not(defer(j)))
                def _():
                    forward(j, peers[k])

        @pl.when(t == min(1, last))
        def _():
            each(release)

        for h in helpable:

            @pl.when(helps(h) & (j == h))
            def _():
                with jax.named_scope("help_out"):
                    help_out(h)

        for h in helpable:

            @pl.when(helps(h) & (j == h))
            def _():
                empty_places()
                send_up(h)

        return carry

    lax.fori_loop(0, planes, far, 0)

    def climb(j):
        @pl.when((plane == 0) & (j > 0))
        def _():
            remote(
                kv.at[j, :, rows(BACK, skip)],
                landed_ref.at[:, rows(0, skip)],
                land_send.at[0],
                arrive_recv.at[0],
                j * PLANE + role,
            )

    descend(climb)

    with jax.named_scope("relay"):
        descend(relay)

    settle = pltpu.make_async_copy(
        kv.at[plane, :, rows(BACK, width)],
        landed_ref.at[:, rows(plane * width, width)],
        leave_sem.at[0],
    )
    settle.start()

    def attend(j, i, variant):
        window = pl.ds(i * tokens, span)
        return soften(
            qs[j, pl.ds(i * tokens, tokens), :],
            kv[j, 0, window, :],
            kv[j, 1, window, :],
            bias[variant, i],
        )

    def finish(j, i, mixed, total):
        real = jnp.concatenate(
            [column < valids[BACK + i * here + b] for b in range(here)], axis=0
        )
        mixed_ref[j, i] = jnp.where(real, mixed / total, 0.0).astype(mixed_ref.dtype)

    def simple(j, i):
        mixed, _, total = attend(j, i, 0)
        finish(j, i, mixed, total)

    def give(j, i):
        target = out_ref.at[:, cols(j * PLANE + role)]

        @pl.when(role == i)
        def _():
            pltpu.make_async_copy(mixed_ref.at[j, i], target, leave_sem.at[0]).start()

        @pl.when(role != i)
        def _():
            remote(mixed_ref.at[j, i], target, share_send.at[0], arrive_recv.at[0], base + i)

    top = PLANE - 1

    def lump(j):
        @pl.when(defer(j))
        def _():
            remote(
                kv.at[j, :, rows(BACK, width)],
                landed_ref.at[:, rows(plane * width, width)],
                land_send.at[0],
                arrive_recv.at[0],
                j * PLANE + role,
            )

    def reach_back(j, waiting):
        with jax.named_scope("wait_halo"):

            @pl.when(late & (j <= plane))
            def _():
                await_halo(j)

        with jax.named_scope("units"):
            for i in range(top - 1, -1, -1):
                simple(j, i)
                if i == top - 1:
                    give(*waiting)
                else:
                    give(j, i + 1)

    def one_head(t, carry):
        j = last - t
        with jax.named_scope("wait_q"):
            await_q(j, False)
        with jax.named_scope("top"):
            simple(j, top)

            @pl.when(t == min(1, last))
            def _():
                descend(lump)

        before = jnp.minimum(j + 1, last)
        earlier = jnp.minimum(j + 2, last)
        full = jnp.logical_not(helped(earlier))

        @pl.when((t > 1) & full)
        def _():
            give(earlier, 0)

        @pl.when((t == 1) | ((t > 1) & jnp.logical_not(full)))
        def _():
            give(before, top)

        @pl.when((t > 0) & jnp.logical_not(helped(before)))
        def _():
            reach_back(before, (j, top))

        return carry

    lax.fori_loop(0, planes, one_head, 0)
    whole = jnp.logical_not(helped(0))

    @pl.when(whole)
    def _():
        reach_back(0, (1, 0))

    settled = pltpu.make_async_copy(
        kv.at[plane, :, rows(0, BACK)], landed_ref.at[:, below], leave_sem.at[0]
    )

    @pl.when(late)
    def _():
        settled.start()

    empty_places()

    @pl.when(whole)
    def _():
        give(0, 0)

    @pl.when(helped(0) & jnp.logical_not(helped(1)))
    def _():
        give(1, 0)

    @pl.when(helped(0) & helped(1))
    def _():
        give(0, top)

    def merge(j):
        with jax.named_scope("wait_part"):
            await_up(j, up_recv)
        with jax.named_scope("merge"):
            for i in range(top - 1, -1, -1):
                mixed, peak, total = attend(j, i, 1)
                mixed = [mixed[b * BLOCK : (b + 1) * BLOCK] for b in range(here)]
                total = [
                    jnp.broadcast_to(total[b * BLOCK : (b + 1) * BLOCK], (BLOCK, BLOCK))
                    for b in range(here)
                ]
                for b in range(here):
                    g = i * here + b
                    if g < FEW:
                        size = jnp.broadcast_to(size_in[j, g, :1], (BLOCK, BLOCK)).T
                        mark = peak[b * BLOCK : (b + 1) * BLOCK]
                        high = jnp.maximum(mark, size)
                        mine_share = jnp.exp2(mark - high)
                        their_share = jnp.exp2(size - high)
                        side, line = divmod(g, NEAR)
                        line = (BACK - NEAR + line) * BLOCK
                        theirs = kv[j, side, line : line + BLOCK, :]
                        mixed[b] = mixed[b] * mine_share + theirs.astype(jnp.float32) * their_share
                        total[b] = total[b] * mine_share + their_share
                finish(
                    j, i, jnp.concatenate(mixed, axis=0), jnp.concatenate(total, axis=0)
                )
                if i < top - 1:
                    give(j, i + 1)
        empty_places()
        give(j, 0)

    for h in helpable:

        @pl.when(helped(h))
        def _():
            merge(h)

    with jax.named_scope("map_places"):
        map_places()


    with jax.named_scope("drain"):
        for h in helpable:

            @pl.when(helps(h))
            def _():
                await_up(h, up_send)

            @pl.when(helped(h))
            def _():
                await_(lower_q.at[h], down_send.at[h])

        for p in range(last):

            @pl.when(plane == p)
            def _():
                count = (planes - len([j for j in helpable if j <= p and 2 * p >= planes - 2])) * BACK
                await_(landed_ref.at[:, rows(0, count)], halo_send.at[0])

        shared = 2 * here * (PLANE - 1)
        outs = here * planes // 2
        passed = (planes - 1) * width

        @pl.when(plane == 0)
        def _():
            await_(landed_ref.at[:, rows(0, (planes - 1) * skip)], land_send.at[0])
            await_(landed_ref.at[:, rows(0, width + outs)], leave_sem.at[0])

        @pl.when(late)
        def _():
            await_(landed_ref.at[:, rows(0, passed)], land_send.at[0])
            await_(landed_ref.at[:, rows(0, width + BACK + outs)], leave_sem.at[0])

        await_(kv.at[:, :, rows(0, shared)], share_send.at[0])

    with jax.named_scope("land"):
        others = outs * (PLANE - 1)

        @pl.when(late)
        def _():
            await_(landed_ref.at[:, rows(0, passed - BACK + others)], arrive_recv.at[0])

        @pl.when(plane == 0)
        def _():
            await_(kv.at[:, :, rows(0, (passed + others) // planes)], arrive_recv.at[0])


def wide_exchange(n, queries, keys, values, block_counts, last_tokens, pack_order):
    tokens, features = queries.shape
    here = tokens // BLOCK
    part = BLOCK // (n // HEADS)
    blocks = here * n
    kind = queries.dtype
    smem = pl.BlockSpec(memory_space=pltpu.SMEM)
    vmem = pl.BlockSpec(memory_space=pltpu.VMEM)
    anywhere = pl.BlockSpec(memory_space=pl.ANY)
    dma = pltpu.SemaphoreType.DMA
    return pl.pallas_call(
        functools.partial(exchange, n),
        out_shape=(
            jax.ShapeDtypeStruct((tokens, features), kind),
            jax.ShapeDtypeStruct((2, blocks * part, HEAD_DIM), kind),
        ),
        in_specs=[smem] * 3 + [anywhere] * 3,
        out_specs=(vmem, anywhere),
        scratch_shapes=[
            pltpu.VMEM((tokens, features), kind),
            pltpu.VMEM((2, tokens, features), kind),
            pltpu.VMEM((2, BACK * BLOCK, features), kind),
            pltpu.VMEM((2, 2 * BLOCK, features), kind),
            pltpu.VMEM((tokens, (BACK + here) * BLOCK), jnp.float32),
            dma((CHUNKS * 18,)),
            dma((BACK + 2, CHUNKS)),
            dma((2,)),
            dma((here,)),
            dma((3,)),
        ],
        compiler_params=pltpu.CompilerParams(
            collective_id=0, has_side_effects=True, vmem_limit_bytes=60 * 1024 * 1024
        ),
    )(block_counts, last_tokens, pack_order, queries, keys, values)


def local(n, queries, keys, values, block_counts, last_tokens, pack_order, decode_slot):
    tokens, features = queries.shape
    here = tokens // BLOCK
    splits = n // HEADS
    part = BLOCK // splits
    blocks = here * n
    kind = queries.dtype
    smem = pl.BlockSpec(memory_space=pltpu.SMEM)
    anywhere = pl.BlockSpec(memory_space=pl.ANY)
    dma = pltpu.SemaphoreType.DMA
    planes = n // PLANE
    few = FEW * BLOCK
    last = planes - 1
    cache = jax.ShapeDtypeStruct((1, blocks, part, HEAD_DIM), kind)
    if splits == 1 and here == 2 and planes > 1:
        attended, landed, places = pl.pallas_call(
            functools.partial(handoff, n),
            out_shape=(
                pltpu.VMEM((tokens, features), kind),
                pltpu.VMEM((2, blocks * part, HEAD_DIM), kind),
                pltpu.SMEM((blocks,), jnp.int32),
            ),
            in_specs=[anywhere] * 7,
            out_specs=(anywhere, anywhere, smem),
            scratch_shapes=[
                pltpu.SMEM(block_counts.shape, jnp.int32),
                pltpu.SMEM(last_tokens.shape, jnp.int32),
                pltpu.SMEM(pack_order.shape, jnp.int32),
                pltpu.SMEM(decode_slot.shape, jnp.int32),
                pltpu.VMEM((tokens, features), kind),
                pltpu.VMEM((2, tokens, features), kind),
                pltpu.VMEM((planes, 2, (BACK + PLANE * here) * BLOCK, HEAD_DIM), kind),
                pltpu.VMEM((planes, PLANE * tokens, HEAD_DIM), kind),
                pltpu.VMEM((planes, PLANE, tokens, HEAD_DIM), kind),
                pltpu.VMEM((2, PLANE, tokens, (BACK + here) * BLOCK), jnp.float32),
                pltpu.VMEM((planes, few, HEAD_DIM), kind),
                pltpu.VMEM((few, BACK * BLOCK), jnp.float32),
                pltpu.VMEM((planes, 2, NEAR * BLOCK, HEAD_DIM), kind),
                pltpu.VMEM((planes, FEW, 8, BLOCK), jnp.float32),
                pltpu.VMEM((planes, FEW, 8, BLOCK), jnp.float32),
                dma((6,)),
                dma((2,)),
                dma((1,)),
                dma((1,)),
                dma((PLANE - 1, planes)),
                dma((2, planes)),
                dma((1,)),
                dma((planes,)),
                dma((1,)),
                dma((1,)),
                dma((last // 2 + 1,)),
                dma((last // 2 + 1,)),
                dma((last // 2 + 1,)),
                dma((last // 2 + 1,)),
            ],
            compiler_params=pltpu.CompilerParams(
                collective_id=0, has_side_effects=True, vmem_limit_bytes=60 * 1024 * 1024
            ),
        )(block_counts, last_tokens, pack_order, decode_slot, queries, keys, values)
        return pl.pallas_call(
            publish,
            out_shape=(jax.ShapeDtypeStruct((tokens, features), kind), cache, cache),
            in_specs=[smem] + [anywhere] * 2,
            out_specs=(anywhere,) * 3,
            scratch_shapes=[dma((3,))],
        )(
            pltpu.with_memory_space_constraint(places, pltpu.SMEM),
            pltpu.with_memory_space_constraint(landed, pltpu.VMEM),
            pltpu.with_memory_space_constraint(attended, pltpu.VMEM),
        )
    attended, landed = wide_exchange(
        n, queries, keys, values, block_counts, last_tokens, pack_order
    )
    cache_keys, cache_values = pl.pallas_call(
        reorder,
        out_shape=(cache, cache),
        in_specs=[smem] * 3 + [anywhere],
        out_specs=(anywhere, anywhere),
        scratch_shapes=[
            pltpu.VMEM((2, blocks, part, HEAD_DIM), kind),
            pltpu.SMEM(block_counts.shape, jnp.int32),
            pltpu.SMEM(block_counts.shape, jnp.int32),
            dma((2,)),
            dma((2,)),
        ],
    )(block_counts, pack_order, decode_slot, landed)
    return attended, cache_keys, cache_values


def solution(mesh):
    rows = P(("groups", "seq"), None)
    small = P("groups")
    cache = P(("groups", "seq"), None, None, None)
    return jax.shard_map(
        functools.partial(local, mesh.shape["seq"]),
        mesh=mesh,
        in_specs=(rows, rows, rows, small, small, small, small),
        out_specs=(rows, cache, cache),
        check_vma=False,
    )
```
